32 devices in a mesh: slab: 8 (over z, y), batch: 4 (over x, core).
Axes of the slice: x: 2, y: 2, z: 4, core: 2. Of those that a mesh axis runs over, the one named last changes fastest.
Arguments:
- velocity_old: float32 [3, 16, 64, 128], P(None, 'slab', 'batch'), may hold values from -40 to 40
- courant: float32 [3, 16, 64, 128], P(None, 'slab', 'batch'), may hold values from -1.5 to 1.5
- cell_ids: int32 [32768], P(('slab', 'batch')), may hold values from 0 to 16383
- forces: float32 [3, 32768], P(None, ('slab', 'batch')), may hold values from -6 to 6
- weights: float32 [32768], P(('slab', 'batch')), may hold values from 0.25 to 4
Outputs:
- velocity_new: float32 [3, 16, 64, 128], P(None, 'slab', 'batch')
- residual: float32 [3, 16, 64, 128], P(None, 'slab', 'batch')
The draws below stay inside these ranges and needn't reach their ends.
Inputs may be any that keep to these rules, and one draw needn't show every extreme that they name: `cell_ids`: each device's block of 1024 particles lists 1 * 128 particles for each destination slab in turn, slab 0 first.
All inputs are finite; a program needn't handle non-finite values.
Results may differ from the reference program's by a relative error of at most 0.0012.
Values may be sent and summed in bfloat16 or wider, within the bound.
No kernel may reach another device: no remote copies, remote signals or barrier semaphores. Data moves between devices by JAX's collectives and lax.ppermute only.
A program may use at most 64 MiB of HBM per device.

```python
import math
import jax
import jax.numpy as jnp
from jax import lax

CZ = 2
NY = 64
NX = 128
TILES = 1
TILE = 128
ITERS = 2
NZ = 16
PART_DEV = 1024
PARTICLES = 32768
N_SLAB = 8


def draw_velocity_old(key, part):
    key_base, key_rows, key_cols = jax.random.split(jax.random.fold_in(key, 11), 3)
    depth_share = (jnp.arange(NZ, dtype=jnp.float32) + 0.5) / NZ
    row_share = (jnp.arange(NY, dtype=jnp.float32) + 0.5) / NY
    column_share = (jnp.arange(NX, dtype=jnp.float32) + 0.5) / NX
    row_scale = jnp.exp(jax.random.uniform(key_rows, (NY,), jnp.float32, math.log(0.3), math.log(3.0)))
    column_scale = jnp.exp(jax.random.uniform(key_cols, (NX,), jnp.float32, math.log(0.6), math.log(1.6)))
    depth_bump = jnp.sin(math.pi * depth_share)
    column_bump = jnp.sin(math.pi * column_share)
    base_values = jnp.clip(jax.random.normal(key_base, (3, NZ, NY, NX), jnp.float32), -3.0, 3.0)
    depth_trend = 1.0 + depth_share
    smooth_level = 0.5 + 7.5 * row_share
    scaled = base_values * depth_trend[:, None, None] * row_scale[:, None] * column_scale[None, :]
    smooth = depth_bump[:, None, None] * smooth_level[None, :, None] * column_bump[None, None, :]
    return scaled + smooth[None]


def touch_ends(values, key, smallest, largest):
    place = [jax.random.randint(jax.random.fold_in(key, axis), (), 0, length) for axis, length in enumerate(values.shape)]
    longest = values.shape.index(max(values.shape))
    neighbour = place[:longest] + [(place[longest] + 1) % values.shape[longest]] + place[longest + 1:]
    return values.at[tuple(place)].set(smallest).at[tuple(neighbour)].set(largest)


def block_levels(stream_key, shape, cuts, low, high):
    level, own = 1.0, jax.random.fold_in(stream_key, 6)
    for axis_at, blocks in cuts:
        draws = jnp.exp(jax.random.uniform(jax.random.fold_in(own, axis_at), (blocks,), jnp.float32, low / len(cuts), high / len(cuts)))
        level = level * jnp.repeat(draws, shape[axis_at] // blocks).reshape([-1 if axis == axis_at else 1 for axis in range(len(shape))])
    return level


def gaussian(own_key, shape, spread, most, cuts=(), kind=jnp.bfloat16):
    drawn = spread * jax.random.normal(own_key, shape, jnp.float32)
    if cuts:
        drawn = drawn * block_levels(own_key, shape, cuts, -0.22, 0.18)
    return jnp.clip(drawn, -most, most).astype(kind)


def setup_inputs(seed: int = 0) -> dict:
    splits = jax.random.split(jax.random.key(seed), 6)
    velocity_old = draw_velocity_old(jax.random.fold_in(splits[5], 71), 0)
    courant = jnp.clip(jax.random.uniform(splits[1], (3, NZ, NY, NX), jnp.float32, -1.5, 1.5) * block_levels(splits[1], (3, NZ, NY, NX), ((1, 8), (2, 4)), -0.4, 0.0), -1.5, 1.5)
    cell_ids = touch_ends(jax.random.randint(splits[2], (PARTICLES,), 0, CZ * NY * NX), jax.random.fold_in(splits[2], 1), 0, (CZ * NY * NX) - 1).astype(jnp.int32)
    forces = gaussian(splits[3], (3, PARTICLES), 1.0, 6.0, ((1, 32),), jnp.float32)
    weights = jnp.clip(jnp.exp(math.log(4.0) - 2.7725887 * jax.random.uniform(splits[4], (PARTICLES,), jnp.float32) ** block_levels(splits[4], (PARTICLES,), ((0, 32),), -0.2, 0.2)), 0.25, 4.0)
    return dict(velocity_old=velocity_old, courant=courant, cell_ids=cell_ids, forces=forces, weights=weights)


diffusion_number = 1.0
diagonal_value = 7.0


def inner_product(left, right):
    return jnp.sum(left * right, axis=(1, 2, 3))


def expand(scalars):
    return scalars[:, None, None, None]


def factorize(upper_planes, lower_planes):
    inverses = []
    ratios = []
    for plane_index in range(len(upper_planes)):
        if plane_index == 0:
            pivot_value = diagonal_value + jnp.zeros_like(upper_planes[0])
        else:
            pivot_value = diagonal_value + lower_planes[plane_index] * ratios[-1]
        inverses.append(1.0 / pivot_value)
        ratios.append(-upper_planes[plane_index] * inverses[-1])
    return inverses, ratios


def solve_planes(value_planes, inverses, ratios, lower_planes):
    forward = []
    for plane_index in range(len(value_planes)):
        current = value_planes[plane_index]
        if plane_index > 0:
            current = current + lower_planes[plane_index] * forward[-1]
        forward.append(current * inverses[plane_index])
    result = [forward[-1]]
    for plane_index in range(len(value_planes) - 2, -1, -1):
        result.insert(0, forward[plane_index] - ratios[plane_index] * result[0])
    return result


def reference(velocity_old, courant, cell_ids, forces, weights):
    momentum = (weights[None, :] * forces).astype(jnp.bfloat16)
    momentum = lax.optimization_barrier(momentum).astype(jnp.float32)
    position = lax.iota(jnp.int32, cell_ids.shape[0])
    target = (position % PART_DEV) // (TILES * TILE)
    flat_cell = (target * (CZ * NY * NX) + cell_ids).astype(jnp.int32)
    source = jnp.zeros((3, NZ * NY * NX), jnp.float32).at[:, flat_cell].add(momentum)
    source = source.reshape(3, NZ, NY, NX)
    right_side = velocity_old + source

    upper = diffusion_number - 0.5 * courant
    lower = diffusion_number + 0.5 * courant

    def operate(values):
        padded = jnp.pad(values, ((0, 0), (1, 1), (1, 1), (1, 1)))
        beside = upper[0] * padded[:, 2:, 1:-1, 1:-1] + lower[0] * padded[:, :-2, 1:-1, 1:-1]
        beside = beside + upper[1] * padded[:, 1:-1, 2:, 1:-1] + lower[1] * padded[:, 1:-1, :-2, 1:-1]
        beside = beside + upper[2] * padded[:, 1:-1, 1:-1, 2:] + lower[2] * padded[:, 1:-1, 1:-1, :-2]
        return diagonal_value * values - beside

    upper_blocks = upper[0].reshape(N_SLAB, CZ, NY, NX)
    lower_blocks = lower[0].reshape(N_SLAB, CZ, NY, NX)
    upper_planes = [upper_blocks[:, plane_index] for plane_index in range(CZ)]
    lower_planes = [lower_blocks[:, plane_index] for plane_index in range(CZ)]
    inverses, ratios = factorize(upper_planes, lower_planes)

    def precondition(values):
        blocks = values.reshape(3, N_SLAB, CZ, NY, NX)
        value_planes = [blocks[:, :, plane_index] for plane_index in range(CZ)]
        result = solve_planes(value_planes, inverses, ratios, lower_planes)
        return jnp.stack(result, axis=2).reshape(3, NZ, NY, NX)

    solution = jnp.zeros_like(right_side)
    residual = right_side
    shadow = right_side
    direction = right_side
    rho_now = inner_product(shadow, residual)
    for iteration in range(ITERS):
        precond_dir = precondition(direction)
        image_dir = operate(precond_dir)
        step_alpha = rho_now / inner_product(shadow, image_dir)
        middle = residual - expand(step_alpha) * image_dir
        precond_mid = precondition(middle)
        turned = operate(precond_mid)
        step_omega = inner_product(turned, middle) / inner_product(turned, turned)
        solution = solution + expand(step_alpha) * precond_dir + expand(step_omega) * precond_mid
        residual = middle - expand(step_omega) * turned
        if iteration + 1 < ITERS:
            rho_next = inner_product(shadow, residual)
            factor = (rho_next / rho_now) * (step_alpha / step_omega)
            direction = residual + expand(factor) * (direction - expand(step_omega) * image_dir)
            rho_now = rho_next
    return (solution, residual)
```

```python
import jax
import jax.numpy as jnp
from jax import lax
from jax.experimental import pallas as pl
from jax.experimental.pallas import tpu as pltpu
from jax.sharding import PartitionSpec as P

ITERS = 2
DEPTH = 2 * ITERS
COMPS = 3
BASIS = DEPTH + 1
PAIRS = [(i, j) for i in range(BASIS) for j in range(i, BASIS)]

diffusion_number = 1.0
diagonal_value = 7.0

VMEM = pl.BlockSpec(memory_space=pltpu.VMEM)
SMEM = pl.BlockSpec(memory_space=pltpu.SMEM)
F32 = jnp.float32


def two_sum(a, b):
    s = a + b
    bb = s - a
    return s, (a - (s - bb)) + (b - bb)


def quick_two_sum(a, b):
    s = a + b
    return s, b - (s - a)


def split(a):
    t = a * 4097.0
    high = t - (t - a)
    return high, a - high


def product_error(p, a, b):
    ah, al = a
    bh, bl = b
    return ((ah * bh - p) + ah * bl + al * bh) + al * bl


def dd_add(a, b):
    s, e = two_sum(a[0], b[0])
    return quick_two_sum(s, e + (a[1] + b[1]))


def dd_neg(a):
    return -a[0], -a[1]


def dd_sub(a, b):
    return dd_add(a, dd_neg(b))


def dd_mul(a, b):
    p = a[0] * b[0]
    e = product_error(p, split(a[0]), split(b[0]))
    return quick_two_sum(p, e + (a[0] * b[1] + a[1] * b[0]))


def dd_div(a, b):
    inverse = 1.0 / b[0]
    q1 = a[0] * inverse
    zero = jnp.zeros_like(q1)
    r = dd_sub(a, dd_mul((q1, zero), b))
    q2 = r[0] * inverse
    r = dd_sub(r, dd_mul((q2, zero), b))
    q3 = r[0] * inverse
    s, e = quick_two_sum(q1, q2)
    return quick_two_sum(s, e + q3)


def solve_block(values, inverses, ratios, lower_planes):
    forward = []
    for k, current in enumerate(values):
        if k > 0:
            current = current + lower_planes[k] * forward[-1]
        forward.append(current * inverses[k])
    result = [forward[-1]]
    for k in range(len(values) - 2, -1, -1):
        result.insert(0, forward[k] - ratios[k] * result[0])
    return result


def make_message(ids, momentum, slabs, copies, row_width):
    tile = ids.shape[0] // slabs
    high = (ids // row_width).astype(jnp.bfloat16)
    low = (ids % row_width).astype(jnp.bfloat16)
    rows = jnp.concatenate(
        [momentum, high[None], low[None], jnp.zeros((3, ids.shape[0]), jnp.bfloat16)], axis=0
    )
    rows = rows.reshape(8, slabs, tile).transpose(1, 0, 2)
    rows = jnp.broadcast_to(rows[:, None], (slabs, copies, 8, tile))
    return rows.reshape(slabs * copies, 8, tile)


def setup_kernel(
    slabs, copies, group,
    place, message, velocity, velocity_halo, courant, courant_halo,
    value_out, solved_out, first_out, last_out, side_out, block_out, momentum_sum,
):
    planes, rows, width = velocity.shape[1:]
    wide = rows + 2 * DEPTH
    height = rows * copies
    slab, batch = place[0], place[1]
    start = batch * rows
    tile = message.shape[2]
    row_iota = lax.broadcasted_iota(jnp.int32, (planes * wide, tile), 0)
    column_iota = lax.broadcasted_iota(jnp.int32, (width, tile), 0)

    def deposit(step):
        row_hot, spread = [], []
        for k in range(group):
            part = message[step * group + k].astype(F32)
            cell_row = part[3:4].astype(jnp.int32)
            column = part[4:5].astype(jnp.int32)
            plane = jnp.zeros_like(cell_row)
            for p in range(1, planes):
                plane = plane + (cell_row >= p * height).astype(jnp.int32)
            away = cell_row - plane * height - start
            away = jnp.where(away < 0, away + height, away)
            spot = jnp.where(away < rows + DEPTH, away, away - height + wide)
            inside = (away < rows + DEPTH) | (away >= height - DEPTH)
            spot = jnp.where(inside, spot + plane * wide, -1)
            row_hot.append(jnp.where(row_iota == spot, 1.0, 0.0).astype(jnp.bfloat16))
            here = column_iota == column
            spread.append(
                jnp.concatenate(
                    [jnp.where(here, part[c : c + 1], 0.0) for c in range(COMPS)], axis=0
                ).astype(jnp.bfloat16)
            )
        return lax.dot_general(
            jnp.concatenate(row_hot, axis=1),
            jnp.concatenate(spread, axis=1),
            (((1,), (1,)), ((), ())),
            preferred_element_type=F32,
        )

    steps = message.shape[0] // group
    if steps <= 4:
        total = deposit(0)
        for step in range(1, steps):
            total = total + deposit(step)
        momentum_sum[...] = total
    else:
        momentum_sum[...] = jnp.zeros_like(momentum_sum)

        def one(step, carry):
            momentum_sum[...] += deposit(step)
            return carry

        lax.fori_loop(0, steps, one, 0)

    spots = lax.broadcasted_iota(jnp.int32, (wide, width), 0)
    lanes = lax.broadcasted_iota(jnp.int32, (wide, width), 1)
    lower_planes, upper_planes, inverses, ratios = [], [], [], []
    for k in range(planes):
        coefs = []
        for d in range(3):
            half = 0.5 * jnp.concatenate([courant[d, k], courant_halo[d, k]], axis=0)
            coefs.append((diffusion_number - half, diffusion_number + half))
        upper_planes.append(coefs[0][0])
        lower_planes.append(coefs[0][1])
        at_top = (spots == rows - 1) & (batch == copies - 1)
        at_bottom = (spots == 0) & (batch == 0)
        side_out[0, k] = jnp.where(at_top, 0.0, coefs[1][0])
        side_out[1, k] = jnp.where(at_bottom, 0.0, coefs[1][1])
        side_out[2, k] = jnp.where(lanes == width - 1, 0.0, coefs[2][0])
        side_out[3, k] = jnp.where(lanes == 0, 0.0, coefs[2][1])
        if k == 0:
            pivot = jnp.full((wide, width), diagonal_value, F32)
        else:
            pivot = diagonal_value + lower_planes[k] * ratios[-1]
        inverses.append(1.0 / pivot)
        ratios.append(-upper_planes[k] * inverses[-1])
        block_out[0, k] = inverses[k]
        block_out[1, k] = ratios[k]
        block_out[2, k] = lower_planes[k]
    block_out[3, 0] = jnp.where(slab == 0, 0.0, lower_planes[0])
    block_out[3, 1] = jnp.where(slab == slabs - 1, 0.0, upper_planes[planes - 1])
    for c in range(COMPS):
        values = []
        for k in range(planes):
            old = jnp.concatenate([velocity[c, k], velocity_halo[c, k]], axis=0)
            value = old + momentum_sum[k * wide : (k + 1) * wide, c * width : (c + 1) * width]
            value_out[c, k] = value
            values.append(value)
        solved = solve_block(values, inverses, ratios, lower_planes)
        for k in range(planes):
            solved_out[c, k] = solved[k]
        first_out[c] = solved[0]
        last_out[c] = solved[planes - 1]


def couple(c, solved, below, above, side, block):
    planes, wide = solved.shape[1:3]
    width = solved.shape[3]
    result = []
    for k in range(planes):
        here = solved[c, k]
        total = side[0, k] * pltpu.roll(here, wide - 1, 0) + side[1, k] * pltpu.roll(here, 1, 0)
        total = total + side[2, k] * pltpu.roll(here, width - 1, 1)
        total = total + side[3, k] * pltpu.roll(here, 1, 1)
        if k == 0:
            total = total + block[3, 0] * below[c]
        if k == planes - 1:
            total = total + block[3, 1] * above[c]
        result.append(total)
    return result


def apply_kernel(
    solved, below, above, side, block, value_out, solved_out, first_out, last_out
):
    planes = solved.shape[1]
    inverses = [block[0, k] for k in range(planes)]
    ratios = [block[1, k] for k in range(planes)]
    lower_planes = [block[2, k] for k in range(planes)]
    for c in range(COMPS):
        values = couple(c, solved, below, above, side, block)
        result = solve_block(values, inverses, ratios, lower_planes)
        for k in range(planes):
            value_out[c, k] = values[k]
            solved_out[c, k] = result[k]
        first_out[c] = result[0]
        last_out[c] = result[planes - 1]


def gram_kernel(slots, *refs):
    solved, below, above, side, block = refs[:5]
    values = refs[5 : 5 + DEPTH]
    value_out, message_out = refs[5 + DEPTH :]
    planes, wide, width = solved.shape[1:]
    rows = wide - 2 * DEPTH
    sums = []
    for c in range(COMPS):
        newest = couple(c, solved, below, above, side, block)
        for k in range(planes):
            value_out[c, k] = newest[k]
        totals = [None] * len(PAIRS)
        for k in range(planes):
            for r in range(0, rows, 8):
                pieces = [values[i][c, k, r : r + 8, :] for i in range(DEPTH)]
                pieces.append(newest[k][r : r + 8])
                halves = [split(piece) for piece in pieces]
                for n, (i, j) in enumerate(PAIRS):
                    p = pieces[i] * pieces[j]
                    e = product_error(p, halves[i], halves[j])
                    if totals[n] is None:
                        totals[n] = (p, e)
                    else:
                        s, t = two_sum(totals[n][0], p)
                        totals[n] = (s, totals[n][1] + (t + e))
        sums.append(totals)
    flat = [sums[c][n] for n in range(len(PAIRS)) for c in range(COMPS)]
    columns = []
    for part in range(2):
        stacked = jnp.concatenate([x[part] for x in flat], axis=0)
        padded = slots * 8 - stacked.shape[0]
        if padded:
            stacked = jnp.concatenate([stacked, jnp.zeros((padded, width), F32)], axis=0)
        columns.append(jnp.transpose(stacked))
    total = (columns[0][:8], columns[1][:8])
    for r in range(8, width, 8):
        total = dd_add(total, (columns[0][r : r + 8], columns[1][r : r + 8]))
    for shift in (4, 2, 1):
        total = dd_add(total, tuple(pltpu.roll(x, shift, 0) for x in total))
    size = slots * 8
    for shift in (4, 2, 1):
        total = dd_add(total, tuple(pltpu.roll(x, size - shift, 1) for x in total))
    row = jnp.concatenate([total[0][:1], total[1][:1]], axis=1)
    message_out[...] = jnp.broadcast_to(row, message_out.shape)


def finish_kernel(slots, *refs):
    gathered = refs[0]
    values = refs[1 : 1 + BASIS]
    solved = refs[1 + BASIS : 1 + BASIS + DEPTH]
    solution_out, residual_out = refs[1 + BASIS + DEPTH :]
    planes, rows, width = solution_out.shape[1:]
    size = slots * 8
    count = gathered.shape[0]
    high, low = gathered[:, :size], gathered[:, size:]
    total = (high[:8], low[:8])
    for r in range(8, count, 8):
        total = dd_add(total, (high[r : r + 8], low[r : r + 8]))
    for shift in (4, 2, 1):
        total = dd_add(total, tuple(pltpu.roll(x, shift, 0) for x in total))
    lane = lax.broadcasted_iota(jnp.int32, (8, 128), 1)
    sub = lax.broadcasted_iota(jnp.int32, (8, 128), 0)

    def entry(n):
        result = []
        for x in total:
            out = None
            for c in range(COMPS):
                at = 8 * (n * COMPS + c)
                chunk = x[:, at // 128 * 128 : at // 128 * 128 + 128]
                moved = pltpu.roll(chunk, (128 - at % 128 + c) % 128, 1)
                out = moved if out is None else jnp.where(lane == c, moved, out)
            result.append(out)
        return tuple(result)

    entries = {pair: entry(n) for n, pair in enumerate(PAIRS)}
    gram = []
    for i in range(BASIS):
        row = None
        for j in range(BASIS):
            item = entries[(min(i, j), max(i, j))]
            if row is None:
                row = item
            else:
                row = tuple(jnp.where(sub == j, x, y) for x, y in zip(item, row))
        gram.append(row)
    zero = jnp.zeros((8, 128), F32)
    nothing = (zero, zero)
    one = (zero + 1.0, zero)

    def stack(poly):
        out = (zero, zero)
        for j, item in enumerate(poly):
            out = tuple(jnp.where(sub == j, x, y) for x, y in zip(item, out))
        return out

    def over_sublanes(x):
        for shift in (4, 2, 1):
            x = dd_add(x, tuple(pltpu.roll(y, shift, 0) for y in x))
        return x

    def gram_times(poly):
        out = None
        for i, item in enumerate(poly):
            term = dd_mul(item, gram[i])
            out = term if out is None else dd_add(out, term)
        return tuple(jnp.where(sub < BASIS, x, 0.0) for x in out)

    def operate(poly):
        out = list(poly) + [nothing]
        return [out[0]] + [dd_sub(out[i], out[i - 1]) for i in range(1, len(out))]

    def combine(first, factor, second):
        out = []
        for i in range(max(len(first), len(second))):
            item = first[i] if i < len(first) else nothing
            if i < len(second):
                item = dd_add(item, dd_mul(factor, second[i]))
            out.append(item)
        return out

    shadow = tuple(jnp.where(sub < BASIS, x, 0.0) for x in gram[0])

    residual = [one]
    direction = [one]
    answer = []
    rho = entries[(0, 0)]
    for iteration in range(ITERS):
        image = operate(direction)
        alpha = dd_div(rho, over_sublanes(dd_mul(shadow, stack(image))))
        middle = combine(residual, dd_neg(alpha), image)
        turned = operate(middle)
        weighted = gram_times(turned)
        cross = over_sublanes(dd_mul(weighted, stack(middle)))
        square = over_sublanes(dd_mul(weighted, stack(turned)))
        omega = dd_div(cross, square)
        answer = combine(answer, alpha, direction)
        answer = combine(answer, omega, middle)
        residual = combine(middle, dd_neg(omega), turned)
        if iteration + 1 < ITERS:
            rho_next = over_sublanes(dd_mul(shadow, stack(residual)))
            factor = dd_mul(dd_div(rho_next, rho), dd_div(alpha, omega))
            direction = combine(direction, dd_neg(omega), image)
            direction = combine(residual, factor, direction)
            rho = rho_next
    for c in range(COMPS):
        answer_at = [item[0][:, c : c + 1] for item in answer]
        residual_at = [item[0][:, c : c + 1] for item in residual]
        for k in range(planes):
            for r in range(0, rows, 8):
                out = answer_at[0] * solved[0][c, k, r : r + 8, :]
                for i in range(1, DEPTH):
                    out = out + answer_at[i] * solved[i][c, k, r : r + 8, :]
                solution_out[c, k, r : r + 8, :] = out
                out = residual_at[0] * values[0][c, k, r : r + 8, :]
                for i in range(1, BASIS):
                    out = out + residual_at[i] * values[i][c, k, r : r + 8, :]
                residual_out[c, k, r : r + 8, :] = out


def ring(array, axis, step):
    count = lax.axis_size(axis)
    return lax.ppermute(array, axis, [(i, (i + step) % count) for i in range(count)])


def local(velocity_old, courant, cell_ids, forces, weights):
    planes, rows, width = velocity_old.shape[1:]
    slabs, copies = lax.axis_size("slab"), lax.axis_size("batch")
    everyone = ("slab", "batch")
    wide = rows + 2 * DEPTH
    height = rows * copies
    assert rows % 8 == 0 and width == 128 and planes * height <= 256 and DEPTH * 2 <= height - rows
    slots = -(-len(PAIRS) * COMPS // 16) * 16
    place = jnp.stack([lax.axis_index("slab"), lax.axis_index("batch")]).astype(jnp.int32)

    momentum = (weights[None, :] * forces).astype(jnp.bfloat16)
    message = make_message(cell_ids, momentum, slabs, copies, width)
    fields = jnp.concatenate([velocity_old, courant], axis=0)
    after = ring(fields[:, :, :DEPTH], "batch", -1)
    before = ring(fields[:, :, rows - DEPTH :], "batch", 1)
    halo = jnp.concatenate([after, before], axis=2)
    received = lax.all_to_all(message, everyone, 0, 0, tiled=True)

    field = jax.ShapeDtypeStruct((COMPS, planes, wide, width), F32)
    face = jax.ShapeDtypeStruct((COMPS, wide, width), F32)
    side_shape = jax.ShapeDtypeStruct((4, planes, wide, width), F32)
    block_shape = jax.ShapeDtypeStruct((4, planes, wide, width), F32)
    group = 8

    def setup(*refs):
        setup_kernel(slabs, copies, group, *refs)

    value, solved, first, last, side, block = pl.pallas_call(
        setup,
        out_shape=(field, field, face, face, side_shape, block_shape),
        in_specs=[SMEM] + [VMEM] * 5,
        out_specs=[VMEM] * 6,
        scratch_shapes=[pltpu.VMEM((planes * wide, COMPS * width), F32)],
        name="setup",
    )(place, received, velocity_old, halo[:COMPS], courant, halo[COMPS:])

    values, solves = [value], [solved]
    for step in range(1, DEPTH + 1):
        below = ring(last, "slab", 1)
        above = ring(first, "slab", -1)
        if step < DEPTH:
            value, solved, first, last = pl.pallas_call(
                apply_kernel,
                out_shape=(field, field, face, face),
                in_specs=[VMEM] * 5,
                out_specs=[VMEM] * 4,
                name="apply",
            )(solved, below, above, side, block)
            solves.append(solved)
        else:

            def gram(*refs):
                gram_kernel(slots, *refs)

            value, message = pl.pallas_call(
                gram,
                out_shape=(
                    field,
                    jax.ShapeDtypeStruct((slabs * copies, 2 * slots * 8), F32),
                ),
                in_specs=[VMEM] * (5 + DEPTH),
                out_specs=[VMEM] * 2,
                name="gram",
            )(solved, below, above, side, block, *values)
        values.append(value)
    gathered = lax.all_to_all(message, everyone, 0, 0, tiled=True)

    def finish(*refs):
        finish_kernel(slots, *refs)

    own = jax.ShapeDtypeStruct(velocity_old.shape, F32)
    return pl.pallas_call(
        finish,
        out_shape=(own, own),
        in_specs=[VMEM] * (1 + BASIS + DEPTH),
        out_specs=[VMEM] * 2,
        name="finish",
    )(gathered, *values, *solves)


def solution(mesh):
    placed = (
        P(None, "slab", "batch", None),
        P(None, "slab", "batch", None),
        P(("slab", "batch")),
        P(None, ("slab", "batch")),
        P(("slab", "batch")),
    )
    return jax.shard_map(
        local,
        mesh=mesh,
        in_specs=placed,
        out_specs=(P(None, "slab", "batch", None), P(None, "slab", "batch", None)),
        check_vma=False,
    )
```

```python
import jax
import jax.numpy as jnp
from jax import lax
from jax.experimental import pallas as pl
from jax.experimental.pallas import tpu as pltpu
from jax.sharding import PartitionSpec as P


ITERS = 2
DEPTH = 2 * ITERS
COMPS = 3
BASIS = DEPTH + 1
PAIRS = [(i, j) for i in range(BASIS) for j in range(i, BASIS)]

diffusion_number = 1.0
diagonal_value = 7.0

VMEM = pl.BlockSpec(memory_space=pltpu.VMEM)
ANY = pl.BlockSpec(memory_space=pl.ANY)
F32 = jnp.float32


def two_sum(a, b):
    s = a + b
    bb = s - a
    return s, (a - (s - bb)) + (b - bb)


def quick_two_sum(a, b):
    s = a + b
    return s, b - (s - a)


def split(a):
    t = a * 4097.0
    high = t - (t - a)
    return high, a - high


def product_error(p, a, b):
    ah, al = a
    bh, bl = b
    return ((ah * bh - p) + ah * bl + al * bh) + al * bl


def dd_add(a, b):
    s, e = two_sum(a[0], b[0])
    return quick_two_sum(s, e + (a[1] + b[1]))


def dd_neg(a):
    return -a[0], -a[1]


def dd_sub(a, b):
    return dd_add(a, dd_neg(b))


def dd_mul(a, b):
    p = a[0] * b[0]
    e = product_error(p, split(a[0]), split(b[0]))
    return quick_two_sum(p, e + (a[0] * b[1] + a[1] * b[0]))


def dd_div(a, b):
    inverse = 1.0 / b[0]
    q1 = a[0] * inverse
    zero = jnp.zeros_like(q1)
    r = dd_sub(a, dd_mul((q1, zero), b))
    q2 = r[0] * inverse
    r = dd_sub(r, dd_mul((q2, zero), b))
    q3 = r[0] * inverse
    s, e = quick_two_sum(q1, q2)
    return quick_two_sum(s, e + q3)


def solve_block(values, inverses, ratios, lower_planes):
    forward = []
    for k, current in enumerate(values):
        if k > 0:
            current = current + lower_planes[k] * forward[-1]
        forward.append(current * inverses[k])
    result = [forward[-1]]
    for k in range(len(values) - 2, -1, -1):
        result.insert(0, forward[k] - ratios[k] * result[0])
    return result


def pack_kernel(slabs, copies, ids_in, forces_in, weights_in, message_out, ids, forces, weights, arrived):
    moves = [
        pltpu.make_async_copy(source, target, arrived.at[n])
        for n, (source, target) in enumerate(
            [(ids_in, ids), (weights_in, weights), (forces_in, forces)]
        )
    ]
    for move in moves:
        move.start()
    for move in moves:
        move.wait()
    tile = ids.shape[1]
    width = 128
    high = ids[...] // width
    low = ids[...] - high * width
    rest = [high.astype(F32), low.astype(F32)]
    rest += [jnp.zeros_like(rest[0])] * (8 - COMPS - len(rest))
    for s in range(slabs):
        at = slice(s * tile, (s + 1) * tile)
        block = jnp.concatenate(
            [forces[:, at] * weights[s : s + 1]] + [part[s : s + 1] for part in rest], axis=0
        )
        for k in range(copies):
            message_out[s * copies + k] = block.astype(jnp.bfloat16)


def edges_kernel(velocity, courant, first_out, last_out):
    rows = velocity.shape[2]
    for n, field in enumerate((velocity, courant)):
        first_out[n * COMPS : (n + 1) * COMPS] = field[:, :, :DEPTH]
        last_out[n * COMPS : (n + 1) * COMPS] = field[:, :, rows - DEPTH :]


def setup_kernel(
    copies, group,
    message, old, block, value_out, solved_out, up_out, down_out, momentum_sum
):
    planes, wide, width = old.shape[1:]
    rows = wide - 2 * DEPTH
    height = rows * copies
    start = lax.axis_index("batch") * rows
    tile = message.shape[2]
    row_iota = lax.broadcasted_iota(jnp.int32, (planes * wide, tile), 0)
    column_iota = lax.broadcasted_iota(jnp.int32, (width, tile), 0)

    def deposit(step):
        row_hot, spread = [], []
        for k in range(group):
            part = message[step * group + k].astype(F32)
            cell_row = part[3:4].astype(jnp.int32)
            column = part[4:5].astype(jnp.int32)
            plane = jnp.zeros_like(cell_row)
            for p in range(1, planes):
                plane = plane + (cell_row >= p * height).astype(jnp.int32)
            away = cell_row - plane * height - start
            away = jnp.where(away < 0, away + height, away)
            spot = jnp.where(away < rows + DEPTH, away, away - height + wide)
            inside = (away < rows + DEPTH) | (away >= height - DEPTH)
            spot = jnp.where(inside, spot + plane * wide, -1)
            row_hot.append(jnp.where(row_iota == spot, 1.0, 0.0).astype(jnp.bfloat16))
            here = column_iota == column
            spread.append(
                jnp.concatenate(
                    [jnp.where(here, part[c : c + 1], 0.0) for c in range(COMPS)], axis=0
                ).astype(jnp.bfloat16)
            )
        return lax.dot_general(
            jnp.concatenate(row_hot, axis=1),
            jnp.concatenate(spread, axis=1),
            (((1,), (1,)), ((), ())),
            preferred_element_type=F32,
        )

    steps = message.shape[0] // group
    if steps <= 4:
        total = deposit(0)
        for step in range(1, steps):
            total = total + deposit(step)
        momentum_sum[...] = total
    else:
        momentum_sum[...] = jnp.zeros_like(momentum_sum)

        def one(step, carry):
            momentum_sum[...] += deposit(step)
            return carry

        lax.fori_loop(0, steps, one, 0)

    inverses, ratios, lower_planes = block_planes(block)
    even = lax.axis_index("batch") % 2 == 0
    for c in range(COMPS):
        values = []
        for k in range(planes):
            deposit_part = momentum_sum[k * wide : (k + 1) * wide, c * width : (c + 1) * width]
            value = old[c, k] + deposit_part
            value_out[c, k] = value
            values.append(value)
        finish_level(c, values, inverses, ratios, lower_planes, even, solved_out, up_out, down_out)


def block_planes(block):
    planes = block.shape[1]
    return tuple([block[n, k] for k in range(planes)] for n in range(3))


def finish_level(c, values, inverses, ratios, lower_planes, even, solved_out, up_out, down_out):
    solved = solve_block(values, inverses, ratios, lower_planes)
    for k, item in enumerate(solved):
        solved_out[c, k] = item
    up_out[c] = jnp.where(even, solved[-1], solved[0])
    down_out[c] = jnp.where(even, solved[0], solved[-1])


def prepare_kernel(
    slabs, copies, velocity, courant, after, before, old_out, side_out, block_out
):
    planes, rows, width = velocity.shape[1:]
    wide = rows + 2 * DEPTH
    slab, batch = lax.axis_index("slab"), lax.axis_index("batch")
    for c in range(COMPS):
        for k in range(planes):
            old_out[c, k] = jnp.concatenate([velocity[c, k], after[c, k], before[c, k]], axis=0)
    spots = lax.broadcasted_iota(jnp.int32, (wide, width), 0)
    lanes = lax.broadcasted_iota(jnp.int32, (wide, width), 1)
    lower_planes, upper_planes, inverses, ratios = [], [], [], []
    for k in range(planes):
        coefs = []
        for d in range(3):
            half = 0.5 * jnp.concatenate(
                [courant[d, k], after[COMPS + d, k], before[COMPS + d, k]], axis=0
            )
            coefs.append((diffusion_number - half, diffusion_number + half))
        upper_planes.append(coefs[0][0])
        lower_planes.append(coefs[0][1])
        at_top = (spots == rows - 1) & (batch == copies - 1)
        at_bottom = (spots == 0) & (batch == 0)
        side_out[0, k] = jnp.where(at_top, 0.0, coefs[1][0])
        side_out[1, k] = jnp.where(at_bottom, 0.0, coefs[1][1])
        side_out[2, k] = jnp.where(lanes == width - 1, 0.0, coefs[2][0])
        side_out[3, k] = jnp.where(lanes == 0, 0.0, coefs[2][1])
        if k == 0:
            pivot = jnp.full((wide, width), diagonal_value, F32)
        else:
            pivot = diagonal_value + lower_planes[k] * ratios[-1]
        inverses.append(1.0 / pivot)
        ratios.append(-upper_planes[k] * inverses[-1])
        block_out[0, k] = inverses[k]
        block_out[1, k] = ratios[k]
        block_out[2, k] = lower_planes[k]
    block_out[3, 0] = jnp.where(slab == 0, 0.0, lower_planes[0])
    block_out[3, 1] = jnp.where(slab == slabs - 1, 0.0, upper_planes[planes - 1])


def couple(solved, one_way, other_way, side, block):
    planes, wide, width = solved.shape[1:]
    even = lax.axis_index("batch") % 2 == 0
    result = []
    for c in range(COMPS):
        values = []
        for k in range(planes):
            here = solved[c, k]
            total = side[0, k] * pltpu.roll(here, wide - 1, 0)
            total = total + side[1, k] * pltpu.roll(here, 1, 0)
            total = total + side[2, k] * pltpu.roll(here, width - 1, 1)
            total = total + side[3, k] * pltpu.roll(here, 1, 1)
            if k == 0:
                total = total + block[3, 0] * jnp.where(even, one_way[c], other_way[c])
            if k == planes - 1:
                total = total + block[3, 1] * jnp.where(even, other_way[c], one_way[c])
            values.append(total)
        result.append(values)
    return result


def apply_kernel(
    solved, one_way, other_way, side, block, value_out, solved_out, up_out, down_out
):
    inverses, ratios, lower_planes = block_planes(block)
    even = lax.axis_index("batch") % 2 == 0
    for c, values in enumerate(couple(solved, one_way, other_way, side, block)):
        for k, item in enumerate(values):
            value_out[c, k] = item
        finish_level(c, values, inverses, ratios, lower_planes, even, solved_out, up_out, down_out)


def gram_kernel(*refs):
    solved, one_way, other_way, side, block = refs[:5]
    values = refs[5 : 5 + DEPTH]
    value_out, message_out = refs[5 + DEPTH :]
    planes, wide, width = solved.shape[1:]
    rows = wide - 2 * DEPTH
    sums = []
    for c, newest in enumerate(couple(solved, one_way, other_way, side, block)):
        for k in range(planes):
            value_out[c, k] = newest[k]
        totals = [None] * len(PAIRS)
        for k in range(planes):
            for r in range(0, rows, 8):
                pieces = [values[i][c, k, r : r + 8, :] for i in range(DEPTH)]
                pieces.append(newest[k][r : r + 8])
                halves = [split(piece) for piece in pieces]
                for n, (i, j) in enumerate(PAIRS):
                    p = pieces[i] * pieces[j]
                    e = product_error(p, halves[i], halves[j])
                    if totals[n] is None:
                        totals[n] = (p, e)
                    else:
                        s, t = two_sum(totals[n][0], p)
                        totals[n] = (s, totals[n][1] + (t + e))
        sums.append(totals)
    flat = [sums[c][n] for n in range(len(PAIRS)) for c in range(COMPS)]
    nothing = (jnp.zeros((8, width), F32),) * 2
    flat += [nothing] * (width // 2 - len(flat))
    rows_of = [sum_to_sublanes(flat[n : n + 8]) for n in range(0, len(flat), 8)]
    turned = [jnp.transpose(jnp.concatenate([x[p] for x in rows_of], axis=0)) for p in (0, 1)]
    total = tuple(x[:8] for x in turned)
    for r in range(8, width, 8):
        total = dd_add(total, tuple(x[r : r + 8] for x in turned))
    for shift in (4, 2, 1):
        total = dd_add(total, tuple(pltpu.roll(x, shift, 0) for x in total))
    row = jnp.concatenate([x[:1] for x in total], axis=1)
    message_out[...] = jnp.broadcast_to(row, message_out.shape)


def sum_to_sublanes(parts):
    sub = lax.broadcasted_iota(jnp.int32, parts[0][0].shape, 0)
    level = parts
    for shift in (4, 2, 1):
        keep = (sub & shift) == 0
        merged = []
        for a, b in zip(level[:shift], level[shift:]):
            stay = tuple(jnp.where(keep, x, y) for x, y in zip(a, b))
            swap = [jnp.where(keep, y, x) for x, y in zip(a, b)]
            moved = tuple(
                pltpu.roll(w, 4, 0)
                if shift == 4
                else jnp.where(keep, pltpu.roll(w, 8 - shift, 0), pltpu.roll(w, shift, 0))
                for w in swap
            )
            merged.append(dd_add(stay, moved))
        level = merged
    return level[0]


def finish_kernel(*refs):
    gathered = refs[0]
    values = refs[1 : 1 + BASIS]
    solved = refs[1 + BASIS : 1 + BASIS + DEPTH]
    solution_out, residual_out = refs[1 + BASIS + DEPTH :]
    planes, rows, _ = solution_out.shape[1:]
    count, lanes = gathered.shape
    total = None
    for r in range(0, count, 8):
        high = gathered[r : r + 8]
        item = (high, pltpu.roll(high, lanes // 2, 1))
        total = item if total is None else dd_add(total, item)
    for shift in (4, 2, 1):
        total = dd_add(total, tuple(pltpu.roll(x, shift, 0) for x in total))
    sub = lax.broadcasted_iota(jnp.int32, (8, lanes), 0)

    def entry(n):
        return tuple(pltpu.roll(x, (lanes - n * COMPS) % lanes, 1) for x in total)

    entries = {pair: entry(n) for n, pair in enumerate(PAIRS)}
    gram = []
    for i in range(BASIS):
        row = None
        for j in range(BASIS):
            item = entries[(min(i, j), max(i, j))]
            if row is None:
                row = item
            else:
                row = tuple(jnp.where(sub == j, x, y) for x, y in zip(item, row))
        gram.append(row)
    zero = jnp.zeros((8, lanes), F32)
    nothing = (zero, zero)
    one = (zero + 1.0, zero)

    def stack(poly):
        out = (zero, zero)
        for j, item in enumerate(poly):
            out = tuple(jnp.where(sub == j, x, y) for x, y in zip(item, out))
        return out

    def over_sublanes(x):
        for shift in (4, 2, 1):
            x = dd_add(x, tuple(pltpu.roll(y, shift, 0) for y in x))
        return x

    def gram_times(poly):
        out = None
        for i, item in enumerate(poly):
            term = dd_mul(item, gram[i])
            out = term if out is None else dd_add(out, term)
        return tuple(jnp.where(sub < BASIS, x, 0.0) for x in out)

    def operate(poly):
        out = list(poly) + [nothing]
        return [out[0]] + [dd_sub(out[i], out[i - 1]) for i in range(1, len(out))]

    def combine(first, factor, second):
        out = []
        for i in range(max(len(first), len(second))):
            item = first[i] if i < len(first) else nothing
            if i < len(second):
                item = dd_add(item, dd_mul(factor, second[i]))
            out.append(item)
        return out

    shadow = tuple(jnp.where(sub < BASIS, x, 0.0) for x in gram[0])

    residual = [one]
    direction = [one]
    answer = []
    rho = entries[(0, 0)]
    for iteration in range(ITERS):
        image = operate(direction)
        alpha = dd_div(rho, over_sublanes(dd_mul(shadow, stack(image))))
        middle = combine(residual, dd_neg(alpha), image)
        turned = operate(middle)
        weighted = gram_times(turned)
        cross = over_sublanes(dd_mul(weighted, stack(middle)))
        square = over_sublanes(dd_mul(weighted, stack(turned)))
        omega = dd_div(cross, square)
        answer = combine(answer, alpha, direction)
        answer = combine(answer, omega, middle)
        residual = combine(middle, dd_neg(omega), turned)
        if iteration + 1 < ITERS:
            rho_next = over_sublanes(dd_mul(shadow, stack(residual)))
            factor = dd_mul(dd_div(rho_next, rho), dd_div(alpha, omega))
            direction = combine(direction, dd_neg(omega), image)
            direction = combine(residual, factor, direction)
            rho = rho_next
    for c in range(COMPS):
        answer_at = [item[0][:, c : c + 1] for item in answer]
        residual_at = [item[0][:, c : c + 1] for item in residual]
        for k in range(planes):
            for r in range(0, rows, 8):
                out = answer_at[0] * solved[0][c, k, r : r + 8, :]
                for i in range(1, DEPTH):
                    out = out + answer_at[i] * solved[i][c, k, r : r + 8, :]
                solution_out[c, k, r : r + 8, :] = out
                out = residual_at[0] * values[0][c, k, r : r + 8, :]
                for i in range(1, BASIS):
                    out = out + residual_at[i] * values[i][c, k, r : r + 8, :]
                residual_out[c, k, r : r + 8, :] = out


def ring(array, axis, step):
    count = lax.axis_size(axis)
    return lax.ppermute(array, axis, [(i, (i + step) % count) for i in range(count)])


def race(array, step):
    slabs, copies = lax.axis_size("slab"), lax.axis_size("batch")
    pairs = []
    for s in range(slabs):
        for b in range(copies):
            t = s + 1 if b % 2 == 0 else s - 1
            target = t * copies + b if 0 <= t < slabs else s * copies + (b ^ 1)
            pairs.append((s * copies + b, target))
    if step < 0:
        pairs = [(t, s) for s, t in pairs]
    return lax.ppermute(array, ("slab", "batch"), sorted(pairs))


def local(velocity_old, courant, cell_ids, forces, weights):
    planes, rows, width = velocity_old.shape[1:]
    slabs, copies = lax.axis_size("slab"), lax.axis_size("batch")
    everyone = ("slab", "batch")
    wide = rows + 2 * DEPTH
    height = rows * copies
    tile = cell_ids.shape[0] // slabs
    assert rows % 8 == 0 and width == 128 and copies % 2 == 0
    assert planes * height <= 256 and 2 * DEPTH <= height - rows
    field = jax.ShapeDtypeStruct((COMPS, planes, wide, width), F32)
    face = jax.ShapeDtypeStruct((COMPS, wide, width), F32)
    quad = jax.ShapeDtypeStruct((4, planes, wide, width), F32)
    edge = jax.ShapeDtypeStruct((2 * COMPS, planes, DEPTH, width), F32)
    own = jax.ShapeDtypeStruct(velocity_old.shape, F32)

    def call(kernel, out_shape, in_specs, mib, scratch=()):
        return pl.pallas_call(
            kernel,
            out_shape=out_shape,
            in_specs=in_specs,
            out_specs=[VMEM] * len(out_shape),
            scratch_shapes=list(scratch),
            compiler_params=pltpu.CompilerParams(vmem_limit_bytes=mib << 20),
        )

    def pack(*refs):
        pack_kernel(slabs, copies, *refs)

    (message,) = call(
        pack,
        (jax.ShapeDtypeStruct((slabs * copies, 8, tile), jnp.bfloat16),),
        [ANY] * 3,
        60,
        [
            pltpu.VMEM((slabs, tile), jnp.int32),
            pltpu.VMEM(forces.shape, F32),
            pltpu.VMEM((slabs, tile), F32),
            pltpu.SemaphoreType.DMA((3,)),
        ],
    )(cell_ids.reshape(slabs, tile), forces, weights.reshape(slabs, tile))
    received = lax.all_to_all(message, everyone, 0, 0, tiled=True)
    first, last = call(edges_kernel, (edge, edge), [VMEM] * 2, 2)(velocity_old, courant)
    after = ring(first, "batch", -1)
    before = ring(last, "batch", 1)

    def prepare(*refs):
        prepare_kernel(slabs, copies, *refs)

    old, side, block = call(
        prepare, (field, quad, quad), [VMEM] * 4, 4
    )(velocity_old, courant, after, before)

    def setup(*refs):
        setup_kernel(copies, 8, *refs)

    value, solved, up, down = call(
        setup,
        (field, field, face, face),
        [VMEM] * 3,
        12,
        [pltpu.VMEM((planes * wide, COMPS * width), F32)],
    )(received, old, block)

    values, solves = [value], [solved]
    for step in range(1, DEPTH + 1):
        known = (solved, race(up, 1), race(down, -1), side, block)
        if step < DEPTH:
            value, solved, up, down = call(
                apply_kernel, (field, field, face, face), [VMEM] * 5, 2
            )(*known)
            solves.append(solved)
        else:
            value, message = call(
                gram_kernel,
                (field, jax.ShapeDtypeStruct((slabs * copies, width), F32)),
                [VMEM] * (5 + DEPTH),
                4,
            )(*known, *values)
        values.append(value)
    gathered = lax.all_to_all(message, everyone, 0, 0, tiled=True)
    return call(
        finish_kernel, (own, own), [VMEM] * (1 + BASIS + DEPTH), 4
    )(gathered, *values, *solves)


def solution(mesh):
    placed = (
        P(None, "slab", "batch", None),
        P(None, "slab", "batch", None),
        P(("slab", "batch")),
        P(None, ("slab", "batch")),
        P(("slab", "batch")),
    )
    return jax.shard_map(
        local,
        mesh=mesh,
        in_specs=placed,
        out_specs=(P(None, "slab", "batch", None), P(None, "slab", "batch", None)),
        check_vma=False,
    )
```

```python
import jax
import jax.numpy as jnp
from jax import lax
from jax.experimental import pallas as pl
from jax.experimental.pallas import tpu as pltpu
from jax.sharding import PartitionSpec as P


ITERS = 2
DEPTH = 2 * ITERS
COMPS = 3
BASIS = DEPTH + 1
PAIRS = [(i, j) for i in range(BASIS) for j in range(i, BASIS)]

diffusion_number = 1.0
diagonal_value = 7.0

VMEM = pl.BlockSpec(memory_space=pltpu.VMEM)
ANY = pl.BlockSpec(memory_space=pl.ANY)
F32 = jnp.float32


def two_sum(a, b):
    s = a + b
    bb = s - a
    return s, (a - (s - bb)) + (b - bb)


def quick_two_sum(a, b):
    s = a + b
    return s, b - (s - a)


def split(a):
    t = a * 4097.0
    high = t - (t - a)
    return high, a - high


def product_error(p, a, b):
    ah, al = a
    bh, bl = b
    return ((ah * bh - p) + ah * bl + al * bh) + al * bl


def dd_add(a, b):
    s, e = two_sum(a[0], b[0])
    return quick_two_sum(s, e + (a[1] + b[1]))


def dd_neg(a):
    return -a[0], -a[1]


def dd_sub(a, b):
    return dd_add(a, dd_neg(b))


def dd_mul(a, b):
    p = a[0] * b[0]
    e = product_error(p, split(a[0]), split(b[0]))
    return quick_two_sum(p, e + (a[0] * b[1] + a[1] * b[0]))


def dd_div(a, b):
    inverse = 1.0 / b[0]
    q1 = a[0] * inverse
    zero = jnp.zeros_like(q1)
    r = dd_sub(a, dd_mul((q1, zero), b))
    q2 = r[0] * inverse
    r = dd_sub(r, dd_mul((q2, zero), b))
    q3 = r[0] * inverse
    s, e = quick_two_sum(q1, q2)
    return quick_two_sum(s, e + q3)


def solve_block(values, inverses, ratios, lower_planes):
    forward = []
    for k, current in enumerate(values):
        if k > 0:
            current = current + lower_planes[k] * forward[-1]
        forward.append(current * inverses[k])
    result = [forward[-1]]
    for k in range(len(values) - 2, -1, -1):
        result.insert(0, forward[k] - ratios[k] * result[0])
    return result


def pack_kernel(slabs, copies, ids_in, forces_in, weights_in, message_out, ids, forces, weights, arrived):
    moves = [
        pltpu.make_async_copy(source, target, arrived.at[n])
        for n, (source, target) in enumerate(
            [(ids_in, ids), (weights_in, weights), (forces_in, forces)]
        )
    ]
    for move in moves:
        move.start()
    for move in moves:
        move.wait()
    tile = ids.shape[1]
    width = 128
    high = ids[...] // width
    low = ids[...] - high * width
    rest = [high.astype(F32), low.astype(F32)]
    rest += [jnp.zeros_like(rest[0])] * (8 - COMPS - len(rest))
    for s in range(slabs):
        at = slice(s * tile, (s + 1) * tile)
        block = jnp.concatenate(
            [forces[:, at] * weights[s : s + 1]] + [part[s : s + 1] for part in rest], axis=0
        )
        for k in range(copies):
            message_out[s * copies + k] = block.astype(jnp.bfloat16)


def edges_kernel(velocity, courant, first_out, last_out):
    rows = velocity.shape[2]
    for n, field in enumerate((velocity, courant)):
        first_out[n * COMPS : (n + 1) * COMPS] = field[:, :, :DEPTH]
        last_out[n * COMPS : (n + 1) * COMPS] = field[:, :, rows - DEPTH :]


def deposit_kernel(rows, copies, group, message, momentum_sum):
    wide = rows + 2 * DEPTH
    height = rows * copies
    planes = momentum_sum.shape[0] // wide
    width = momentum_sum.shape[1] // COMPS
    start = lax.axis_index("batch") * rows
    tile = message.shape[2]
    row_iota = lax.broadcasted_iota(jnp.int32, (planes * wide, tile), 0)
    column_iota = lax.broadcasted_iota(jnp.int32, (width, tile), 0)

    def deposit(step):
        row_hot, spread = [], []
        for k in range(group):
            part = message[step * group + k].astype(F32)
            cell_row = part[3:4].astype(jnp.int32)
            column = part[4:5].astype(jnp.int32)
            plane = jnp.zeros_like(cell_row)
            for p in range(1, planes):
                plane = plane + (cell_row >= p * height).astype(jnp.int32)
            away = cell_row - plane * height - start
            away = jnp.where(away < 0, away + height, away)
            spot = jnp.where(away < rows + DEPTH, away, away - height + wide)
            inside = (away < rows + DEPTH) | (away >= height - DEPTH)
            spot = jnp.where(inside, spot + plane * wide, -1)
            row_hot.append(jnp.where(row_iota == spot, 1.0, 0.0).astype(jnp.bfloat16))
            here = column_iota == column
            spread.append(
                jnp.concatenate(
                    [jnp.where(here, part[c : c + 1], 0.0) for c in range(COMPS)], axis=0
                ).astype(jnp.bfloat16)
            )
        return lax.dot_general(
            jnp.concatenate(row_hot, axis=1),
            jnp.concatenate(spread, axis=1),
            (((1,), (1,)), ((), ())),
            preferred_element_type=F32,
        )

    steps = message.shape[0] // group
    if steps <= 4:
        total = deposit(0)
        for step in range(1, steps):
            total = total + deposit(step)
        momentum_sum[...] = total
    else:
        momentum_sum[...] = jnp.zeros_like(momentum_sum)

        def one(step, carry):
            momentum_sum[...] += deposit(step)
            return carry

        lax.fori_loop(0, steps, one, 0)


def fill_coefficients(courant, slab, slabs, batch, copies, rows, side, block):
    planes, wide, width = side.shape[1:]
    spots = lax.broadcasted_iota(jnp.int32, (wide, width), 0)
    lanes = lax.broadcasted_iota(jnp.int32, (wide, width), 1)
    at_top = (spots == rows - 1) & (batch == copies - 1)
    at_bottom = (spots == 0) & (batch == 0)
    ratio = None
    for k in range(planes):
        upper, lower = [], []
        for d in range(3):
            half = 0.5 * courant(d, k)
            upper.append(diffusion_number - half)
            lower.append(diffusion_number + half)
        side[0, k] = jnp.where(at_top, 0.0, upper[1])
        side[1, k] = jnp.where(at_bottom, 0.0, lower[1])
        side[2, k] = jnp.where(lanes == width - 1, 0.0, upper[2])
        side[3, k] = jnp.where(lanes == 0, 0.0, lower[2])
        if k == 0:
            pivot = jnp.full((wide, width), diagonal_value, F32)
            block[3, 0] = jnp.where(slab <= 0, 0.0, lower[0])
        else:
            pivot = diagonal_value + lower[0] * ratio
        if k == planes - 1:
            block[3, 1] = jnp.where(slab >= slabs - 1, 0.0, upper[0])
        inverse = 1.0 / pivot
        ratio = -upper[0] * inverse
        block[0, k] = inverse
        block[1, k] = ratio
        block[2, k] = lower[0]


def solve(values, block):
    planes = len(values)
    return solve_block(values, *([block[n, k] for k in range(planes)] for n in range(3)))


def couple(planes_here, below, above, side, block):
    planes = len(planes_here)
    wide, width = planes_here[0].shape
    values = []
    for k, here in enumerate(planes_here):
        total = side[0, k] * pltpu.roll(here, wide - 1, 0)
        total = total + side[1, k] * pltpu.roll(here, 1, 0)
        total = total + side[2, k] * pltpu.roll(here, width - 1, 1)
        total = total + side[3, k] * pltpu.roll(here, 1, 1)
        if k == 0:
            total = total + block[3, 0] * below
        if k == planes - 1:
            total = total + block[3, 1] * above
        values.append(total)
    return values


def store_solved(c, solved, even, near_out, up_out, down_out):
    for k, item in enumerate(solved):
        near_out[c, k] = item
    up_out[c] = jnp.where(even, solved[-1], solved[0])
    down_out[c] = jnp.where(even, solved[0], solved[-1])


def setup_kernel(
    slabs, copies, velocity, courant, after, before, momentum_sum,
    value_out, near_out, up_out, down_out, side, block,
):
    planes, rows, width = velocity.shape[1:]
    wide = rows + 2 * DEPTH
    batch = lax.axis_index("batch")
    for d in range(3):
        for k in range(planes):
            near_out[COMPS + d, k] = jnp.concatenate(
                [courant[d, k], after[COMPS + d, k], before[COMPS + d, k]], axis=0
            )
    fill_coefficients(
        lambda d, k: near_out[COMPS + d, k],
        lax.axis_index("slab"), slabs, batch, copies, rows, side, block,
    )
    for c in range(COMPS):
        values = []
        for k in range(planes):
            old = jnp.concatenate([velocity[c, k], after[c, k], before[c, k]], axis=0)
            value = old + momentum_sum[k * wide : (k + 1) * wide, c * width : (c + 1) * width]
            value_out[c, k] = value
            values.append(value)
        store_solved(c, solve(values, block), batch % 2 == 0, near_out, up_out, down_out)


def two_levels(slabs, copies, solved, origin, arrived, sides, blocks):
    near, far, first = arrived[:2], arrived[2:4], arrived[4:]
    planes, wide = solved.shape[1:3]
    rows = wide - 2 * DEPTH
    slab, batch = lax.axis_index("slab"), lax.axis_index("batch")
    even = batch % 2 == 0

    def low(pair, at):
        return jnp.where(even, pair[0][at], pair[1][at])

    def high(pair, at):
        return jnp.where(even, pair[1][at], pair[0][at])

    for n, courant in enumerate(
        (
            lambda d, k: low(first, (COMPS + d, k)),
            lambda d, k: origin[COMPS + d, k],
            lambda d, k: high(first, (COMPS + d, k)),
        )
    ):
        fill_coefficients(
            courant, slab + n - 1, slabs, batch, copies, rows, sides.at[n], blocks.at[n]
        )
    for c in range(COMPS):
        here = [solved[c, k] for k in range(planes)]
        under = [low(near, (c, k)) for k in range(planes)]
        over = [high(near, (c, k)) for k in range(planes)]
        face_under = solve(
            couple(under, low(far, c), here[0], sides.at[0], blocks.at[0]), blocks.at[0]
        )[-1]
        face_over = solve(
            couple(over, here[-1], high(far, c), sides.at[2], blocks.at[2]), blocks.at[2]
        )[0]
        one = couple(here, under[-1], over[0], sides.at[1], blocks.at[1])
        one_solved = solve(one, blocks.at[1])
        two = couple(one_solved, face_under, face_over, sides.at[1], blocks.at[1])
        yield c, one, one_solved, two


def advance_kernel(
    slabs, copies, solved, origin, near1, near2, far1, far2, first1, first2,
    value_out, solved_out, second_out, near_out, up_out, down_out, sides, blocks,
):
    even = lax.axis_index("batch") % 2 == 0
    arrived = (near1, near2, far1, far2, first1, first2)
    for c, one, one_solved, two in two_levels(
        slabs, copies, solved, origin, arrived, sides, blocks
    ):
        for k in range(len(one)):
            value_out[c, k] = one[k]
            solved_out[c, k] = one_solved[k]
            second_out[c, k] = two[k]
        store_solved(c, solve(two, blocks.at[1]), even, near_out, up_out, down_out)


def gram_kernel(slabs, copies, *refs):
    solved, origin = refs[:2]
    arrived = refs[2:8]
    values = refs[8 : 7 + DEPTH]
    value_out, solved_out, second_out, message_out, sides, blocks = refs[7 + DEPTH :]
    planes, wide, width = solved.shape[1:]
    rows = wide - 2 * DEPTH
    sums = []
    for c, one, one_solved, two in two_levels(
        slabs, copies, solved, origin, arrived, sides, blocks
    ):
        for k in range(planes):
            value_out[c, k] = one[k]
            solved_out[c, k] = one_solved[k]
            second_out[c, k] = two[k]
        totals = [None] * len(PAIRS)
        for k in range(planes):
            for r in range(0, rows, 8):
                pieces = [value[c, k, r : r + 8, :] for value in values]
                pieces += [one[k][r : r + 8], two[k][r : r + 8]]
                halves = [split(piece) for piece in pieces]
                for n, (i, j) in enumerate(PAIRS):
                    p = pieces[i] * pieces[j]
                    e = product_error(p, halves[i], halves[j])
                    if totals[n] is None:
                        totals[n] = (p, e)
                    else:
                        s, t = two_sum(totals[n][0], p)
                        totals[n] = (s, totals[n][1] + (t + e))
        sums.append(totals)
    flat = [sums[c][n] for n in range(len(PAIRS)) for c in range(COMPS)]
    nothing = (jnp.zeros((8, width), F32),) * 2
    flat += [nothing] * (width // 2 - len(flat))
    rows_of = [sum_to_sublanes(flat[n : n + 8]) for n in range(0, len(flat), 8)]
    turned = [jnp.transpose(jnp.concatenate([x[p] for x in rows_of], axis=0)) for p in (0, 1)]
    total = tuple(x[:8] for x in turned)
    for r in range(8, width, 8):
        total = dd_add(total, tuple(x[r : r + 8] for x in turned))
    for shift in (4, 2, 1):
        total = dd_add(total, tuple(pltpu.roll(x, shift, 0) for x in total))
    row = jnp.concatenate([x[:1] for x in total], axis=1)
    message_out[...] = jnp.broadcast_to(row, message_out.shape)


def sum_to_sublanes(parts):
    sub = lax.broadcasted_iota(jnp.int32, parts[0][0].shape, 0)
    level = parts
    for shift in (4, 2, 1):
        keep = (sub & shift) == 0
        merged = []
        for a, b in zip(level[:shift], level[shift:]):
            stay = tuple(jnp.where(keep, x, y) for x, y in zip(a, b))
            swap = [jnp.where(keep, y, x) for x, y in zip(a, b)]
            moved = tuple(
                pltpu.roll(w, 4, 0)
                if shift == 4
                else jnp.where(keep, pltpu.roll(w, 8 - shift, 0), pltpu.roll(w, shift, 0))
                for w in swap
            )
            merged.append(dd_add(stay, moved))
        level = merged
    return level[0]


def finish_kernel(*refs):
    gathered = refs[0]
    values = refs[1 : 1 + BASIS]
    solved = refs[1 + BASIS : 1 + BASIS + DEPTH]
    solution_out, residual_out = refs[1 + BASIS + DEPTH :]
    planes, rows, _ = solution_out.shape[1:]
    count, lanes = gathered.shape
    total = None
    for r in range(0, count, 8):
        high = gathered[r : r + 8]
        item = (high, pltpu.roll(high, lanes // 2, 1))
        total = item if total is None else dd_add(total, item)
    for shift in (4, 2, 1):
        total = dd_add(total, tuple(pltpu.roll(x, shift, 0) for x in total))
    sub = lax.broadcasted_iota(jnp.int32, (8, lanes), 0)

    def entry(n):
        return tuple(pltpu.roll(x, (lanes - n * COMPS) % lanes, 1) for x in total)

    entries = {pair: entry(n) for n, pair in enumerate(PAIRS)}
    gram = []
    for i in range(BASIS):
        row = None
        for j in range(BASIS):
            item = entries[(min(i, j), max(i, j))]
            if row is None:
                row = item
            else:
                row = tuple(jnp.where(sub == j, x, y) for x, y in zip(item, row))
        gram.append(row)
    zero = jnp.zeros((8, lanes), F32)
    nothing = (zero, zero)
    one = (zero + 1.0, zero)

    def stack(poly):
        out = (zero, zero)
        for j, item in enumerate(poly):
            out = tuple(jnp.where(sub == j, x, y) for x, y in zip(item, out))
        return out

    def over_sublanes(x):
        for shift in (4, 2, 1):
            x = dd_add(x, tuple(pltpu.roll(y, shift, 0) for y in x))
        return x

    def gram_times(poly):
        out = None
        for i, item in enumerate(poly):
            term = dd_mul(item, gram[i])
            out = term if out is None else dd_add(out, term)
        return tuple(jnp.where(sub < BASIS, x, 0.0) for x in out)

    def operate(poly):
        out = list(poly) + [nothing]
        return [out[0]] + [dd_sub(out[i], out[i - 1]) for i in range(1, len(out))]

    def combine(first, factor, second):
        out = []
        for i in range(max(len(first), len(second))):
            item = first[i] if i < len(first) else nothing
            if i < len(second):
                item = dd_add(item, dd_mul(factor, second[i]))
            out.append(item)
        return out

    shadow = tuple(jnp.where(sub < BASIS, x, 0.0) for x in gram[0])

    residual = [one]
    direction = [one]
    answer = []
    rho = entries[(0, 0)]
    for iteration in range(ITERS):
        image = operate(direction)
        alpha = dd_div(rho, over_sublanes(dd_mul(shadow, stack(image))))
        middle = combine(residual, dd_neg(alpha), image)
        turned = operate(middle)
        weighted = gram_times(turned)
        cross = over_sublanes(dd_mul(weighted, stack(middle)))
        square = over_sublanes(dd_mul(weighted, stack(turned)))
        omega = dd_div(cross, square)
        answer = combine(answer, alpha, direction)
        answer = combine(answer, omega, middle)
        residual = combine(middle, dd_neg(omega), turned)
        if iteration + 1 < ITERS:
            rho_next = over_sublanes(dd_mul(shadow, stack(residual)))
            factor = dd_mul(dd_div(rho_next, rho), dd_div(alpha, omega))
            direction = combine(direction, dd_neg(omega), image)
            direction = combine(residual, factor, direction)
            rho = rho_next
    for c in range(COMPS):
        answer_at = [item[0][:, c : c + 1] for item in answer]
        residual_at = [item[0][:, c : c + 1] for item in residual]
        for k in range(planes):
            for r in range(0, rows, 8):
                out = answer_at[0] * solved[0][c, k, r : r + 8, :]
                for i in range(1, DEPTH):
                    out = out + answer_at[i] * solved[i][c, k, r : r + 8, :]
                solution_out[c, k, r : r + 8, :] = out
                out = residual_at[0] * values[0][c, k, r : r + 8, :]
                for i in range(1, BASIS):
                    out = out + residual_at[i] * values[i][c, k, r : r + 8, :]
                residual_out[c, k, r : r + 8, :] = out


def ring(array, axis, step):
    count = lax.axis_size(axis)
    return lax.ppermute(array, axis, [(i, (i + step) % count) for i in range(count)])


def race(array, step):
    slabs, copies = lax.axis_size("slab"), lax.axis_size("batch")
    pairs = []
    for s in range(slabs):
        for b in range(copies):
            t = s + abs(step) if b % 2 == 0 else s - abs(step)
            target = t * copies + b if 0 <= t < slabs else s * copies + (b ^ 1)
            pairs.append((s * copies + b, target))
    if step < 0:
        pairs = [(t, s) for s, t in pairs]
    return lax.ppermute(array, ("slab", "batch"), sorted(pairs))


def local(velocity_old, courant, cell_ids, forces, weights):
    planes, rows, width = velocity_old.shape[1:]
    slabs, copies = lax.axis_size("slab"), lax.axis_size("batch")
    everyone = ("slab", "batch")
    wide = rows + 2 * DEPTH
    height = rows * copies
    tile = cell_ids.shape[0] // slabs
    assert rows % 8 == 0 and width == 128 and copies % 2 == 0
    assert planes * height <= 256 and 2 * DEPTH <= height - rows
    field = jax.ShapeDtypeStruct((COMPS, planes, wide, width), F32)
    face = jax.ShapeDtypeStruct((COMPS, wide, width), F32)
    quad = (4, planes, wide, width)
    edge = jax.ShapeDtypeStruct((2 * COMPS, planes, DEPTH, width), F32)
    own = jax.ShapeDtypeStruct(velocity_old.shape, F32)

    def call(kernel, out_shape, in_specs, mib, scratch=()):
        return pl.pallas_call(
            kernel,
            out_shape=out_shape,
            in_specs=in_specs,
            out_specs=[VMEM] * len(out_shape),
            scratch_shapes=list(scratch),
            compiler_params=pltpu.CompilerParams(vmem_limit_bytes=mib << 20),
        )

    def pack(*refs):
        pack_kernel(slabs, copies, *refs)

    (message,) = call(
        pack,
        (jax.ShapeDtypeStruct((slabs * copies, 8, tile), jnp.bfloat16),),
        [ANY] * 3,
        8,
        [
            pltpu.VMEM((slabs, tile), jnp.int32),
            pltpu.VMEM(forces.shape, F32),
            pltpu.VMEM((slabs, tile), F32),
            pltpu.SemaphoreType.DMA((3,)),
        ],
    )(
        *(
            pltpu.with_memory_space_constraint(x, pltpu.HBM)
            for x in (cell_ids.reshape(slabs, tile), forces, weights.reshape(slabs, tile))
        )
    )
    received = lax.all_to_all(message, everyone, 0, 0, tiled=True)
    first, last = call(edges_kernel, (edge, edge), [VMEM] * 2, 2)(velocity_old, courant)
    after = ring(first, "batch", -1)
    before = ring(last, "batch", 1)

    def deposit(*refs):
        deposit_kernel(rows, copies, 8, *refs)

    (deposited,) = call(
        deposit,
        (jax.ShapeDtypeStruct((planes * wide, COMPS * width), F32),),
        [VMEM],
        12,
    )(received)

    def placed(kernel):
        return lambda *refs: kernel(slabs, copies, *refs)

    near_shape = jax.ShapeDtypeStruct((2 * COMPS, planes, wide, width), F32)
    value, near, up, down = call(
        placed(setup_kernel),
        (field, near_shape, face, face),
        [VMEM] * 5,
        2,
        [pltpu.VMEM(quad, F32)] * 2,
    )(velocity_old, courant, after, before, deposited)

    values, solves = [value], [near]
    origin, first_near = near, None
    for iteration in range(ITERS):
        nears = [race(near, 1), race(near, -1)]
        first_near = first_near or nears
        known = (near, origin, *nears, race(up, 2), race(down, -2), *first_near)
        coefficients = [pltpu.VMEM((3, *quad), F32)] * 2
        if iteration + 1 < ITERS:
            value, solved, second, near, up, down = call(
                placed(advance_kernel),
                (field, field, field, field, face, face),
                [VMEM] * 8,
                4,
                coefficients,
            )(*known)
            solves += [solved, near]
        else:
            value, solved, second, message = call(
                placed(gram_kernel),
                (
                    field,
                    field,
                    field,
                    jax.ShapeDtypeStruct((slabs * copies, width), F32),
                ),
                [VMEM] * (8 + len(values)),
                4,
                coefficients,
            )(*known, *values)
            solves += [solved]
        values += [value, second]
    gathered = lax.all_to_all(message, everyone, 0, 0, tiled=True)
    return call(
        finish_kernel, (own, own), [VMEM] * (1 + BASIS + DEPTH), 4
    )(gathered, *values, *solves)


def solution(mesh):
    placed = (
        P(None, "slab", "batch", None),
        P(None, "slab", "batch", None),
        P(("slab", "batch")),
        P(None, ("slab", "batch")),
        P(("slab", "batch")),
    )
    return jax.shard_map(
        local,
        mesh=mesh,
        in_specs=placed,
        out_specs=(P(None, "slab", "batch", None), P(None, "slab", "batch", None)),
        check_vma=False,
    )
```

```python
import jax
import jax.numpy as jnp
from jax import lax
from jax.experimental import pallas as pl
from jax.experimental.pallas import tpu as pltpu
from jax.sharding import PartitionSpec as P


ITERS = 2
DEPTH = 2 * ITERS
COMPS = 3
BASIS = DEPTH + 1
EARLY = DEPTH - 1
PAIRS = sorted(((i, j) for j in range(BASIS) for i in range(j + 1)), key=lambda p: p[1] >= EARLY)
EARLY_PAIRS = [p for p in PAIRS if p[1] < EARLY]
LATE_PAIRS = [p for p in PAIRS if p[1] >= EARLY]
EARLY_ROWS = -(-len(EARLY_PAIRS) * COMPS // 8) * 8

diffusion_number = 1.0
diagonal_value = 7.0

VMEM = pl.BlockSpec(memory_space=pltpu.VMEM)
ANY = pl.BlockSpec(memory_space=pl.ANY)
F32 = jnp.float32


def two_sum(a, b):
    s = a + b
    bb = s - a
    return s, (a - (s - bb)) + (b - bb)


def quick_two_sum(a, b):
    s = a + b
    return s, b - (s - a)


def split(a):
    t = a * 4097.0
    high = t - (t - a)
    return high, a - high


def product_error(p, a, b):
    ah, al = a
    bh, bl = b
    return ((ah * bh - p) + ah * bl + al * bh) + al * bl


def dd_add(a, b):
    if isinstance(b, int):
        a, b = b, a
    if isinstance(a, int):
        if isinstance(b, int):
            return a + b
        if a == 0:
            return b
        a = (jnp.full_like(b[0], a), jnp.zeros_like(b[0]))
    s, e = two_sum(a[0], b[0])
    return quick_two_sum(s, e + (a[1] + b[1]))


def dd_neg(a):
    return -a if isinstance(a, int) else (-a[0], -a[1])


def dd_sub(a, b):
    return dd_add(a, dd_neg(b))


def dd_mul(a, b):
    if isinstance(b, int):
        a, b = b, a
    if isinstance(a, int):
        if isinstance(b, int):
            return a * b
        return {0: 0, 1: b, -1: dd_neg(b)}[a]
    p = a[0] * b[0]
    e = product_error(p, split(a[0]), split(b[0]))
    return quick_two_sum(p, e + (a[0] * b[1] + a[1] * b[0]))


def dd_div(a, b):
    inverse = 1.0 / b[0]
    q1 = a[0] * inverse
    zero = jnp.zeros_like(q1)
    r = dd_sub(a, dd_mul((q1, zero), b))
    q2 = r[0] * inverse
    return quick_two_sum(q1, q2)


def solve_block(values, inverses, ratios, lower_planes):
    forward = []
    for k, current in enumerate(values):
        if k > 0:
            current = current + lower_planes[k] * forward[-1]
        forward.append(current * inverses[k])
    result = [forward[-1]]
    for k in range(len(values) - 2, -1, -1):
        result.insert(0, forward[k] - ratios[k] * result[0])
    return result


def pack_kernel(slabs, copies, ids_in, forces_in, weights_in, message_out, ids, forces, weights, arrived):
    moves = [
        pltpu.make_async_copy(source, target, arrived.at[n])
        for n, (source, target) in enumerate(
            [(ids_in, ids), (weights_in, weights), (forces_in, forces)]
        )
    ]
    for move in moves:
        move.start()
    for move in moves:
        move.wait()
    tile = ids.shape[1]
    width = 128
    high = ids[...] // width
    low = ids[...] - high * width
    rest = [high.astype(F32), low.astype(F32)]
    rest += [jnp.zeros_like(rest[0])] * (8 - COMPS - len(rest))
    for s in range(slabs):
        at = slice(s * tile, (s + 1) * tile)
        block = jnp.concatenate(
            [forces[:, at] * weights[s : s + 1]] + [part[s : s + 1] for part in rest], axis=0
        )
        for k in range(copies):
            message_out[s * copies + k] = block.astype(jnp.bfloat16)


def edges_kernel(velocity, courant, first_out, last_out):
    rows = velocity.shape[2]
    for n, field in enumerate((velocity, courant)):
        first_out[n * COMPS : (n + 1) * COMPS] = field[:, :, :DEPTH]
        last_out[n * COMPS : (n + 1) * COMPS] = field[:, :, rows - DEPTH :]


def deposit_kernel(rows, copies, group, message, momentum_sum):
    wide = rows + 2 * DEPTH
    height = rows * copies
    planes = momentum_sum.shape[0] // (COMPS * wide)
    width = momentum_sum.shape[1]
    start = lax.axis_index("batch") * rows
    tile = message.shape[2]
    narrow = jnp.bfloat16
    count = lax.broadcasted_iota(jnp.int32, (16, tile), 0).astype(F32)
    counts = [(count + 16.0 * g).astype(narrow) for g in range(width // 16)]
    nothing = jnp.zeros((16, tile), narrow)
    one = jnp.ones((16, tile), narrow)

    def over_sixteen(row):
        return jnp.broadcast_to(row, (16, tile)).astype(narrow)

    def deposit(step):
        row_values, column_hot = [], []
        for k in range(group):
            part = message[step * group + k].astype(F32)
            cell_row = part[3:4].astype(jnp.int32)
            plane = jnp.zeros_like(cell_row)
            for p in range(1, planes):
                plane = plane + (cell_row >= p * height).astype(jnp.int32)
            away = cell_row - plane * height - start
            away = jnp.where(away < 0, away + height, away)
            spot = jnp.where(away < rows + DEPTH, away, away - height + wide)
            inside = (away < rows + DEPTH) | (away >= height - DEPTH)
            spot = over_sixteen(jnp.where(inside, spot + plane * wide, -1).astype(F32))
            column = over_sixteen(part[4:5])
            values = [over_sixteen(part[c : c + 1]) for c in range(COMPS)]
            here = [counts[g] == spot for g in range(planes * wide // 16)]
            row_values.append(
                jnp.concatenate(
                    [jnp.where(at, value, nothing) for value in values for at in here], axis=0
                )
            )
            column_hot.append(
                jnp.concatenate([jnp.where(n == column, one, nothing) for n in counts], axis=0)
            )
        return lax.dot_general(
            jnp.concatenate(row_values, axis=1),
            jnp.concatenate(column_hot, axis=1),
            (((1,), (1,)), ((), ())),
            preferred_element_type=F32,
        )

    steps = message.shape[0] // group
    if steps <= 4:
        total = deposit(0)
        for step in range(1, steps):
            total = total + deposit(step)
        momentum_sum[...] = total
    else:
        momentum_sum[...] = jnp.zeros_like(momentum_sum)

        def add_step(step, carry):
            momentum_sum[...] += deposit(step)
            return carry

        lax.fori_loop(0, steps, add_step, 0)


def fill_coefficients(courant, slab, slabs, batch, copies, rows, side, block):
    planes, wide, width = side.shape[1:]
    spots = lax.broadcasted_iota(jnp.int32, (wide, width), 0)
    lanes = lax.broadcasted_iota(jnp.int32, (wide, width), 1)
    at_top = (spots == rows - 1) & (batch == copies - 1)
    at_bottom = (spots == 0) & (batch == 0)
    ratio = None
    for k in range(planes):
        upper, lower = [], []
        for d in range(3):
            half = 0.5 * courant(d, k)
            upper.append(diffusion_number - half)
            lower.append(diffusion_number + half)
        side[0, k] = jnp.where(at_top, 0.0, upper[1])
        side[1, k] = jnp.where(at_bottom, 0.0, lower[1])
        side[2, k] = jnp.where(lanes == width - 1, 0.0, upper[2])
        side[3, k] = jnp.where(lanes == 0, 0.0, lower[2])
        if k == 0:
            pivot = jnp.full((wide, width), diagonal_value, F32)
            block[3, 0] = jnp.where(slab <= 0, 0.0, lower[0])
        else:
            pivot = diagonal_value + lower[0] * ratio
        if k == planes - 1:
            block[3, 1] = jnp.where(slab >= slabs - 1, 0.0, upper[0])
        inverse = 1.0 / pivot
        ratio = -upper[0] * inverse
        block[0, k] = inverse
        block[1, k] = ratio
        block[2, k] = lower[0]


def solve(values, block):
    planes = len(values)
    return solve_block(values, *([block[n, k] for k in range(planes)] for n in range(3)))


def in_plane(planes_here, side):
    wide, width = planes_here[0].shape
    values = []
    for k, here in enumerate(planes_here):
        total = side[0, k] * pltpu.roll(here, wide - 1, 0)
        total = total + side[1, k] * pltpu.roll(here, 1, 0)
        total = total + side[2, k] * pltpu.roll(here, width - 1, 1)
        total = total + side[3, k] * pltpu.roll(here, 1, 1)
        values.append(total)
    return values


def add_outside(values, below, above, block):
    values = list(values)
    values[0] = values[0] + block[3, 0] * below
    values[-1] = values[-1] + block[3, 1] * above
    return values


def store_messages(c, solved, nearby, rows, even, near_out, far_out):
    wide = solved[0].shape[0]
    one, other = (jnp.where(even, x[-1], x[0]) for x in (solved, nearby))
    at, beside = (jnp.where(even, x[0], x[-1]) for x in (solved, nearby))
    for n, (face, part) in enumerate(((one, other), (at, beside))):
        near_out[n][c * wide : (c + 1) * wide] = face
        start = COMPS * wide + c * rows
        near_out[n][start : start + rows] = part[:rows]
        far_out[n][c] = face[: far_out[n].shape[1]]


def setup_kernel(
    slabs, copies, velocity, courant, after, before, momentum_sum,
    value_out, solved_out, inner_out, near1, near2, far1, far2, side, block, wide_courant,
):
    planes, rows, width = velocity.shape[1:]
    wide = rows + 2 * DEPTH
    batch = lax.axis_index("batch")
    even = batch % 2 == 0
    for d in range(3):
        for k in range(planes):
            wide_courant[d, k] = jnp.concatenate(
                [courant[d, k], after[COMPS + d, k], before[COMPS + d, k]], axis=0
            )
    fill_coefficients(
        lambda d, k: wide_courant[d, k],
        lax.axis_index("slab"), slabs, batch, copies, rows, side, block,
    )
    zero = jnp.zeros((wide, width), F32)
    from_below = solve([block[3, 0]] + [zero] * (planes - 1), block)
    from_above = solve([zero] * (planes - 1) + [block[3, 1]], block)
    start = 2 * COMPS * wide
    for n, part in enumerate((from_below, from_above)):
        at = slice(start + n * wide, start + (n + 1) * wide)
        near1[at] = jnp.where(even, part[-1], part[0])
        near2[at] = jnp.where(even, part[0], part[-1])
    for c in range(COMPS):
        values = []
        for k in range(planes):
            old = jnp.concatenate([velocity[c, k], after[c, k], before[c, k]], axis=0)
            at = (c * planes + k) * wide
            value = old + momentum_sum[at : at + wide]
            value_out[c, k] = value
            values.append(value)
        solved = solve(values, block)
        inner = in_plane(solved, side)
        for k in range(planes):
            solved_out[c, k] = solved[k]
            inner_out[c, k] = inner[k]
        store_messages(c, solved, solve(inner, block), wide, even, (near1, near2), (far1, far2))


def two_levels(solved, inner, near1, near2, far1, far2, first1, first2, side, block):
    planes, wide = solved.shape[1:3]
    rows = far1.shape[1]
    even = lax.axis_index("batch") % 2 == 0

    def low(one, other):
        return jnp.where(even, one, other)

    def high(one, other):
        return jnp.where(even, other, one)

    def part(pick, start, count):
        at = slice(start, start + count)
        return pick(near1[at], near2[at])

    def response(pick, n):
        at = slice((2 * COMPS + n) * wide, (2 * COMPS + n) * wide + rows)
        return pick(first1[at], first2[at])

    low_below, low_above = response(low, 0), response(low, 1)
    high_below, high_above = response(high, 0), response(high, 1)
    pad = jnp.zeros((wide - rows, solved.shape[3]), F32)

    def widen(x):
        return x if rows == wide else jnp.concatenate([x, pad], axis=0)

    for c in range(COMPS):
        own = COMPS * wide + c * rows
        below, above = part(low, c * wide, wide), part(high, c * wide, wide)
        one = add_outside([inner[c, k] for k in range(planes)], below, above, block)
        one_solved = solve(one, block)
        next_below = (
            part(low, own, rows)
            + low_above * solved[c, 0][:rows]
            + low_below * low(far1[c], far2[c])
        )
        next_above = (
            part(high, own, rows)
            + high_below * solved[c, planes - 1][:rows]
            + high_above * high(far1[c], far2[c])
        )
        two = add_outside(
            in_plane(one_solved, side), widen(next_below), widen(next_above), block
        )
        yield c, one, one_solved, two


def advance_kernel(
    solved, inner, near1, near2, far1, far2, first1, first2, side, block,
    value_out, solved_out, second_out, last_out, inner_out, to1, to2, beyond1, beyond2,
):
    even = lax.axis_index("batch") % 2 == 0
    for c, one, one_solved, two in two_levels(
        solved, inner, near1, near2, far1, far2, first1, first2, side, block
    ):
        two_solved = solve(two, block)
        within = in_plane(two_solved, side)
        for k in range(len(one)):
            value_out[c, k] = one[k]
            solved_out[c, k] = one_solved[k]
            second_out[c, k] = two[k]
            last_out[c, k] = two_solved[k]
            inner_out[c, k] = within[k]
        rows = beyond1.shape[1]
        store_messages(c, two_solved, solve(within, block), rows, even, (to1, to2), (beyond1, beyond2))


def gram_sums(pieces, pairs, totals):
    halves = [split(piece) for piece in pieces]
    for n, (i, j) in enumerate(pairs):
        p = pieces[i] * pieces[j]
        e = product_error(p, halves[i], halves[j])
        if totals[n] is None:
            totals[n] = (p, e)
        else:
            s, t = two_sum(totals[n][0], p)
            totals[n] = (s, totals[n][1] + (t + e))


def stack_sums(sums, count):
    flat = [sums[c][n] for n in range(len(sums[0])) for c in range(COMPS)]
    flat += [(jnp.zeros_like(flat[0][0]),) * 2] * (count - len(flat))
    rows_of = [sum_to_sublanes(flat[n : n + 8]) for n in range(0, count, 8)]
    return [jnp.concatenate([x[p] for x in rows_of], axis=0) for p in (0, 1)]


def early_kernel(rows, *refs):
    values, (high_out, low_out) = refs[:EARLY], refs[EARLY:]
    sums = []
    for c in range(COMPS):
        totals = [None] * len(EARLY_PAIRS)
        for k in range(values[0].shape[1]):
            for r in range(0, rows, 8):
                gram_sums([v[c, k, r : r + 8, :] for v in values], EARLY_PAIRS, totals)
        sums.append(totals)
    high_out[...], low_out[...] = stack_sums(sums, EARLY_ROWS)


def gram_kernel(*refs):
    known = refs[:10]
    values = refs[10 : 10 + EARLY]
    early = refs[10 + EARLY : 12 + EARLY]
    value_out, solved_out, second_out, message_out = refs[12 + EARLY :]
    planes, wide, width = value_out.shape[1:]
    rows = wide - 2 * DEPTH
    sums = []
    for c, one, one_solved, two in two_levels(*known):
        totals = [None] * len(LATE_PAIRS)
        for k in range(planes):
            value_out[c, k] = one[k]
            solved_out[c, k] = one_solved[k]
            second_out[c, k] = two[k]
            for r in range(0, rows, 8):
                pieces = [value[c, k, r : r + 8, :] for value in values]
                gram_sums(pieces + [one[k][r : r + 8], two[k][r : r + 8]], LATE_PAIRS, totals)
        sums.append(totals)
    late = stack_sums(sums, width // 2 - EARLY_ROWS)
    turned = [jnp.transpose(jnp.concatenate([e[...], x], axis=0)) for e, x in zip(early, late)]
    total = tuple(x[:8] for x in turned)
    for r in range(8, width, 8):
        total = dd_add(total, tuple(x[r : r + 8] for x in turned))
    for shift in (4, 2, 1):
        total = dd_add(total, tuple(pltpu.roll(x, shift, 0) for x in total))
    row = jnp.concatenate([x[:1] for x in total], axis=1)
    message_out[...] = jnp.broadcast_to(row, message_out.shape)


def sum_to_sublanes(parts):
    sub = lax.broadcasted_iota(jnp.int32, parts[0][0].shape, 0)
    level = parts
    for shift in (4, 2, 1):
        keep = (sub & shift) == 0
        merged = []
        for a, b in zip(level[:shift], level[shift:]):
            stay = tuple(jnp.where(keep, x, y) for x, y in zip(a, b))
            swap = [jnp.where(keep, y, x) for x, y in zip(a, b)]
            moved = tuple(
                pltpu.roll(w, 4, 0)
                if shift == 4
                else jnp.where(keep, pltpu.roll(w, 8 - shift, 0), pltpu.roll(w, shift, 0))
                for w in swap
            )
            merged.append(dd_add(stay, moved))
        level = merged
    return level[0]


def finish_kernel(*refs):
    gathered = refs[0]
    values = refs[1 : 1 + BASIS]
    solved = refs[1 + BASIS : 1 + BASIS + DEPTH]
    solution_out, residual_out, solution_here, residual_here, sent = refs[1 + BASIS + DEPTH :]
    planes, rows, _ = solution_here.shape[1:]
    count, lanes = gathered.shape
    total = None
    for r in range(0, count, 8):
        high = gathered[r : r + 8]
        item = (high, pltpu.roll(high, lanes // 2, 1))
        total = item if total is None else dd_add(total, item)
    for shift in (4, 2, 1):
        total = dd_add(total, tuple(pltpu.roll(x, shift, 0) for x in total))
    sub = lax.broadcasted_iota(jnp.int32, (8, lanes), 0)

    def entry(n):
        start = n * COMPS
        if n >= len(EARLY_PAIRS):
            start = EARLY_ROWS + (n - len(EARLY_PAIRS)) * COMPS
        return tuple(pltpu.roll(x, (lanes - start) % lanes, 1) for x in total)

    entries = {pair: entry(n) for n, pair in enumerate(PAIRS)}
    gram = []
    for i in range(BASIS):
        row = None
        for j in range(BASIS):
            item = entries[(min(i, j), max(i, j))]
            if row is None:
                row = item
            else:
                row = tuple(jnp.where(sub == j, x, y) for x, y in zip(item, row))
        gram.append(row)
    zero = jnp.zeros((8, lanes), F32)

    def stack(poly):
        out = (zero, zero)
        for j, item in enumerate(poly):
            if isinstance(item, int):
                item = (zero + item, zero)
            out = tuple(jnp.where(sub == j, x, y) for x, y in zip(item, out))
        return out

    def over_sublanes(x):
        for shift in (4, 2, 1):
            x = dd_add(x, tuple(pltpu.roll(y, shift, 0) for y in x))
        return x

    def gram_times(poly):
        out = 0
        for i, item in enumerate(poly):
            out = dd_add(out, dd_mul(item, gram[i]))
        return tuple(jnp.where(sub < BASIS, x, 0.0) for x in out)

    def with_shadow(poly):
        terms = [dd_mul(item, entries[(0, i)]) for i, item in enumerate(poly)]
        while len(terms) > 1:
            pairs = [dd_add(*terms[i : i + 2]) for i in range(0, len(terms) - 1, 2)]
            terms = pairs + terms[len(pairs) * 2 :]
        return terms[0]

    def operate(poly):
        out = list(poly) + [0]
        return [out[0]] + [dd_sub(out[i], out[i - 1]) for i in range(1, len(out))]

    def combine(first, factor, second):
        out = []
        for i in range(max(len(first), len(second))):
            item = first[i] if i < len(first) else 0
            if i < len(second):
                item = dd_add(item, dd_mul(factor, second[i]))
            out.append(item)
        return out

    residual = [1]
    direction = [1]
    answer = []
    rho = entries[(0, 0)]
    for iteration in range(ITERS):
        image = operate(direction)
        alpha = dd_div(rho, with_shadow(image))
        middle = combine(residual, dd_neg(alpha), image)
        turned = operate(middle)
        weighted = gram_times(turned)
        cross = over_sublanes(dd_mul(weighted, stack(middle)))
        square = over_sublanes(dd_mul(weighted, stack(turned)))
        omega = dd_div(cross, square)
        answer = combine(answer, alpha, direction)
        answer = combine(answer, omega, middle)
        residual = combine(middle, dd_neg(omega), turned)
        if iteration + 1 < ITERS:
            rho_next = with_shadow(residual)
            factor = dd_mul(dd_div(rho_next, rho), dd_div(alpha, omega))
            direction = combine(direction, dd_neg(omega), image)
            direction = combine(residual, factor, direction)
            rho = rho_next
    moves = []
    for c in range(COMPS):
        for n, (poly, basis, here, out) in enumerate(
            (
                (answer, solved, solution_here, solution_out),
                (residual, values, residual_here, residual_out),
            )
        ):
            scales = [item[0][:, c : c + 1] for item in poly]
            for k in range(planes):
                for r in range(0, rows, 8):
                    total = scales[0] * basis[0][c, k, r : r + 8, :]
                    for i in range(1, len(scales)):
                        total = total + scales[i] * basis[i][c, k, r : r + 8, :]
                    here[c, k, r : r + 8, :] = total
            moves.append(pltpu.make_async_copy(here.at[c], out.at[c], sent.at[n * COMPS + c]))
            moves[-1].start()
    for move in moves:
        move.wait()


def ring(array, axis, step):
    count = lax.axis_size(axis)
    return lax.ppermute(array, axis, [(i, (i + step) % count) for i in range(count)])


def race(array, step):
    slabs, copies = lax.axis_size("slab"), lax.axis_size("batch")
    pairs = []
    for s in range(slabs):
        for b in range(copies):
            t = s + abs(step) if b % 2 == 0 else s - abs(step)
            target = t * copies + b if 0 <= t < slabs else s * copies + (b ^ 1)
            pairs.append((s * copies + b, target))
    if step < 0:
        pairs = [(t, s) for s, t in pairs]
    return lax.ppermute(array, ("slab", "batch"), sorted(pairs))


def local(velocity_old, courant, cell_ids, forces, weights):
    planes, rows, width = velocity_old.shape[1:]
    slabs, copies = lax.axis_size("slab"), lax.axis_size("batch")
    everyone = ("slab", "batch")
    wide = rows + 2 * DEPTH
    height = rows * copies
    tile = cell_ids.shape[0] // slabs
    assert rows % 8 == 0 and width == 128 and copies % 2 == 0
    assert planes * height <= 256 and 2 * DEPTH <= height - rows
    field = jax.ShapeDtypeStruct((COMPS, planes, wide, width), F32)
    quad = jax.ShapeDtypeStruct((4, planes, wide, width), F32)
    edge = jax.ShapeDtypeStruct((2 * COMPS, planes, DEPTH, width), F32)
    own = jax.ShapeDtypeStruct(velocity_old.shape, F32)

    def call(kernel, out_shape, in_specs, mib, scratch=(), out_space=VMEM, cost=None):
        if cost is not None:
            cost = pl.CostEstimate(flops=cost, bytes_accessed=0, transcendentals=0)
        return pl.pallas_call(
            kernel,
            out_shape=out_shape,
            in_specs=in_specs,
            out_specs=[out_space] * len(out_shape),
            cost_estimate=cost,
            scratch_shapes=list(scratch),
            compiler_params=pltpu.CompilerParams(vmem_limit_bytes=mib << 20),
        )

    def pack(*refs):
        pack_kernel(slabs, copies, *refs)

    (message,) = call(
        pack,
        (jax.ShapeDtypeStruct((slabs * copies, 8, tile), jnp.bfloat16),),
        [ANY] * 3,
        8,
        [
            pltpu.VMEM((slabs, tile), jnp.int32),
            pltpu.VMEM(forces.shape, F32),
            pltpu.VMEM((slabs, tile), F32),
            pltpu.SemaphoreType.DMA((3,)),
        ],
    )(
        *(
            pltpu.with_memory_space_constraint(x, pltpu.HBM)
            for x in (cell_ids.reshape(slabs, tile), forces, weights.reshape(slabs, tile))
        )
    )
    received = lax.all_to_all(message, everyone, 0, 0, tiled=True)
    first, last = call(edges_kernel, (edge, edge), [VMEM] * 2, 2)(velocity_old, courant)
    after = ring(first, "batch", -1)
    before = ring(last, "batch", 1)

    def deposit(*refs):
        deposit_kernel(rows, copies, 8, *refs)

    (deposited,) = call(
        deposit, (jax.ShapeDtypeStruct((COMPS * planes * wide, width), F32),), [VMEM], 12
    )(received)

    def setup(*refs):
        setup_kernel(slabs, copies, *refs)

    def flat(count):
        return jax.ShapeDtypeStruct((count, width), F32)

    def faces(count):
        return jax.ShapeDtypeStruct((COMPS, count, width), F32)

    value, solved, inner, *sent, side, block = call(
        setup,
        (field,) * 3 + (flat((2 * COMPS + 2) * wide),) * 2 + (faces(wide),) * 2 + (quad,) * 2,
        [VMEM] * 5,
        2,
        [pltpu.VMEM((3, planes, wide, width), F32)],
    )(velocity_old, courant, after, before, deposited)

    values, solves = [value], [solved]
    first = None
    for iteration in range(ITERS):
        near = [race(sent[0], 1), race(sent[1], -1)]
        far = [race(sent[2], 2), race(sent[3], -2)]
        first = first or near
        known = (solved, inner, *near, *far, *first, side, block)
        if iteration + 1 < ITERS:
            reach = wide if iteration + 2 < ITERS else rows
            value, one_solved, second, solved, inner, *sent = call(
                advance_kernel,
                (field,) * 5 + (flat(COMPS * (wide + reach)),) * 2 + (faces(reach),) * 2,
                [VMEM] * 10,
                2,
            )(*known)
            solves += [one_solved, solved]
        else:
            def early(*refs):
                early_kernel(rows, *refs)

            sums = call(early, (flat(EARLY_ROWS),) * 2, [VMEM] * EARLY, 2, cost=4000000)(*values)
            value, one_solved, second, message = call(
                gram_kernel, (field,) * 3 + (flat(slabs * copies),), [VMEM] * (12 + EARLY), 4
            )(*known, *values, *sums)
            solves += [one_solved]
        values += [value, second]
    gathered = lax.all_to_all(message, everyone, 0, 0, tiled=True)
    return call(
        finish_kernel,
        (own, own),
        [VMEM] * (1 + BASIS + DEPTH),
        4,
        [pltpu.VMEM(own.shape, F32)] * 2 + [pltpu.SemaphoreType.DMA((2 * COMPS,))],
        ANY,
    )(gathered, *values, *solves)


def solution(mesh):
    placed = (
        P(None, "slab", "batch", None),
        P(None, "slab", "batch", None),
        P(("slab", "batch")),
        P(None, ("slab", "batch")),
        P(("slab", "batch")),
    )
    return jax.shard_map(
        local,
        mesh=mesh,
        in_specs=placed,
        out_specs=(P(None, "slab", "batch", None), P(None, "slab", "batch", None)),
        check_vma=False,
    )
```

```python
import jax
import jax.numpy as jnp
from jax import lax
from jax.experimental import pallas as pl
from jax.experimental.pallas import tpu as pltpu
from jax.sharding import PartitionSpec as P


ITERS = 2
DEPTH = 2 * ITERS
COMPS = 3
BASIS = DEPTH + 1
EARLY = DEPTH - 1
PAIRS = sorted(((i, j) for j in range(BASIS) for i in range(j + 1)), key=lambda p: p[1] >= EARLY)
EARLY_PAIRS = [p for p in PAIRS if p[1] < EARLY]
LATE_PAIRS = [p for p in PAIRS if p[1] >= EARLY]
EARLY_ROWS = -(-len(EARLY_PAIRS) * COMPS // 8) * 8

diffusion_number = 1.0
diagonal_value = 7.0

VMEM = pl.BlockSpec(memory_space=pltpu.VMEM)
ANY = pl.BlockSpec(memory_space=pl.ANY)
F32 = jnp.float32


def two_sum(a, b):
    s = a + b
    bb = s - a
    return s, (a - (s - bb)) + (b - bb)


def quick_two_sum(a, b):
    s = a + b
    return s, b - (s - a)


def split(a):
    t = a * 4097.0
    high = t - (t - a)
    return high, a - high


def product_error(p, a, b):
    ah, al = a
    bh, bl = b
    return ((ah * bh - p) + ah * bl + al * bh) + al * bl


def dd_add(a, b):
    if isinstance(b, int):
        a, b = b, a
    if isinstance(a, int):
        if isinstance(b, int):
            return a + b
        if a == 0:
            return b
        a = (jnp.full_like(b[0], a), jnp.zeros_like(b[0]))
    s, e = two_sum(a[0], b[0])
    return quick_two_sum(s, e + (a[1] + b[1]))


def dd_neg(a):
    return -a if isinstance(a, int) else (-a[0], -a[1])


def dd_sub(a, b):
    return dd_add(a, dd_neg(b))


def dd_mul(a, b):
    if isinstance(b, int):
        a, b = b, a
    if isinstance(a, int):
        if isinstance(b, int):
            return a * b
        return {0: 0, 1: b, -1: dd_neg(b)}[a]
    p = a[0] * b[0]
    e = product_error(p, split(a[0]), split(b[0]))
    return quick_two_sum(p, e + (a[0] * b[1] + a[1] * b[0]))


def dd_scale(factor, b):
    if isinstance(b, int):
        return 0 if b == 0 else (b * factor, jnp.zeros_like(factor))
    p = factor * b[0]
    e = product_error(p, split(factor), split(b[0]))
    return quick_two_sum(p, e + factor * b[1])


def solve_block(values, inverses, ratios, lower_planes):
    forward = []
    for k, current in enumerate(values):
        if k > 0:
            current = current + lower_planes[k] * forward[-1]
        forward.append(current * inverses[k])
    result = [forward[-1]]
    for k in range(len(values) - 2, -1, -1):
        result.insert(0, forward[k] - ratios[k] * result[0])
    return result


def pack_kernel(slabs, copies, ids_in, forces_in, weights_in, message_out, ids, forces, weights, arrived):
    moves = [
        pltpu.make_async_copy(source, target, arrived.at[n])
        for n, (source, target) in enumerate(
            [(ids_in, ids), (weights_in, weights), (forces_in, forces)]
        )
    ]
    for move in moves:
        move.start()
    for move in moves:
        move.wait()
    tile = ids.shape[1]
    width = 128
    high = ids[...] // width
    low = ids[...] - high * width
    rest = [high.astype(F32), low.astype(F32)]
    rest += [jnp.zeros_like(rest[0])] * (8 - COMPS - len(rest))
    for s in range(slabs):
        at = slice(s * tile, (s + 1) * tile)
        block = jnp.concatenate(
            [forces[:, at] * weights[s : s + 1]] + [part[s : s + 1] for part in rest], axis=0
        )
        for k in range(copies):
            message_out[s * copies + k] = block.astype(jnp.bfloat16)


def edges_kernel(velocity, courant, first_out, last_out):
    rows = velocity.shape[2]
    for n, field in enumerate((velocity, courant)):
        first_out[n * COMPS : (n + 1) * COMPS] = field[:, :, :DEPTH]
        last_out[n * COMPS : (n + 1) * COMPS] = field[:, :, rows - DEPTH :]


def deposit_kernel(rows, copies, group, message, momentum_sum):
    wide = rows + 2 * DEPTH
    height = rows * copies
    planes = momentum_sum.shape[0] // (COMPS * wide)
    width = momentum_sum.shape[1]
    start = lax.axis_index("batch") * rows
    tile = message.shape[2]
    narrow = jnp.bfloat16
    count = lax.broadcasted_iota(jnp.int32, (16, tile), 0).astype(F32)
    counts = [(count + 16.0 * g).astype(narrow) for g in range(width // 16)]
    nothing = jnp.zeros((16, tile), narrow)
    one = jnp.ones((16, tile), narrow)

    def over_sixteen(row):
        return jnp.broadcast_to(row, (16, tile)).astype(narrow)

    def deposit(step):
        row_values, column_hot = [], []
        for k in range(group):
            part = message[step * group + k].astype(F32)
            cell_row = part[3:4].astype(jnp.int32)
            plane = jnp.zeros_like(cell_row)
            for p in range(1, planes):
                plane = plane + (cell_row >= p * height).astype(jnp.int32)
            away = cell_row - plane * height - start
            away = jnp.where(away < 0, away + height, away)
            spot = jnp.where(away < rows + DEPTH, away, away - height + wide)
            inside = (away < rows + DEPTH) | (away >= height - DEPTH)
            spot = over_sixteen(jnp.where(inside, spot + plane * wide, -1).astype(F32))
            column = over_sixteen(part[4:5])
            values = [over_sixteen(part[c : c + 1]) for c in range(COMPS)]
            here = [counts[g] == spot for g in range(planes * wide // 16)]
            row_values.append(
                jnp.concatenate(
                    [jnp.where(at, value, nothing) for value in values for at in here], axis=0
                )
            )
            column_hot.append(
                jnp.concatenate([jnp.where(n == column, one, nothing) for n in counts], axis=0)
            )
        return lax.dot_general(
            jnp.concatenate(row_values, axis=1),
            jnp.concatenate(column_hot, axis=1),
            (((1,), (1,)), ((), ())),
            preferred_element_type=F32,
        )

    steps = message.shape[0] // group
    if steps <= 4:
        total = deposit(0)
        for step in range(1, steps):
            total = total + deposit(step)
        momentum_sum[...] = total
    else:
        momentum_sum[...] = jnp.zeros_like(momentum_sum)

        def add_step(step, carry):
            momentum_sum[...] += deposit(step)
            return carry

        lax.fori_loop(0, steps, add_step, 0)


def fill_coefficients(courant, slab, slabs, batch, copies, rows, side, block):
    planes, wide, width = side.shape[1:]
    spots = lax.broadcasted_iota(jnp.int32, (wide, width), 0)
    lanes = lax.broadcasted_iota(jnp.int32, (wide, width), 1)
    at_top = (spots == rows - 1) & (batch == copies - 1)
    at_bottom = (spots == 0) & (batch == 0)
    ratio = None
    for k in range(planes):
        upper, lower = [], []
        for d in range(3):
            half = 0.5 * courant(d, k)
            upper.append(diffusion_number - half)
            lower.append(diffusion_number + half)
        side[0, k] = jnp.where(at_top, 0.0, upper[1])
        side[1, k] = jnp.where(at_bottom, 0.0, lower[1])
        side[2, k] = jnp.where(lanes == width - 1, 0.0, upper[2])
        side[3, k] = jnp.where(lanes == 0, 0.0, lower[2])
        if k == 0:
            pivot = jnp.full((wide, width), diagonal_value, F32)
            block[3, 0] = jnp.where(slab <= 0, 0.0, lower[0])
        else:
            pivot = diagonal_value + lower[0] * ratio
        if k == planes - 1:
            block[3, 1] = jnp.where(slab >= slabs - 1, 0.0, upper[0])
        inverse = 1.0 / pivot
        ratio = -upper[0] * inverse
        block[0, k] = inverse
        block[1, k] = ratio
        block[2, k] = lower[0]


def solve(values, block):
    planes = len(values)
    return solve_block(values, *([block[n, k] for k in range(planes)] for n in range(3)))


def in_plane(planes_here, side):
    wide, width = planes_here[0].shape
    values = []
    for k, here in enumerate(planes_here):
        total = side[0, k] * pltpu.roll(here, wide - 1, 0)
        total = total + side[1, k] * pltpu.roll(here, 1, 0)
        total = total + side[2, k] * pltpu.roll(here, width - 1, 1)
        total = total + side[3, k] * pltpu.roll(here, 1, 1)
        values.append(total)
    return values


def add_outside(values, below, above, block):
    values = list(values)
    values[0] = values[0] + block[3, 0] * below
    values[-1] = values[-1] + block[3, 1] * above
    return values


def store_messages(c, solved, nearby, rows, even, near_out, far_out):
    wide = solved[0].shape[0]
    one, other = (jnp.where(even, x[-1], x[0]) for x in (solved, nearby))
    at, beside = (jnp.where(even, x[0], x[-1]) for x in (solved, nearby))
    for n, (face, part) in enumerate(((one, other), (at, beside))):
        near_out[n][c * wide : (c + 1) * wide] = face
        start = COMPS * wide + c * rows
        near_out[n][start : start + rows] = part[:rows]
        far_out[n][c] = face[: far_out[n].shape[1]]


def setup_kernel(
    slabs, copies, velocity, courant, after, before, momentum_sum,
    value_out, solved_out, inner_out, near1, near2, far1, far2, side, block, wide_courant,
):
    planes, rows, width = velocity.shape[1:]
    wide = rows + 2 * DEPTH
    batch = lax.axis_index("batch")
    even = batch % 2 == 0
    for d in range(3):
        for k in range(planes):
            wide_courant[d, k] = jnp.concatenate(
                [courant[d, k], after[COMPS + d, k], before[COMPS + d, k]], axis=0
            )
    fill_coefficients(
        lambda d, k: wide_courant[d, k],
        lax.axis_index("slab"), slabs, batch, copies, rows, side, block,
    )
    zero = jnp.zeros((wide, width), F32)
    from_below = solve([block[3, 0]] + [zero] * (planes - 1), block)
    from_above = solve([zero] * (planes - 1) + [block[3, 1]], block)
    start = 2 * COMPS * wide
    for n, part in enumerate((from_below, from_above)):
        at = slice(start + n * wide, start + (n + 1) * wide)
        near1[at] = jnp.where(even, part[-1], part[0])
        near2[at] = jnp.where(even, part[0], part[-1])
    for c in range(COMPS):
        values = []
        for k in range(planes):
            old = jnp.concatenate([velocity[c, k], after[c, k], before[c, k]], axis=0)
            at = (c * planes + k) * wide
            value = old + momentum_sum[at : at + wide]
            value_out[c, k] = value
            values.append(value)
        solved = solve(values, block)
        inner = in_plane(solved, side)
        for k in range(planes):
            solved_out[c, k] = solved[k]
            inner_out[c, k] = inner[k]
        store_messages(c, solved, solve(inner, block), wide, even, (near1, near2), (far1, far2))


def two_levels(solved, inner, near1, near2, far1, far2, first1, first2, side, block):
    planes, wide = solved.shape[1:3]
    rows = far1.shape[1]
    even = lax.axis_index("batch") % 2 == 0

    def low(one, other):
        return jnp.where(even, one, other)

    def high(one, other):
        return jnp.where(even, other, one)

    def part(pick, start, count):
        at = slice(start, start + count)
        return pick(near1[at], near2[at])

    def response(pick, n):
        at = slice((2 * COMPS + n) * wide, (2 * COMPS + n) * wide + rows)
        return pick(first1[at], first2[at])

    low_below, low_above = response(low, 0), response(low, 1)
    high_below, high_above = response(high, 0), response(high, 1)
    pad = jnp.zeros((wide - rows, solved.shape[3]), F32)

    def widen(x):
        return x if rows == wide else jnp.concatenate([x, pad], axis=0)

    for c in range(COMPS):
        own = COMPS * wide + c * rows
        below, above = part(low, c * wide, wide), part(high, c * wide, wide)
        one = add_outside([inner[c, k] for k in range(planes)], below, above, block)
        one_solved = solve(one, block)
        next_below = (
            part(low, own, rows)
            + low_above * solved[c, 0][:rows]
            + low_below * low(far1[c], far2[c])
        )
        next_above = (
            part(high, own, rows)
            + high_below * solved[c, planes - 1][:rows]
            + high_above * high(far1[c], far2[c])
        )
        two = add_outside(
            in_plane(one_solved, side), widen(next_below), widen(next_above), block
        )
        yield c, one, one_solved, two


def advance_kernel(
    solved, inner, near1, near2, far1, far2, first1, first2, side, block,
    value_out, solved_out, second_out, last_out, inner_out, to1, to2, beyond1, beyond2,
):
    even = lax.axis_index("batch") % 2 == 0
    for c, one, one_solved, two in two_levels(
        solved, inner, near1, near2, far1, far2, first1, first2, side, block
    ):
        two_solved = solve(two, block)
        within = in_plane(two_solved, side)
        for k in range(len(one)):
            value_out[c, k] = one[k]
            solved_out[c, k] = one_solved[k]
            second_out[c, k] = two[k]
            last_out[c, k] = two_solved[k]
            inner_out[c, k] = within[k]
        rows = beyond1.shape[1]
        store_messages(c, two_solved, solve(within, block), rows, even, (to1, to2), (beyond1, beyond2))


def gram_sums(pieces, pairs, totals):
    halves = [split(piece) for piece in pieces]
    for n, (i, j) in enumerate(pairs):
        p = pieces[i] * pieces[j]
        e = product_error(p, halves[i], halves[j])
        if totals[n] is None:
            totals[n] = (p, e)
        else:
            s, t = two_sum(totals[n][0], p)
            totals[n] = (s, totals[n][1] + (t + e))


def stack_sums(sums, count):
    flat = [sums[c][n] for n in range(len(sums[0])) for c in range(COMPS)]
    flat += [(jnp.zeros_like(flat[0][0]),) * 2] * (count - len(flat))
    rows_of = [sum_to_sublanes(flat[n : n + 8]) for n in range(0, count, 8)]
    return [jnp.concatenate([x[p] for x in rows_of], axis=0) for p in (0, 1)]


def early_kernel(rows, *refs):
    values, (high_out, low_out) = refs[:EARLY], refs[EARLY:]
    sums = []
    for c in range(COMPS):
        totals = [None] * len(EARLY_PAIRS)
        for k in range(values[0].shape[1]):
            for r in range(0, rows, 8):
                gram_sums([v[c, k, r : r + 8, :] for v in values], EARLY_PAIRS, totals)
        sums.append(totals)
    high_out[...], low_out[...] = stack_sums(sums, EARLY_ROWS)


def gram_kernel(*refs):
    known = refs[:10]
    values = refs[10 : 10 + EARLY]
    early = refs[10 + EARLY : 12 + EARLY]
    value_out, solved_out, second_out, message_out = refs[12 + EARLY :]
    planes, wide, width = value_out.shape[1:]
    rows = wide - 2 * DEPTH
    sums = []
    for c, one, one_solved, two in two_levels(*known):
        totals = [None] * len(LATE_PAIRS)
        for k in range(planes):
            value_out[c, k] = one[k]
            solved_out[c, k] = one_solved[k]
            second_out[c, k] = two[k]
            for r in range(0, rows, 8):
                pieces = [value[c, k, r : r + 8, :] for value in values]
                gram_sums(pieces + [one[k][r : r + 8], two[k][r : r + 8]], LATE_PAIRS, totals)
        sums.append(totals)
    late = stack_sums(sums, width // 2 - EARLY_ROWS)
    turned = [jnp.transpose(jnp.concatenate([e[...], x], axis=0)) for e, x in zip(early, late)]
    total = tuple(x[:8] for x in turned)
    for r in range(8, width, 8):
        total = dd_add(total, tuple(x[r : r + 8] for x in turned))
    for shift in (4, 2, 1):
        total = dd_add(total, tuple(pltpu.roll(x, shift, 0) for x in total))
    row = jnp.concatenate([x[:1] for x in total], axis=1)
    message_out[...] = jnp.broadcast_to(row, message_out.shape)


def sum_to_sublanes(parts):
    sub = lax.broadcasted_iota(jnp.int32, parts[0][0].shape, 0)
    level = parts
    for shift in (4, 2, 1):
        keep = (sub & shift) == 0
        merged = []
        for a, b in zip(level[:shift], level[shift:]):
            stay = tuple(jnp.where(keep, x, y) for x, y in zip(a, b))
            swap = [jnp.where(keep, y, x) for x, y in zip(a, b)]
            moved = tuple(
                pltpu.roll(w, 4, 0)
                if shift == 4
                else jnp.where(keep, pltpu.roll(w, 8 - shift, 0), pltpu.roll(w, shift, 0))
                for w in swap
            )
            merged.append(dd_add(stay, moved))
        level = merged
    return level[0]


def finish_kernel(*refs):
    gathered = refs[0]
    values = refs[1 : 1 + BASIS]
    solved = refs[1 + BASIS : 1 + BASIS + DEPTH]
    solution_out, residual_out, solution_here, residual_here, sent = refs[1 + BASIS + DEPTH :]
    planes, rows, _ = solution_here.shape[1:]
    count, lanes = gathered.shape
    total = None
    for r in range(0, count, 8):
        high = gathered[r : r + 8]
        item = (high, pltpu.roll(high, lanes // 2, 1))
        total = item if total is None else dd_add(total, item)
    for shift in (4, 2, 1):
        total = dd_add(total, tuple(pltpu.roll(x, shift, 0) for x in total))
    sub = lax.broadcasted_iota(jnp.int32, (8, lanes), 0)

    def entry(n):
        start = n * COMPS
        if n >= len(EARLY_PAIRS):
            start = EARLY_ROWS + (n - len(EARLY_PAIRS)) * COMPS
        return tuple(pltpu.roll(x, (lanes - start) % lanes, 1) for x in total)

    entries = {pair: entry(n) for n, pair in enumerate(PAIRS)}
    gram = []
    for i in range(BASIS):
        row = None
        for j in range(BASIS):
            item = entries[(min(i, j), max(i, j))]
            if row is None:
                row = item
            else:
                row = tuple(jnp.where(sub == j, x, y) for x, y in zip(item, row))
        gram.append(row)
    zero = jnp.zeros((8, lanes), F32)

    def stack(poly):
        out = (zero, zero)
        for j, item in enumerate(poly):
            if isinstance(item, int):
                item = (zero + item, zero)
            out = tuple(jnp.where(sub == j, x, y) for x, y in zip(item, out))
        return out

    def over_sublanes(x):
        for shift in (4, 2, 1):
            x = dd_add(x, tuple(pltpu.roll(y, shift, 0) for y in x))
        return x

    def gram_times(poly):
        out = 0
        for i, item in enumerate(poly):
            out = dd_add(out, dd_mul(item, gram[i]))
        return tuple(jnp.where(sub < BASIS, x, 0.0) for x in out)

    def with_shadow(poly):
        terms = [dd_mul(item, entries[(0, i)]) for i, item in enumerate(poly)]
        while len(terms) > 1:
            pairs = [dd_add(*terms[i : i + 2]) for i in range(0, len(terms) - 1, 2)]
            terms = pairs + terms[len(pairs) * 2 :]
        return terms[0]

    def operate(poly):
        out = list(poly) + [0]
        return [out[0]] + [dd_sub(out[i], out[i - 1]) for i in range(1, len(out))]

    def combine(first, factor, second):
        out = []
        for i in range(max(len(first), len(second))):
            item = first[i] if i < len(first) else 0
            if i < len(second):
                item = dd_add(item, dd_scale(factor, second[i]))
            out.append(item)
        return out

    def rounded(poly):
        return [zero + item if isinstance(item, int) else item[0] for item in poly]

    residual = [1]
    direction = [1]
    rho = entries[(0, 0)]
    steps = []
    for iteration in range(ITERS):
        image = operate(direction)
        alpha = rho[0] / with_shadow(image)[0]
        middle = combine(residual, -alpha, image)
        turned = operate(middle)
        weighted = gram_times(turned)
        cross = over_sublanes(dd_mul(weighted, stack(middle)))
        square = over_sublanes(dd_mul(weighted, stack(turned)))
        omega = cross[0] / square[0]
        steps += [(alpha, rounded(direction)), (omega, rounded(middle))]
        residual = combine(middle, -omega, turned)
        if iteration + 1 < ITERS:
            rho_next = with_shadow(residual)
            factor = (rho_next[0] / rho[0]) * (alpha / omega)
            direction = combine(direction, -omega, image)
            direction = combine(residual, factor, direction)
            rho = rho_next
    residual = rounded(residual)
    answer = []
    for step, poly in steps:
        for i, item in enumerate(poly):
            if i == len(answer):
                answer.append(step * item)
            else:
                answer[i] = answer[i] + step * item
    moves = []
    for c in range(COMPS):
        for n, (poly, basis, here, out) in enumerate(
            (
                (answer, solved, solution_here, solution_out),
                (residual, values, residual_here, residual_out),
            )
        ):
            scales = [item[:, c : c + 1] for item in poly]
            for k in range(planes):
                for r in range(0, rows, 8):
                    total = scales[0] * basis[0][c, k, r : r + 8, :]
                    for i in range(1, len(scales)):
                        total = total + scales[i] * basis[i][c, k, r : r + 8, :]
                    here[c, k, r : r + 8, :] = total
            moves.append(pltpu.make_async_copy(here.at[c], out.at[c], sent.at[n * COMPS + c]))
            moves[-1].start()
    for move in moves:
        move.wait()


def ring(array, axis, step):
    count = lax.axis_size(axis)
    return lax.ppermute(array, axis, [(i, (i + step) % count) for i in range(count)])


def race(array, step):
    slabs, copies = lax.axis_size("slab"), lax.axis_size("batch")
    pairs = []
    for s in range(slabs):
        for b in range(copies):
            t = s + abs(step) if b % 2 == 0 else s - abs(step)
            target = t * copies + b if 0 <= t < slabs else s * copies + (b ^ 1)
            pairs.append((s * copies + b, target))
    if step < 0:
        pairs = [(t, s) for s, t in pairs]
    return lax.ppermute(array, ("slab", "batch"), sorted(pairs))


def local(velocity_old, courant, cell_ids, forces, weights):
    planes, rows, width = velocity_old.shape[1:]
    slabs, copies = lax.axis_size("slab"), lax.axis_size("batch")
    everyone = ("slab", "batch")
    wide = rows + 2 * DEPTH
    height = rows * copies
    tile = cell_ids.shape[0] // slabs
    assert rows % 8 == 0 and width == 128 and copies % 2 == 0
    assert planes * height <= 256 and 2 * DEPTH <= height - rows
    field = jax.ShapeDtypeStruct((COMPS, planes, wide, width), F32)
    quad = jax.ShapeDtypeStruct((4, planes, wide, width), F32)
    edge = jax.ShapeDtypeStruct((2 * COMPS, planes, DEPTH, width), F32)
    own = jax.ShapeDtypeStruct(velocity_old.shape, F32)

    def call(kernel, out_shape, in_specs, mib, scratch=(), out_space=VMEM, cost=None):
        if cost is not None:
            cost = pl.CostEstimate(flops=cost, bytes_accessed=0, transcendentals=0)
        return pl.pallas_call(
            kernel,
            out_shape=out_shape,
            in_specs=in_specs,
            out_specs=[out_space] * len(out_shape),
            cost_estimate=cost,
            scratch_shapes=list(scratch),
            compiler_params=pltpu.CompilerParams(vmem_limit_bytes=mib << 20),
        )

    def pack(*refs):
        pack_kernel(slabs, copies, *refs)

    (message,) = call(
        pack,
        (jax.ShapeDtypeStruct((slabs * copies, 8, tile), jnp.bfloat16),),
        [ANY] * 3,
        8,
        [
            pltpu.VMEM((slabs, tile), jnp.int32),
            pltpu.VMEM(forces.shape, F32),
            pltpu.VMEM((slabs, tile), F32),
            pltpu.SemaphoreType.DMA((3,)),
        ],
    )(
        *(
            pltpu.with_memory_space_constraint(x, pltpu.HBM)
            for x in (cell_ids.reshape(slabs, tile), forces, weights.reshape(slabs, tile))
        )
    )
    received = lax.all_to_all(message, everyone, 0, 0, tiled=True)
    first, last = call(edges_kernel, (edge, edge), [VMEM] * 2, 2)(velocity_old, courant)
    after = ring(first, "batch", -1)
    before = ring(last, "batch", 1)

    def deposit(*refs):
        deposit_kernel(rows, copies, 8, *refs)

    (deposited,) = call(
        deposit, (jax.ShapeDtypeStruct((COMPS * planes * wide, width), F32),), [VMEM], 12
    )(received)

    def setup(*refs):
        setup_kernel(slabs, copies, *refs)

    def flat(count):
        return jax.ShapeDtypeStruct((count, width), F32)

    def faces(count):
        return jax.ShapeDtypeStruct((COMPS, count, width), F32)

    value, solved, inner, *sent, side, block = call(
        setup,
        (field,) * 3 + (flat((2 * COMPS + 2) * wide),) * 2 + (faces(wide),) * 2 + (quad,) * 2,
        [VMEM] * 5,
        2,
        [pltpu.VMEM((3, planes, wide, width), F32)],
    )(velocity_old, courant, after, before, deposited)

    values, solves = [value], [solved]
    first = None
    for iteration in range(ITERS):
        near, far = [], []
        for n, sign in enumerate((1, -1)):
            near.append(race(sent[n], sign))
            far.append(race(sent[2 + n], 2 * sign))
        first = first or near
        known = (solved, inner, *near, *far, *first, side, block)
        if iteration + 1 < ITERS:
            reach = wide if iteration + 2 < ITERS else rows
            value, one_solved, second, solved, inner, *sent = call(
                advance_kernel,
                (field,) * 5 + (flat(COMPS * (wide + reach)),) * 2 + (faces(reach),) * 2,
                [VMEM] * 10,
                2,
            )(*known)
            solves += [one_solved, solved]
        else:
            def early(*refs):
                early_kernel(rows, *refs)

            sums = call(early, (flat(EARLY_ROWS),) * 2, [VMEM] * EARLY, 2, cost=4000000)(*values)
            value, one_solved, second, message = call(
                gram_kernel, (field,) * 3 + (flat(slabs * copies),), [VMEM] * (12 + EARLY), 4
            )(*known, *values, *sums)
            solves += [one_solved]
        values += [value, second]
    gathered = lax.all_to_all(message, everyone, 0, 0, tiled=True)
    return call(
        finish_kernel,
        (own, own),
        [VMEM] * (1 + BASIS + DEPTH),
        4,
        [pltpu.VMEM(own.shape, F32)] * 2 + [pltpu.SemaphoreType.DMA((2 * COMPS,))],
        ANY,
    )(gathered, *values, *solves)


def solution(mesh):
    placed = (
        P(None, "slab", "batch", None),
        P(None, "slab", "batch", None),
        P(("slab", "batch")),
        P(None, ("slab", "batch")),
        P(("slab", "batch")),
    )
    return jax.shard_map(
        local,
        mesh=mesh,
        in_specs=placed,
        out_specs=(P(None, "slab", "batch", None), P(None, "slab", "batch", None)),
        check_vma=False,
    )
```

```python
import jax
import jax.numpy as jnp
from jax import lax
from jax.experimental import pallas as pl
from jax.experimental.pallas import tpu as pltpu
from jax.sharding import PartitionSpec as P


ITERS = 2
DEPTH = 2 * ITERS
COMPS = 3
BASIS = DEPTH + 1
EARLY = DEPTH - 1
PAIRS = sorted(((i, j) for j in range(BASIS) for i in range(j + 1)), key=lambda p: p[1] >= EARLY)
EARLY_PAIRS = [p for p in PAIRS if p[1] < EARLY]
LATE_PAIRS = [p for p in PAIRS if p[1] >= EARLY]
EARLY_ROWS = -(-len(EARLY_PAIRS) * COMPS // 8) * 8

diffusion_number = 1.0
diagonal_value = 7.0

VMEM = pl.BlockSpec(memory_space=pltpu.VMEM)
ANY = pl.BlockSpec(memory_space=pl.ANY)
F32 = jnp.float32


def two_sum(a, b):
    s = a + b
    bb = s - a
    return s, (a - (s - bb)) + (b - bb)


def quick_two_sum(a, b):
    s = a + b
    return s, b - (s - a)


def split(a):
    t = a * 4097.0
    high = t - (t - a)
    return high, a - high


def product_error(p, a, b):
    ah, al = a
    bh, bl = b
    return ((ah * bh - p) + ah * bl + al * bh) + al * bl


def dd_add(a, b):
    if isinstance(b, int):
        a, b = b, a
    if isinstance(a, int):
        if isinstance(b, int):
            return a + b
        if a == 0:
            return b
        a = (jnp.full_like(b[0], a), jnp.zeros_like(b[0]))
    s, e = two_sum(a[0], b[0])
    return quick_two_sum(s, e + (a[1] + b[1]))


def dd_neg(a):
    return -a if isinstance(a, int) else (-a[0], -a[1])


def dd_sub(a, b):
    return dd_add(a, dd_neg(b))


def dd_mul(a, b):
    if isinstance(b, int):
        a, b = b, a
    if isinstance(a, int):
        if isinstance(b, int):
            return a * b
        return {0: 0, 1: b, -1: dd_neg(b)}[a]
    p = a[0] * b[0]
    e = product_error(p, split(a[0]), split(b[0]))
    return quick_two_sum(p, e + (a[0] * b[1] + a[1] * b[0]))


def dd_scale(factor, b):
    if isinstance(b, int):
        return 0 if b == 0 else (b * factor, jnp.zeros_like(factor))
    p = factor * b[0]
    e = product_error(p, split(factor), split(b[0]))
    return quick_two_sum(p, e + factor * b[1])


def solve_block(values, inverses, ratios, lower_planes):
    forward = []
    for k, current in enumerate(values):
        if k > 0:
            current = current + lower_planes[k] * forward[-1]
        forward.append(current * inverses[k])
    result = [forward[-1]]
    for k in range(len(values) - 2, -1, -1):
        result.insert(0, forward[k] - ratios[k] * result[0])
    return result


def pack_kernel(
    slabs, copies, ids_in, forces_in, weights_in, velocity_in, courant_in,
    message_out, fields_out, ids, forces, weights, arrived,
):
    moves = [
        pltpu.make_async_copy(source, target, arrived.at[n])
        for n, (source, target) in enumerate(
            [
                (ids_in, ids),
                (weights_in, weights),
                (forces_in, forces),
                (velocity_in, fields_out.at[0]),
                (courant_in, fields_out.at[1]),
            ]
        )
    ]
    for move in moves:
        move.start()
    for move in moves[:3]:
        move.wait()
    tile = ids.shape[1]
    width = 128
    high = ids[...] // width
    low = ids[...] - high * width
    rest = [high.astype(F32), low.astype(F32)]
    rest += [jnp.zeros_like(rest[0])] * (8 - COMPS - len(rest))
    for pair in range(0, slabs, 2):
        blocks = []
        for s in (pair, pair + 1):
            at = slice(s * tile, (s + 1) * tile)
            blocks += [forces[:, at] * weights[s : s + 1]] + [part[s : s + 1] for part in rest]
        block = jnp.concatenate(blocks, axis=0).astype(jnp.bfloat16)
        for k in range(2 * copies):
            message_out[pair * copies + k] = block
    for move in moves[3:]:
        move.wait()


def own_block():
    return lax.axis_index("slab") % 2


def edges_kernel(here, beside, first_out, last_out):
    rows = here.shape[3]
    own = own_block()
    for block in range(2):
        for n in range(2):
            for d in range(COMPS):
                for out, at in ((first_out, slice(0, DEPTH)), (last_out, slice(rows - DEPTH, rows))):
                    out[block, n * COMPS + d] = jnp.where(
                        own == block, here[n, d, :, at], beside[n, d, :, at]
                    )


def deposit_kernel(rows, copies, group, message, momentum_sum):
    wide = rows + 2 * DEPTH
    height = rows * copies
    planes = momentum_sum.shape[1] // (COMPS * wide)
    width = momentum_sum.shape[2]
    start = lax.axis_index("batch") * rows
    tile = message.shape[2]
    narrow = jnp.bfloat16
    count = lax.broadcasted_iota(jnp.int32, (16, tile), 0).astype(F32)
    counts = [(count + 16.0 * g).astype(narrow) for g in range(width // 16)]
    nothing = jnp.zeros((16, tile), narrow)
    one = jnp.ones((16, tile), narrow)

    def over_sixteen(row):
        return jnp.broadcast_to(row, (16, tile)).astype(narrow)

    def deposit(block, step):
        row_values, column_hot = [], []
        for k in range(group):
            part = message[step * group + k, 8 * block : 8 * block + 8].astype(F32)
            cell_row = part[3:4].astype(jnp.int32)
            plane = jnp.zeros_like(cell_row)
            for p in range(1, planes):
                plane = plane + (cell_row >= p * height).astype(jnp.int32)
            away = cell_row - plane * height - start
            away = jnp.where(away < 0, away + height, away)
            spot = jnp.where(away < rows + DEPTH, away, away - height + wide)
            inside = (away < rows + DEPTH) | (away >= height - DEPTH)
            spot = over_sixteen(jnp.where(inside, spot + plane * wide, -1).astype(F32))
            column = over_sixteen(part[4:5])
            values = [over_sixteen(part[c : c + 1]) for c in range(COMPS)]
            here = [counts[g] == spot for g in range(planes * wide // 16)]
            row_values.append(
                jnp.concatenate(
                    [jnp.where(at, value, nothing) for value in values for at in here], axis=0
                )
            )
            column_hot.append(
                jnp.concatenate([jnp.where(n == column, one, nothing) for n in counts], axis=0)
            )
        return lax.dot_general(
            jnp.concatenate(row_values, axis=1),
            jnp.concatenate(column_hot, axis=1),
            (((1,), (1,)), ((), ())),
            preferred_element_type=F32,
        )

    steps = message.shape[0] // group
    for block in range(2):
        if steps <= 4:
            total = deposit(block, 0)
            for step in range(1, steps):
                total = total + deposit(block, step)
            momentum_sum[block] = total
        else:
            momentum_sum[block] = jnp.zeros(momentum_sum.shape[1:], F32)

            def add_step(step, carry):
                momentum_sum[block] += deposit(block, step)
                return carry

            lax.fori_loop(0, steps, add_step, 0)


def fill_coefficients(courant, slab, slabs, batch, copies, rows, side, block):
    planes, wide, width = side.shape[1:]
    spots = lax.broadcasted_iota(jnp.int32, (wide, width), 0)
    lanes = lax.broadcasted_iota(jnp.int32, (wide, width), 1)
    at_top = (spots == rows - 1) & (batch == copies - 1)
    at_bottom = (spots == 0) & (batch == 0)
    ratio = None
    for k in range(planes):
        upper, lower = [], []
        for d in range(3):
            half = 0.5 * courant(d, k)
            upper.append(diffusion_number - half)
            lower.append(diffusion_number + half)
        side[0, k] = jnp.where(at_top, 0.0, upper[1])
        side[1, k] = jnp.where(at_bottom, 0.0, lower[1])
        side[2, k] = jnp.where(lanes == width - 1, 0.0, upper[2])
        side[3, k] = jnp.where(lanes == 0, 0.0, lower[2])
        if k == 0:
            pivot = jnp.full((wide, width), diagonal_value, F32)
            block[3, 0] = jnp.where(slab <= 0, 0.0, lower[0])
        else:
            pivot = diagonal_value + lower[0] * ratio
        if k == planes - 1:
            block[3, 1] = jnp.where(slab >= slabs - 1, 0.0, upper[0])
        inverse = 1.0 / pivot
        ratio = -upper[0] * inverse
        block[0, k] = inverse
        block[1, k] = ratio
        block[2, k] = lower[0]


def solve(values, block):
    planes = len(values)
    return solve_block(values, *([block[n, k] for k in range(planes)] for n in range(3)))


def in_plane(planes_here, side):
    wide, width = planes_here[0].shape
    values = []
    for k, here in enumerate(planes_here):
        total = side[0, k] * pltpu.roll(here, wide - 1, 0)
        total = total + side[1, k] * pltpu.roll(here, 1, 0)
        total = total + side[2, k] * pltpu.roll(here, width - 1, 1)
        total = total + side[3, k] * pltpu.roll(here, 1, 1)
        values.append(total)
    return values


def add_below(values, face, block):
    return [values[0] + block[3, 0] * face] + list(values[1:])


def add_above(values, face, block):
    return list(values[:-1]) + [values[-1] + block[3, 1] * face]


def inside_pair(lower, upper, side, block):
    return (
        add_above(in_plane(lower, side.at[0]), upper[0], block.at[0]),
        add_below(in_plane(upper, side.at[1]), lower[-1], block.at[1]),
    )


def store_pair(c, pair, out):
    for n, values in enumerate(pair):
        for k, item in enumerate(values):
            out[n, c, k] = item


def store_own(c, pair, out):
    own = own_block()
    for k, (one, other) in enumerate(zip(*pair)):
        out[c, k] = jnp.where(own == 0, one, other)


def store_messages(c, solved, inner, block, rows, near_out):
    even = lax.axis_index("batch") % 2 == 0
    wide = solved[0][0].shape[0]
    up = (solved[1][-1], solve(inner[1], block.at[1])[-1])
    down = (solved[0][0], solve(inner[0], block.at[0])[0])
    start = COMPS * wide + c * rows
    for n, (one, other) in enumerate(((up, down), (down, up))):
        near_out[n][c * wide : (c + 1) * wide] = jnp.where(even, one[0], other[0])
        near_out[n][start : start + rows] = jnp.where(even, one[1], other[1])[:rows]


def setup_kernel(
    slabs, copies,
    here, beside, after, before, momentum_sum,
    value_out, own_out, solved_out, inner_out, near1, near2, side, block, wide_courant,
):
    planes, rows, width = here.shape[2:]
    wide = rows + 2 * DEPTH
    batch = lax.axis_index("batch")
    even = batch % 2 == 0
    slab, own = lax.axis_index("slab"), own_block()
    for n in range(2):
        for d in range(3):
            for k in range(planes):
                wide_courant[n, d, k] = jnp.concatenate(
                    [
                        jnp.where(own == n, here[1, d, k], beside[1, d, k]),
                        after[n, COMPS + d, k],
                        before[n, COMPS + d, k],
                    ],
                    axis=0,
                )
        fill_coefficients(
            lambda d, k: wide_courant[n, d, k],
            slab - own + n, slabs, batch, copies, rows, side.at[n], block.at[n],
        )
    zero = jnp.zeros((wide, width), F32)
    from_below = solve([block[0, 3, 0]] + [zero] * (planes - 1), block.at[0])[0]
    from_above = solve([zero] * (planes - 1) + [block[1, 3, 1]], block.at[1])[-1]
    at = slice(2 * COMPS * wide, (2 * COMPS + 1) * wide)
    near1[at] = jnp.where(even, from_above, from_below)
    near2[at] = jnp.where(even, from_below, from_above)
    for c in range(COMPS):
        pair, solved = [], []
        for n in range(2):
            values = []
            for k in range(planes):
                old = jnp.concatenate(
                    [
                        jnp.where(own == n, here[0, c, k], beside[0, c, k]),
                        after[n, c, k],
                        before[n, c, k],
                    ],
                    axis=0,
                )
                at = (c * planes + k) * wide
                values.append(old + momentum_sum[n, at : at + wide])
            pair.append(values)
            solved.append(solve(values, block.at[n]))
        inner = inside_pair(*solved, side, block)
        store_own(c, pair, value_out)
        store_own(c, solved, own_out)
        store_pair(c, solved, solved_out)
        store_pair(c, inner, inner_out)
        store_messages(c, solved, inner, block, wide, (near1, near2))


def next_level(solved, inner, near1, near2, first1, first2, block):
    planes, wide = solved.shape[2:4]
    rows = near1.shape[0] // COMPS - wide
    if near1 is first1:
        rows = wide
    even = lax.axis_index("batch") % 2 == 0

    def low(one, other):
        return jnp.where(even, one, other)

    def high(one, other):
        return jnp.where(even, other, one)

    def part(pick, start, count):
        at = slice(start, start + count)
        return pick(near1[at], near2[at])

    at = slice(2 * COMPS * wide, 2 * COMPS * wide + rows)
    low_response, high_response = (pick(first1[at], first2[at]) for pick in (low, high))
    pad = jnp.zeros((wide - rows, solved.shape[4]), F32)

    def widen(x):
        return x if rows == wide else jnp.concatenate([x, pad], axis=0)

    for c in range(COMPS):
        own = COMPS * wide + c * rows
        lower = [inner[0, c, k] for k in range(planes)]
        upper = [inner[1, c, k] for k in range(planes)]
        one = (
            add_below(lower, part(low, c * wide, wide), block.at[0]),
            add_above(upper, part(high, c * wide, wide), block.at[1]),
        )
        one_solved = tuple(solve(one[n], block.at[n]) for n in range(2))
        below = part(low, own, rows) + low_response * solved[0, c, 0][:rows]
        above = part(high, own, rows) + high_response * solved[1, c, planes - 1][:rows]
        yield c, one, one_solved, widen(below), widen(above)


def advance_kernel(
    repeat, *refs,
):
    solved, inner, near1, near2, first1, first2, side, block = refs[:8]
    if repeat:
        first1, first2 = near1, near2
    value_out, own_out, second_out, last_out, solved_out, inner_out, to1, to2 = refs[8:]
    wide = solved.shape[3]
    rows = to1.shape[0] // COMPS - wide
    for c, one, one_solved, below, above in next_level(
        solved, inner, near1, near2, first1, first2, block
    ):
        within = inside_pair(*one_solved, side, block)
        two = (
            add_below(within[0], below, block.at[0]),
            add_above(within[1], above, block.at[1]),
        )
        two_solved = tuple(solve(two[n], block.at[n]) for n in range(2))
        inner_next = inside_pair(*two_solved, side, block)
        store_own(c, one, value_out)
        store_own(c, one_solved, own_out)
        store_own(c, two, second_out)
        store_own(c, two_solved, last_out)
        store_pair(c, two_solved, solved_out)
        store_pair(c, inner_next, inner_out)
        store_messages(c, two_solved, inner_next, block, rows, (to1, to2))


def gram_sums(pieces, pairs, totals):
    halves = [split(piece) for piece in pieces]
    for n, (i, j) in enumerate(pairs):
        p = pieces[i] * pieces[j]
        e = product_error(p, halves[i], halves[j])
        if totals[n] is None:
            totals[n] = (p, e)
        else:
            s, t = two_sum(totals[n][0], p)
            totals[n] = (s, totals[n][1] + (t + e))


def stack_sums(sums, count):
    flat = [sums[c][n] for n in range(len(sums[0])) for c in range(COMPS)]
    flat += [(jnp.zeros_like(flat[0][0]),) * 2] * (count - len(flat))
    rows_of = [sum_to_sublanes(flat[n : n + 8]) for n in range(0, count, 8)]
    return [jnp.concatenate([x[p] for x in rows_of], axis=0) for p in (0, 1)]


def early_kernel(rows, *refs):
    values, (high_out, low_out) = refs[:EARLY], refs[EARLY:]
    sums = []
    for c in range(COMPS):
        totals = [None] * len(EARLY_PAIRS)
        for k in range(values[0].shape[1]):
            for r in range(0, rows, 8):
                gram_sums([v[c, k, r : r + 8, :] for v in values], EARLY_PAIRS, totals)
        sums.append(totals)
    high_out[...], low_out[...] = stack_sums(sums, EARLY_ROWS)


def gram_kernel(*refs):
    solved, inner, near1, near2, first1, first2, side, block = refs[:8]
    values = refs[8 : 8 + EARLY]
    early = refs[8 + EARLY : 10 + EARLY]
    value_out, solved_out, second_out, message_out = refs[10 + EARLY :]
    own = own_block()
    planes, wide, width = value_out.shape[1:]
    rows = wide - 2 * DEPTH
    sums = []
    for c, ones, one_pair, below, above in next_level(
        solved, inner, near1, near2, first1, first2, block
    ):
        one, one_solved = (
            [jnp.where(own == 0, x, y) for x, y in zip(*pair)] for pair in (ones, one_pair)
        )
        two = in_plane(one_solved, side.at[own])
        two = add_below(two, jnp.where(own == 0, below, one_pair[0][-1]), block.at[own])
        two = add_above(two, jnp.where(own == 0, one_pair[1][0], above), block.at[own])
        totals = [None] * len(LATE_PAIRS)
        for k in range(planes):
            value_out[c, k] = one[k]
            solved_out[c, k] = one_solved[k]
            second_out[c, k] = two[k]
            for r in range(0, rows, 8):
                pieces = [value[c, k, r : r + 8, :] for value in values]
                gram_sums(pieces + [one[k][r : r + 8], two[k][r : r + 8]], LATE_PAIRS, totals)
        sums.append(totals)
    late = stack_sums(sums, width // 2 - EARLY_ROWS)
    turned = [jnp.transpose(jnp.concatenate([e[...], x], axis=0)) for e, x in zip(early, late)]
    total = tuple(x[:8] for x in turned)
    for r in range(8, width, 8):
        total = dd_add(total, tuple(x[r : r + 8] for x in turned))
    for shift in (4, 2, 1):
        total = dd_add(total, tuple(pltpu.roll(x, shift, 0) for x in total))
    row = jnp.concatenate([x[:1] for x in total], axis=1)
    message_out[...] = jnp.broadcast_to(row, message_out.shape)


def sum_to_sublanes(parts):
    sub = lax.broadcasted_iota(jnp.int32, parts[0][0].shape, 0)
    level = parts
    for shift in (4, 2, 1):
        keep = (sub & shift) == 0
        merged = []
        for a, b in zip(level[:shift], level[shift:]):
            stay = tuple(jnp.where(keep, x, y) for x, y in zip(a, b))
            swap = [jnp.where(keep, y, x) for x, y in zip(a, b)]
            moved = tuple(
                pltpu.roll(w, 4, 0)
                if shift == 4
                else jnp.where(keep, pltpu.roll(w, 8 - shift, 0), pltpu.roll(w, shift, 0))
                for w in swap
            )
            merged.append(dd_add(stay, moved))
        level = merged
    return level[0]


def finish_kernel(*refs):
    gathered = refs[0]
    values = refs[1 : 1 + BASIS]
    solved = refs[1 + BASIS : 1 + BASIS + DEPTH]
    solution_out, residual_out, solution_here, residual_here, sent = refs[1 + BASIS + DEPTH :]
    planes, rows, _ = solution_here.shape[1:]
    count, lanes = gathered.shape
    total = None
    for r in range(0, count, 8):
        high = gathered[r : r + 8]
        item = (high, pltpu.roll(high, lanes // 2, 1))
        total = item if total is None else dd_add(total, item)
    for shift in (4, 2, 1):
        total = dd_add(total, tuple(pltpu.roll(x, shift, 0) for x in total))
    sub = lax.broadcasted_iota(jnp.int32, (8, lanes), 0)

    def entry(n):
        start = n * COMPS
        if n >= len(EARLY_PAIRS):
            start = EARLY_ROWS + (n - len(EARLY_PAIRS)) * COMPS
        return tuple(pltpu.roll(x, (lanes - start) % lanes, 1) for x in total)

    entries = {pair: entry(n) for n, pair in enumerate(PAIRS)}
    gram = []
    for i in range(BASIS):
        row = None
        for j in range(BASIS):
            item = entries[(min(i, j), max(i, j))]
            if row is None:
                row = item
            else:
                row = tuple(jnp.where(sub == j, x, y) for x, y in zip(item, row))
        gram.append(row)
    zero = jnp.zeros((8, lanes), F32)

    def stack(poly):
        out = (zero, zero)
        for j, item in enumerate(poly):
            if isinstance(item, int):
                item = (zero + item, zero)
            out = tuple(jnp.where(sub == j, x, y) for x, y in zip(item, out))
        return out

    def over_sublanes(x):
        for shift in (4, 2, 1):
            x = dd_add(x, tuple(pltpu.roll(y, shift, 0) for y in x))
        return x

    def gram_times(poly):
        out = 0
        for i, item in enumerate(poly):
            out = dd_add(out, dd_mul(item, gram[i]))
        return tuple(jnp.where(sub < BASIS, x, 0.0) for x in out)

    def with_shadow(poly):
        terms = [dd_mul(item, entries[(0, i)]) for i, item in enumerate(poly)]
        while len(terms) > 1:
            pairs = [dd_add(*terms[i : i + 2]) for i in range(0, len(terms) - 1, 2)]
            terms = pairs + terms[len(pairs) * 2 :]
        return terms[0]

    def operate(poly):
        out = list(poly) + [0]
        return [out[0]] + [dd_sub(out[i], out[i - 1]) for i in range(1, len(out))]

    def combine(first, factor, second):
        out = []
        for i in range(max(len(first), len(second))):
            item = first[i] if i < len(first) else 0
            if i < len(second):
                item = dd_add(item, dd_scale(factor, second[i]))
            out.append(item)
        return out

    def rounded(poly):
        return [zero + item if isinstance(item, int) else item[0] for item in poly]

    residual = [1]
    direction = [1]
    rho = entries[(0, 0)]
    steps = []
    for iteration in range(ITERS):
        image = operate(direction)
        alpha = rho[0] / with_shadow(image)[0]
        middle = combine(residual, -alpha, image)
        turned = operate(middle)
        weighted = gram_times(turned)
        cross = over_sublanes(dd_mul(weighted, stack(middle)))
        square = over_sublanes(dd_mul(weighted, stack(turned)))
        omega = cross[0] / square[0]
        steps += [(alpha, rounded(direction)), (omega, rounded(middle))]
        residual = combine(middle, -omega, turned)
        if iteration + 1 < ITERS:
            rho_next = with_shadow(residual)
            factor = (rho_next[0] / rho[0]) * (alpha / omega)
            direction = combine(direction, -omega, image)
            direction = combine(residual, factor, direction)
            rho = rho_next
    residual = rounded(residual)
    answer = []
    for step, poly in steps:
        for i, item in enumerate(poly):
            if i == len(answer):
                answer.append(step * item)
            else:
                answer[i] = answer[i] + step * item
    moves = []
    for c in range(COMPS):
        for n, (poly, basis, here, out) in enumerate(
            (
                (answer, solved, solution_here, solution_out),
                (residual, values, residual_here, residual_out),
            )
        ):
            scales = [item[:, c : c + 1] for item in poly]
            for k in range(planes):
                for r in range(0, rows, 8):
                    total = scales[0] * basis[0][c, k, r : r + 8, :]
                    for i in range(1, len(scales)):
                        total = total + scales[i] * basis[i][c, k, r : r + 8, :]
                    here[c, k, r : r + 8, :] = total
            moves.append(pltpu.make_async_copy(here.at[c], out.at[c], sent.at[n * COMPS + c]))
            moves[-1].start()
    for move in moves:
        move.wait()


def ring(array, axis, step):
    count = lax.axis_size(axis)
    return lax.ppermute(array, axis, [(i, (i + step) % count) for i in range(count)])


def race(array, step):
    slabs, copies = lax.axis_size("slab"), lax.axis_size("batch")
    pairs = []
    for s in range(slabs):
        for b in range(copies):
            t = s + abs(step) if b % 2 == 0 else s - abs(step)
            target = t * copies + b if 0 <= t < slabs else s * copies + (b ^ 1)
            pairs.append((s * copies + b, target))
    if step < 0:
        pairs = [(t, s) for s, t in pairs]
    return lax.ppermute(array, ("slab", "batch"), sorted(pairs))


def local(velocity_old, courant, cell_ids, forces, weights):
    planes, rows, width = velocity_old.shape[1:]
    slabs, copies = lax.axis_size("slab"), lax.axis_size("batch")
    everyone = ("slab", "batch")
    wide = rows + 2 * DEPTH
    height = rows * copies
    tile = cell_ids.shape[0] // slabs
    assert rows % 8 == 0 and width == 128 and copies % 2 == 0 and slabs % 2 == 0
    assert planes * height <= 256 and 2 * DEPTH <= height - rows
    field = jax.ShapeDtypeStruct((COMPS, planes, wide, width), F32)
    quad = jax.ShapeDtypeStruct((2, 4, planes, wide, width), F32)
    both = jax.ShapeDtypeStruct((2, COMPS, planes, wide, width), F32)
    edge = jax.ShapeDtypeStruct((2, 2 * COMPS, planes, DEPTH, width), F32)
    own = jax.ShapeDtypeStruct(velocity_old.shape, F32)

    def call(kernel, out_shape, in_specs, mib, scratch=(), out_space=VMEM, cost=None):
        if cost is not None:
            cost = pl.CostEstimate(flops=cost, bytes_accessed=0, transcendentals=0)
        return pl.pallas_call(
            kernel,
            out_shape=out_shape,
            in_specs=in_specs,
            out_specs=[out_space] * len(out_shape),
            cost_estimate=cost,
            scratch_shapes=list(scratch),
            compiler_params=pltpu.CompilerParams(vmem_limit_bytes=mib << 20),
        )

    def pack(*refs):
        pack_kernel(slabs, copies, *refs)

    message, fields = call(
        pack,
        (
            jax.ShapeDtypeStruct((slabs * copies, 16, tile), jnp.bfloat16),
            jax.ShapeDtypeStruct((2, *velocity_old.shape), F32),
        ),
        [ANY] * 5,
        8,
        [
            pltpu.VMEM((slabs, tile), jnp.int32),
            pltpu.VMEM(forces.shape, F32),
            pltpu.VMEM((slabs, tile), F32),
            pltpu.SemaphoreType.DMA((5,)),
        ],
    )(
        *(
            pltpu.with_memory_space_constraint(x, pltpu.HBM)
            for x in (
                cell_ids.reshape(slabs, tile),
                forces,
                weights.reshape(slabs, tile),
                velocity_old,
                courant,
            )
        )
    )
    beside = lax.ppermute(fields, "slab", [(s, s ^ 1) for s in range(slabs)])
    received = lax.all_to_all(message, everyone, 0, 0, tiled=True)
    first, last = call(edges_kernel, (edge, edge), [VMEM] * 2, 2)(fields, beside)
    after = ring(first, "batch", -1)
    before = ring(last, "batch", 1)

    def deposit(*refs):
        deposit_kernel(rows, copies, 8, *refs)

    (deposited,) = call(
        deposit, (jax.ShapeDtypeStruct((2, COMPS * planes * wide, width), F32),), [VMEM], 12
    )(received)

    def setup(*refs):
        setup_kernel(slabs, copies, *refs)

    def flat(count):
        return jax.ShapeDtypeStruct((count, width), F32)

    value, own_solved, solved, inner, *sent, side, block = call(
        setup,
        (field,) * 2 + (both,) * 2 + (flat((2 * COMPS + 1) * wide),) * 2 + (quad,) * 2,
        [VMEM] * 5,
        2,
        [pltpu.VMEM((2, 3, planes, wide, width), F32)],
    )(fields, beside, after, before, deposited)

    values, solves = [value], [own_solved]
    first = None
    for iteration in range(ITERS):
        near = [race(sent[0], 2), race(sent[1], -2)]
        repeat = first is None
        first = first or near
        known = (solved, inner, *near, *first, side, block)
        if iteration + 1 < ITERS:
            reach = wide if iteration + 2 < ITERS else rows

            def advance(*refs):
                advance_kernel(repeat, *refs)

            value, one_solved, second, last_solved, solved, inner, *sent = call(
                advance,
                (field,) * 4 + (both,) * 2 + (flat(COMPS * (wide + reach)),) * 2,
                [VMEM] * 8,
                3,
            )(*known)
            solves += [one_solved, last_solved]
        else:

            def early(*refs):
                early_kernel(rows, *refs)

            sums = call(early, (flat(EARLY_ROWS),) * 2, [VMEM] * EARLY, 2, cost=4000000)(*values)
            value, one_solved, second, message = call(
                gram_kernel, (field,) * 3 + (flat(slabs * copies),), [VMEM] * (10 + EARLY), 4
            )(*known, *values, *sums)
            solves += [one_solved]
        values += [value, second]
    gathered = lax.all_to_all(message, everyone, 0, 0, tiled=True)
    return call(
        finish_kernel,
        (own, own),
        [VMEM] * (1 + BASIS + DEPTH),
        4,
        [pltpu.VMEM(own.shape, F32)] * 2 + [pltpu.SemaphoreType.DMA((2 * COMPS,))],
        ANY,
    )(gathered, *values, *solves)


def solution(mesh):
    placed = (
        P(None, "slab", "batch", None),
        P(None, "slab", "batch", None),
        P(("slab", "batch")),
        P(None, ("slab", "batch")),
        P(("slab", "batch")),
    )
    return jax.shard_map(
        local,
        mesh=mesh,
        in_specs=placed,
        out_specs=(P(None, "slab", "batch", None), P(None, "slab", "batch", None)),
        check_vma=False,
    )
```

```python
import jax
import jax.numpy as jnp
from jax import lax
from jax.experimental import pallas as pl
from jax.experimental.pallas import tpu as pltpu
from jax.sharding import PartitionSpec as P


ITERS = 2
DEPTH = 2 * ITERS
COMPS = 3
BASIS = DEPTH + 1
EARLY = DEPTH - 1
LOWEST = -63
PAIRS = sorted(((i, j) for j in range(BASIS) for i in range(j + 1)), key=lambda p: p[1] >= EARLY)
EARLY_PAIRS = [p for p in PAIRS if p[1] < EARLY]
LATE_PAIRS = [p for p in PAIRS if p[1] >= EARLY]
EARLY_ROWS = -(-len(EARLY_PAIRS) * COMPS // 8) * 8

diffusion_number = 1.0
diagonal_value = 7.0

VMEM = pl.BlockSpec(memory_space=pltpu.VMEM)
ANY = pl.BlockSpec(memory_space=pl.ANY)
F32 = jnp.float32


def two_sum(a, b):
    s = a + b
    bb = s - a
    return s, (a - (s - bb)) + (b - bb)


def quick_two_sum(a, b):
    s = a + b
    return s, b - (s - a)


def split(a):
    t = a * 4097.0
    high = t - (t - a)
    return high, a - high


def product_error(p, a, b):
    ah, al = a
    bh, bl = b
    return ((ah * bh - p) + ah * bl + al * bh) + al * bl


def dd_add(a, b):
    if isinstance(b, int):
        a, b = b, a
    if isinstance(a, int):
        if isinstance(b, int):
            return a + b
        if a == 0:
            return b
        a = (jnp.full_like(b[0], a), jnp.zeros_like(b[0]))
    s, e = two_sum(a[0], b[0])
    return quick_two_sum(s, e + (a[1] + b[1]))


def dd_neg(a):
    return -a if isinstance(a, int) else (-a[0], -a[1])


def dd_sub(a, b):
    return dd_add(a, dd_neg(b))


def dd_mul(a, b):
    if isinstance(b, int):
        a, b = b, a
    if isinstance(a, int):
        if isinstance(b, int):
            return a * b
        return {0: 0, 1: b, -1: dd_neg(b)}[a]
    p = a[0] * b[0]
    e = product_error(p, split(a[0]), split(b[0]))
    return quick_two_sum(p, e + (a[0] * b[1] + a[1] * b[0]))


def dd_scale(factor, b):
    if isinstance(b, int):
        return 0 if b == 0 else (b * factor, jnp.zeros_like(factor))
    p = factor * b[0]
    e = product_error(p, split(factor), split(b[0]))
    return quick_two_sum(p, e + factor * b[1])


def solve_block(values, inverses, ratios, lower_planes):
    forward = []
    for k, current in enumerate(values):
        if k > 0:
            current = current + lower_planes[k] * forward[-1]
        forward.append(current * inverses[k])
    result = [forward[-1]]
    for k in range(len(values) - 2, -1, -1):
        result.insert(0, forward[k] - ratios[k] * result[0])
    return result


def pack_kernel(
    slabs, copies, ids_in, forces_in, weights_in, velocity_in, courant_in,
    message_out, fields_out, ids, forces, weights, arrived,
):
    moves = [
        pltpu.make_async_copy(source, target, arrived.at[n])
        for n, (source, target) in enumerate(
            [
                (ids_in, ids),
                (weights_in, weights),
                (forces_in, forces),
                (velocity_in, fields_out.at[0]),
                (courant_in, fields_out.at[1]),
            ]
        )
    ]
    for move in moves:
        move.start()
    for move in moves[:3]:
        move.wait()
    tile = ids.shape[1]
    width = 128
    high = ids[...] // width
    code = 1.0 + (ids[...] - high * width).astype(F32) * (1.0 / width)
    code = code * 2.0**LOWEST
    for k in range(7):
        code = code * jnp.where((high >> k) & 1 == 1, 2.0 ** (2**k), 1.0)
    for pair in range(0, slabs, 2):
        blocks = []
        for s in (pair, pair + 1):
            at = slice(s * tile, (s + 1) * tile)
            blocks.append(forces[:, at] * weights[s : s + 1])
        blocks.append(code[pair : pair + 2])
        block = jnp.concatenate(blocks, axis=0).astype(jnp.bfloat16)
        for k in range(2 * copies):
            message_out[pair * copies + k] = block
    for move in moves[3:]:
        move.wait()


def own_block():
    return lax.axis_index("slab") % 2


def edges_kernel(here, beside, first_out, last_out):
    rows = here.shape[3]
    own = own_block()
    for block in range(2):
        for n in range(2):
            for d in range(COMPS):
                for out, at in ((first_out, slice(0, DEPTH)), (last_out, slice(rows - DEPTH, rows))):
                    out[block, n * COMPS + d] = jnp.where(
                        own == block, here[n, d, :, at], beside[n, d, :, at]
                    )


def deposit_kernel(rows, copies, group, message, momentum_sum):
    wide = rows + 2 * DEPTH
    height = rows * copies
    planes = momentum_sum.shape[1] // (COMPS * wide)
    width = momentum_sum.shape[2]
    start = lax.axis_index("batch") * rows
    tile = message.shape[2]
    narrow = jnp.bfloat16
    count = lax.broadcasted_iota(jnp.int32, (16, tile), 0).astype(F32)
    counts = [(count + 16.0 * g).astype(narrow) for g in range(width // 16)]
    nothing = jnp.zeros((16, tile), narrow)
    one = jnp.ones((16, tile), narrow)

    def over_sixteen(row):
        return jnp.broadcast_to(row, (16, tile)).astype(narrow)

    def deposit(step):
        row_values, column_hot = [[], []], [[], []]
        for k in range(group):
            part = message[step * group + k].astype(F32)
            rest = part * 2.0**-LOWEST
            cell_row = jnp.zeros(part.shape, jnp.int32)
            for bit in range(6, -1, -1):
                more = rest >= 2.0 ** (2**bit)
                rest = jnp.where(more, rest * 2.0 ** -(2**bit), rest)
                cell_row = cell_row + jnp.where(more, 2**bit, 0)
            columns = (rest - 1.0) * width
            plane = jnp.zeros_like(cell_row)
            for p in range(1, planes):
                plane = plane + (cell_row >= p * height).astype(jnp.int32)
            away = cell_row - plane * height - start
            away = jnp.where(away < 0, away + height, away)
            spot = jnp.where(away < rows + DEPTH, away, away - height + wide)
            inside = (away < rows + DEPTH) | (away >= height - DEPTH)
            spots = jnp.where(inside, spot + plane * wide, -1).astype(F32)
            for block in range(2):
                at = 2 * COMPS + block
                spot = over_sixteen(spots[at : at + 1])
                column = over_sixteen(columns[at : at + 1])
                here = [counts[g] == spot for g in range(planes * wide // 16)]
                first = block * COMPS
                values = [over_sixteen(part[c : c + 1]) for c in range(first, first + COMPS)]
                row_values[block].append(
                    jnp.concatenate(
                        [jnp.where(at, value, nothing) for value in values for at in here], axis=0
                    )
                )
                column_hot[block].append(
                    jnp.concatenate([jnp.where(n == column, one, nothing) for n in counts], axis=0)
                )
        return [
            lax.dot_general(
                jnp.concatenate(row_values[block], axis=1),
                jnp.concatenate(column_hot[block], axis=1),
                (((1,), (1,)), ((), ())),
                preferred_element_type=F32,
            )
            for block in range(2)
        ]

    steps = message.shape[0] // group
    if steps <= 4:
        totals = deposit(0)
        for step in range(1, steps):
            totals = [x + y for x, y in zip(totals, deposit(step))]
        for block in range(2):
            momentum_sum[block] = totals[block]
    else:
        momentum_sum[...] = jnp.zeros(momentum_sum.shape, F32)

        def add_step(step, carry):
            for block, total in enumerate(deposit(step)):
                momentum_sum[block] += total
            return carry

        lax.fori_loop(0, steps, add_step, 0)


def fill_coefficients(courant, slab, slabs, batch, copies, rows, side, block):
    planes, wide, width = side.shape[1:]
    spots = lax.broadcasted_iota(jnp.int32, (wide, width), 0)
    lanes = lax.broadcasted_iota(jnp.int32, (wide, width), 1)
    at_top = (spots == rows - 1) & (batch == copies - 1)
    at_bottom = (spots == 0) & (batch == 0)
    ratio = None
    for k in range(planes):
        upper, lower = [], []
        for d in range(3):
            half = 0.5 * courant(d, k)
            upper.append(diffusion_number - half)
            lower.append(diffusion_number + half)
        side[0, k] = jnp.where(at_top, 0.0, upper[1])
        side[1, k] = jnp.where(at_bottom, 0.0, lower[1])
        side[2, k] = jnp.where(lanes == width - 1, 0.0, upper[2])
        side[3, k] = jnp.where(lanes == 0, 0.0, lower[2])
        if k == 0:
            pivot = jnp.full((wide, width), diagonal_value, F32)
            block[3, 0] = jnp.where(slab <= 0, 0.0, lower[0])
        else:
            pivot = diagonal_value + lower[0] * ratio
        if k == planes - 1:
            block[3, 1] = jnp.where(slab >= slabs - 1, 0.0, upper[0])
        inverse = 1.0 / pivot
        ratio = -upper[0] * inverse
        block[0, k] = inverse
        block[1, k] = ratio
        block[2, k] = lower[0]


def solve(values, block):
    planes = len(values)
    return solve_block(values, *([block[n, k] for k in range(planes)] for n in range(3)))


def in_plane(planes_here, side):
    wide, width = planes_here[0].shape
    values = []
    for k, here in enumerate(planes_here):
        total = side[0, k] * pltpu.roll(here, wide - 1, 0)
        total = total + side[1, k] * pltpu.roll(here, 1, 0)
        total = total + side[2, k] * pltpu.roll(here, width - 1, 1)
        total = total + side[3, k] * pltpu.roll(here, 1, 1)
        values.append(total)
    return values


def add_below(values, face, block):
    return [values[0] + block[3, 0] * face] + list(values[1:])


def add_above(values, face, block):
    return list(values[:-1]) + [values[-1] + block[3, 1] * face]


def inside_pair(lower, upper, side, block):
    return (
        add_above(in_plane(lower, side.at[0]), upper[0], block.at[0]),
        add_below(in_plane(upper, side.at[1]), lower[-1], block.at[1]),
    )


def store_pair(c, pair, out):
    for n, values in enumerate(pair):
        for k, item in enumerate(values):
            out[n, c, k] = item


def store_own(c, pair, out):
    own = own_block()
    for k, (one, other) in enumerate(zip(*pair)):
        out[c, k] = jnp.where(own == 0, one, other)


def store_messages(c, solved, inner, block, rows, near_out):
    even = lax.axis_index("batch") % 2 == 0
    wide = solved[0][0].shape[0]
    up = (solved[1][-1], solve(inner[1], block.at[1])[-1])
    down = (solved[0][0], solve(inner[0], block.at[0])[0])
    start = COMPS * wide + c * rows
    for n, (one, other) in enumerate(((up, down), (down, up))):
        near_out[n][c * wide : (c + 1) * wide] = jnp.where(even, one[0], other[0])
        near_out[n][start : start + rows] = jnp.where(even, one[1], other[1])[:rows]


def setup_kernel(
    slabs, copies,
    here, beside, after, before, momentum_sum,
    value_out, own_out, solved_out, inner_out, near1, near2, side, block, wide_courant,
):
    planes, rows, width = here.shape[2:]
    wide = rows + 2 * DEPTH
    batch = lax.axis_index("batch")
    even = batch % 2 == 0
    slab, own = lax.axis_index("slab"), own_block()
    for n in range(2):
        for d in range(3):
            for k in range(planes):
                wide_courant[n, d, k] = jnp.concatenate(
                    [
                        jnp.where(own == n, here[1, d, k], beside[1, d, k]),
                        after[n, COMPS + d, k],
                        before[n, COMPS + d, k],
                    ],
                    axis=0,
                )
        fill_coefficients(
            lambda d, k: wide_courant[n, d, k],
            slab - own + n, slabs, batch, copies, rows, side.at[n], block.at[n],
        )
    zero = jnp.zeros((wide, width), F32)
    from_below = solve([block[0, 3, 0]] + [zero] * (planes - 1), block.at[0])[0]
    from_above = solve([zero] * (planes - 1) + [block[1, 3, 1]], block.at[1])[-1]
    at = slice(2 * COMPS * wide, (2 * COMPS + 1) * wide)
    near1[at] = jnp.where(even, from_above, from_below)
    near2[at] = jnp.where(even, from_below, from_above)
    for c in range(COMPS):
        pair, solved = [], []
        for n in range(2):
            values = []
            for k in range(planes):
                old = jnp.concatenate(
                    [
                        jnp.where(own == n, here[0, c, k], beside[0, c, k]),
                        after[n, c, k],
                        before[n, c, k],
                    ],
                    axis=0,
                )
                at = (c * planes + k) * wide
                values.append(old + momentum_sum[n, at : at + wide])
            pair.append(values)
            solved.append(solve(values, block.at[n]))
        inner = inside_pair(*solved, side, block)
        store_own(c, pair, value_out)
        store_own(c, solved, own_out)
        store_pair(c, solved, solved_out)
        store_pair(c, inner, inner_out)
        store_messages(c, solved, inner, block, wide, (near1, near2))


def next_level(solved, inner, near1, near2, first1, first2, block):
    planes, wide = solved.shape[2:4]
    rows = near1.shape[0] // COMPS - wide
    if near1 is first1:
        rows = wide
    even = lax.axis_index("batch") % 2 == 0

    def low(one, other):
        return jnp.where(even, one, other)

    def high(one, other):
        return jnp.where(even, other, one)

    def part(pick, start, count):
        at = slice(start, start + count)
        return pick(near1[at], near2[at])

    at = slice(2 * COMPS * wide, 2 * COMPS * wide + rows)
    low_response, high_response = (pick(first1[at], first2[at]) for pick in (low, high))
    pad = jnp.zeros((wide - rows, solved.shape[4]), F32)

    def widen(x):
        return x if rows == wide else jnp.concatenate([x, pad], axis=0)

    for c in range(COMPS):
        own = COMPS * wide + c * rows
        lower = [inner[0, c, k] for k in range(planes)]
        upper = [inner[1, c, k] for k in range(planes)]
        one = (
            add_below(lower, part(low, c * wide, wide), block.at[0]),
            add_above(upper, part(high, c * wide, wide), block.at[1]),
        )
        one_solved = tuple(solve(one[n], block.at[n]) for n in range(2))
        below = part(low, own, rows) + low_response * solved[0, c, 0][:rows]
        above = part(high, own, rows) + high_response * solved[1, c, planes - 1][:rows]
        yield c, one, one_solved, widen(below), widen(above)


def advance_kernel(
    repeat, *refs,
):
    solved, inner, near1, near2, first1, first2, side, block = refs[:8]
    if repeat:
        first1, first2 = near1, near2
    value_out, own_out, second_out, last_out, solved_out, inner_out, to1, to2 = refs[8:]
    wide = solved.shape[3]
    rows = to1.shape[0] // COMPS - wide
    for c, one, one_solved, below, above in next_level(
        solved, inner, near1, near2, first1, first2, block
    ):
        within = inside_pair(*one_solved, side, block)
        two = (
            add_below(within[0], below, block.at[0]),
            add_above(within[1], above, block.at[1]),
        )
        two_solved = tuple(solve(two[n], block.at[n]) for n in range(2))
        inner_next = inside_pair(*two_solved, side, block)
        store_own(c, one, value_out)
        store_own(c, one_solved, own_out)
        store_own(c, two, second_out)
        store_own(c, two_solved, last_out)
        store_pair(c, two_solved, solved_out)
        store_pair(c, inner_next, inner_out)
        store_messages(c, two_solved, inner_next, block, rows, (to1, to2))


def gram_sums(pieces, pairs, totals):
    halves = [split(piece) for piece in pieces]
    for n, (i, j) in enumerate(pairs):
        p = pieces[i] * pieces[j]
        e = product_error(p, halves[i], halves[j])
        if totals[n] is None:
            totals[n] = (p, e)
        else:
            s, t = two_sum(totals[n][0], p)
            totals[n] = (s, totals[n][1] + (t + e))


def stack_sums(sums, count):
    flat = [sums[c][n] for n in range(len(sums[0])) for c in range(COMPS)]
    flat += [(jnp.zeros_like(flat[0][0]),) * 2] * (count - len(flat))
    rows_of = [sum_to_sublanes(flat[n : n + 8]) for n in range(0, count, 8)]
    return [jnp.concatenate([x[p] for x in rows_of], axis=0) for p in (0, 1)]


def early_kernel(rows, *refs):
    values, (high_out, low_out) = refs[:EARLY], refs[EARLY:]
    sums = []
    for c in range(COMPS):
        totals = [None] * len(EARLY_PAIRS)
        for k in range(values[0].shape[1]):
            for r in range(0, rows, 8):
                gram_sums([v[c, k, r : r + 8, :] for v in values], EARLY_PAIRS, totals)
        sums.append(totals)
    high_out[...], low_out[...] = stack_sums(sums, EARLY_ROWS)


def gram_kernel(*refs):
    solved, inner, near1, near2, first1, first2, side, block = refs[:8]
    values = refs[8 : 8 + EARLY]
    early = refs[8 + EARLY : 10 + EARLY]
    value_out, solved_out, second_out, message_out = refs[10 + EARLY :]
    own = own_block()
    planes, wide, width = value_out.shape[1:]
    rows = wide - 2 * DEPTH
    sums = []
    for c, ones, one_pair, below, above in next_level(
        solved, inner, near1, near2, first1, first2, block
    ):
        one, one_solved = (
            [jnp.where(own == 0, x, y) for x, y in zip(*pair)] for pair in (ones, one_pair)
        )
        two = in_plane(one_solved, side.at[own])
        two = add_below(two, jnp.where(own == 0, below, one_pair[0][-1]), block.at[own])
        two = add_above(two, jnp.where(own == 0, one_pair[1][0], above), block.at[own])
        totals = [None] * len(LATE_PAIRS)
        for k in range(planes):
            value_out[c, k] = one[k]
            solved_out[c, k] = one_solved[k]
            second_out[c, k] = two[k]
            for r in range(0, rows, 8):
                pieces = [value[c, k, r : r + 8, :] for value in values]
                gram_sums(pieces + [one[k][r : r + 8], two[k][r : r + 8]], LATE_PAIRS, totals)
        sums.append(totals)
    late = stack_sums(sums, width // 2 - EARLY_ROWS)
    turned = [jnp.transpose(jnp.concatenate([e[...], x], axis=0)) for e, x in zip(early, late)]
    total = tuple(x[:8] for x in turned)
    for r in range(8, width, 8):
        total = dd_add(total, tuple(x[r : r + 8] for x in turned))
    for shift in (4, 2, 1):
        total = dd_add(total, tuple(pltpu.roll(x, shift, 0) for x in total))
    row = jnp.concatenate([x[:1] for x in total], axis=1)
    message_out[...] = jnp.broadcast_to(row, message_out.shape)


def sum_to_sublanes(parts):
    sub = lax.broadcasted_iota(jnp.int32, parts[0][0].shape, 0)
    level = parts
    for shift in (4, 2, 1):
        keep = (sub & shift) == 0
        merged = []
        for a, b in zip(level[:shift], level[shift:]):
            stay = tuple(jnp.where(keep, x, y) for x, y in zip(a, b))
            swap = [jnp.where(keep, y, x) for x, y in zip(a, b)]
            moved = tuple(
                pltpu.roll(w, 4, 0)
                if shift == 4
                else jnp.where(keep, pltpu.roll(w, 8 - shift, 0), pltpu.roll(w, shift, 0))
                for w in swap
            )
            merged.append(dd_add(stay, moved))
        level = merged
    return level[0]


def finish_kernel(*refs):
    gathered = refs[0]
    values = refs[1 : 1 + BASIS]
    solved = refs[1 + BASIS : 1 + BASIS + DEPTH]
    solution_out, residual_out, solution_here, residual_here, sent = refs[1 + BASIS + DEPTH :]
    planes, rows, _ = solution_here.shape[1:]
    count, lanes = gathered.shape
    total = None
    for r in range(0, count, 8):
        high = gathered[r : r + 8]
        item = (high, pltpu.roll(high, lanes // 2, 1))
        total = item if total is None else dd_add(total, item)
    for shift in (4, 2, 1):
        total = dd_add(total, tuple(pltpu.roll(x, shift, 0) for x in total))
    sub = lax.broadcasted_iota(jnp.int32, (8, lanes), 0)

    def entry(n):
        start = n * COMPS
        if n >= len(EARLY_PAIRS):
            start = EARLY_ROWS + (n - len(EARLY_PAIRS)) * COMPS
        return tuple(pltpu.roll(x, (lanes - start) % lanes, 1) for x in total)

    entries = {pair: entry(n) for n, pair in enumerate(PAIRS)}
    gram = []
    for i in range(BASIS):
        row = None
        for j in range(BASIS):
            item = entries[(min(i, j), max(i, j))]
            if row is None:
                row = item
            else:
                row = tuple(jnp.where(sub == j, x, y) for x, y in zip(item, row))
        gram.append(row)
    zero = jnp.zeros((8, lanes), F32)

    def stack(poly):
        out = (zero, zero)
        for j, item in enumerate(poly):
            if isinstance(item, int):
                item = (zero + item, zero)
            out = tuple(jnp.where(sub == j, x, y) for x, y in zip(item, out))
        return out

    def over_sublanes(x):
        for shift in (4, 2, 1):
            x = dd_add(x, tuple(pltpu.roll(y, shift, 0) for y in x))
        return x

    def gram_times(poly):
        out = 0
        for i, item in enumerate(poly):
            out = dd_add(out, dd_mul(item, gram[i]))
        return tuple(jnp.where(sub < BASIS, x, 0.0) for x in out)

    def with_shadow(poly):
        terms = [dd_mul(item, entries[(0, i)]) for i, item in enumerate(poly)]
        while len(terms) > 1:
            pairs = [dd_add(*terms[i : i + 2]) for i in range(0, len(terms) - 1, 2)]
            terms = pairs + terms[len(pairs) * 2 :]
        return terms[0]

    def operate(poly):
        out = list(poly) + [0]
        return [out[0]] + [dd_sub(out[i], out[i - 1]) for i in range(1, len(out))]

    def combine(first, factor, second):
        out = []
        for i in range(max(len(first), len(second))):
            item = first[i] if i < len(first) else 0
            if i < len(second):
                item = dd_add(item, dd_scale(factor, second[i]))
            out.append(item)
        return out

    def rounded(poly):
        return [zero + item if isinstance(item, int) else item[0] for item in poly]

    residual = [1]
    direction = [1]
    rho = entries[(0, 0)]
    steps = []
    for iteration in range(ITERS):
        image = operate(direction)
        alpha = rho[0] / with_shadow(image)[0]
        middle = combine(residual, -alpha, image)
        turned = operate(middle)
        weighted = gram_times(turned)
        cross = over_sublanes(dd_mul(weighted, stack(middle)))
        square = over_sublanes(dd_mul(weighted, stack(turned)))
        omega = cross[0] / square[0]
        steps += [(alpha, rounded(direction)), (omega, rounded(middle))]
        residual = combine(middle, -omega, turned)
        if iteration + 1 < ITERS:
            rho_next = with_shadow(residual)
            factor = (rho_next[0] / rho[0]) * (alpha / omega)
            direction = combine(direction, -omega, image)
            direction = combine(residual, factor, direction)
            rho = rho_next
    residual = rounded(residual)
    answer = []
    for step, poly in steps:
        for i, item in enumerate(poly):
            if i == len(answer):
                answer.append(step * item)
            else:
                answer[i] = answer[i] + step * item
    moves = []
    for c in range(COMPS):
        for n, (poly, basis, here, out) in enumerate(
            (
                (answer, solved, solution_here, solution_out),
                (residual, values, residual_here, residual_out),
            )
        ):
            scales = [item[:, c : c + 1] for item in poly]
            for k in range(planes):
                for r in range(0, rows, 8):
                    total = scales[0] * basis[0][c, k, r : r + 8, :]
                    for i in range(1, len(scales)):
                        total = total + scales[i] * basis[i][c, k, r : r + 8, :]
                    here[c, k, r : r + 8, :] = total
            moves.append(pltpu.make_async_copy(here.at[c], out.at[c], sent.at[n * COMPS + c]))
            moves[-1].start()
    for move in moves:
        move.wait()


def ring(array, axis, step):
    count = lax.axis_size(axis)
    return lax.ppermute(array, axis, [(i, (i + step) % count) for i in range(count)])


def race(array, step):
    slabs, copies = lax.axis_size("slab"), lax.axis_size("batch")
    pairs = []
    for s in range(slabs):
        for b in range(copies):
            t = s + abs(step) if b % 2 == 0 else s - abs(step)
            target = t * copies + b if 0 <= t < slabs else s * copies + (b ^ 1)
            pairs.append((s * copies + b, target))
    if step < 0:
        pairs = [(t, s) for s, t in pairs]
    return lax.ppermute(array, ("slab", "batch"), sorted(pairs))


def local(velocity_old, courant, cell_ids, forces, weights):
    planes, rows, width = velocity_old.shape[1:]
    slabs, copies = lax.axis_size("slab"), lax.axis_size("batch")
    everyone = ("slab", "batch")
    wide = rows + 2 * DEPTH
    height = rows * copies
    tile = cell_ids.shape[0] // slabs
    assert rows % 8 == 0 and width == 128 and copies % 2 == 0 and slabs % 2 == 0
    assert planes * height <= 128 and 2 * DEPTH <= height - rows
    field = jax.ShapeDtypeStruct((COMPS, planes, wide, width), F32)
    quad = jax.ShapeDtypeStruct((2, 4, planes, wide, width), F32)
    both = jax.ShapeDtypeStruct((2, COMPS, planes, wide, width), F32)
    edge = jax.ShapeDtypeStruct((2, 2 * COMPS, planes, DEPTH, width), F32)
    own = jax.ShapeDtypeStruct(velocity_old.shape, F32)

    def call(kernel, out_shape, in_specs, mib, scratch=(), out_space=VMEM, cost=None):
        if cost is not None:
            cost = pl.CostEstimate(flops=cost, bytes_accessed=0, transcendentals=0)
        return pl.pallas_call(
            kernel,
            out_shape=out_shape,
            in_specs=in_specs,
            out_specs=[out_space] * len(out_shape),
            cost_estimate=cost,
            scratch_shapes=list(scratch),
            compiler_params=pltpu.CompilerParams(vmem_limit_bytes=mib << 20),
        )

    def pack(*refs):
        pack_kernel(slabs, copies, *refs)

    message, fields = call(
        pack,
        (
            jax.ShapeDtypeStruct((slabs * copies, 2 * (COMPS + 1), tile), jnp.bfloat16),
            jax.ShapeDtypeStruct((2, *velocity_old.shape), F32),
        ),
        [ANY] * 5,
        8,
        [
            pltpu.VMEM((slabs, tile), jnp.int32),
            pltpu.VMEM(forces.shape, F32),
            pltpu.VMEM((slabs, tile), F32),
            pltpu.SemaphoreType.DMA((5,)),
        ],
    )(
        *(
            pltpu.with_memory_space_constraint(x, pltpu.HBM)
            for x in (
                cell_ids.reshape(slabs, tile),
                forces,
                weights.reshape(slabs, tile),
                velocity_old,
                courant,
            )
        )
    )
    beside = lax.ppermute(fields, "slab", [(s, s ^ 1) for s in range(slabs)])
    received = lax.all_to_all(message, everyone, 0, 0, tiled=True)
    first, last = call(edges_kernel, (edge, edge), [VMEM] * 2, 2)(fields, beside)
    after = ring(first, "batch", -1)
    before = ring(last, "batch", 1)

    def deposit(*refs):
        deposit_kernel(rows, copies, 8, *refs)

    (deposited,) = call(
        deposit, (jax.ShapeDtypeStruct((2, COMPS * planes * wide, width), F32),), [VMEM], 12
    )(received)

    def setup(*refs):
        setup_kernel(slabs, copies, *refs)

    def flat(count):
        return jax.ShapeDtypeStruct((count, width), F32)

    value, own_solved, solved, inner, *sent, side, block = call(
        setup,
        (field,) * 2 + (both,) * 2 + (flat((2 * COMPS + 1) * wide),) * 2 + (quad,) * 2,
        [VMEM] * 5,
        2,
        [pltpu.VMEM((2, 3, planes, wide, width), F32)],
    )(fields, beside, after, before, deposited)

    values, solves = [value], [own_solved]
    first = None
    for iteration in range(ITERS):
        near = [race(sent[0], 2), race(sent[1], -2)]
        repeat = first is None
        first = first or near
        known = (solved, inner, *near, *first, side, block)
        if iteration + 1 < ITERS:
            reach = wide if iteration + 2 < ITERS else rows

            def advance(*refs):
                advance_kernel(repeat, *refs)

            value, one_solved, second, last_solved, solved, inner, *sent = call(
                advance,
                (field,) * 4 + (both,) * 2 + (flat(COMPS * (wide + reach)),) * 2,
                [VMEM] * 8,
                3,
            )(*known)
            solves += [one_solved, last_solved]
        else:

            def early(*refs):
                early_kernel(rows, *refs)

            sums = call(early, (flat(EARLY_ROWS),) * 2, [VMEM] * EARLY, 2, cost=4000000)(*values)
            value, one_solved, second, message = call(
                gram_kernel, (field,) * 3 + (flat(slabs * copies),), [VMEM] * (10 + EARLY), 4
            )(*known, *values, *sums)
            solves += [one_solved]
        values += [value, second]
    gathered = lax.all_to_all(message, everyone, 0, 0, tiled=True)
    return call(
        finish_kernel,
        (own, own),
        [VMEM] * (1 + BASIS + DEPTH),
        4,
        [pltpu.VMEM(own.shape, F32)] * 2 + [pltpu.SemaphoreType.DMA((2 * COMPS,))],
        ANY,
    )(gathered, *values, *solves)


def solution(mesh):
    placed = (
        P(None, "slab", "batch", None),
        P(None, "slab", "batch", None),
        P(("slab", "batch")),
        P(None, ("slab", "batch")),
        P(("slab", "batch")),
    )
    return jax.shard_map(
        local,
        mesh=mesh,
        in_specs=placed,
        out_specs=(P(None, "slab", "batch", None), P(None, "slab", "batch", None)),
        check_vma=False,
    )
```

```python
import jax
import jax.numpy as jnp
from jax import lax
from jax.experimental import pallas as pl
from jax.experimental.pallas import tpu as pltpu
from jax.sharding import PartitionSpec as P


ITERS = 2
DEPTH = 2 * ITERS
COMPS = 3
BASIS = DEPTH + 1
EARLY = DEPTH - 1
LOWEST = -63
PAIRS = sorted(((i, j) for j in range(BASIS) for i in range(j + 1)), key=lambda p: p[1] >= EARLY)
EARLY_PAIRS = [p for p in PAIRS if p[1] < EARLY]
LATE_PAIRS = [p for p in PAIRS if p[1] >= EARLY]
EARLY_ROWS = -(-len(EARLY_PAIRS) * COMPS // 8) * 8

diffusion_number = 1.0
diagonal_value = 7.0

VMEM = pl.BlockSpec(memory_space=pltpu.VMEM)
ANY = pl.BlockSpec(memory_space=pl.ANY)
F32 = jnp.float32


def two_sum(a, b):
    s = a + b
    bb = s - a
    return s, (a - (s - bb)) + (b - bb)


def quick_two_sum(a, b):
    s = a + b
    return s, b - (s - a)


def split(a):
    t = a * 4097.0
    high = t - (t - a)
    return high, a - high


def product_error(p, a, b):
    ah, al = a
    bh, bl = b
    return ((ah * bh - p) + ah * bl + al * bh) + al * bl


def dd_add(a, b):
    if isinstance(b, int):
        a, b = b, a
    if isinstance(a, int):
        if isinstance(b, int):
            return a + b
        if a == 0:
            return b
        a = (jnp.full_like(b[0], a), jnp.zeros_like(b[0]))
    s, e = two_sum(a[0], b[0])
    return quick_two_sum(s, e + (a[1] + b[1]))


def dd_neg(a):
    return -a if isinstance(a, int) else (-a[0], -a[1])


def dd_sub(a, b):
    return dd_add(a, dd_neg(b))


def dd_mul(a, b):
    if isinstance(b, int):
        a, b = b, a
    if isinstance(a, int):
        if isinstance(b, int):
            return a * b
        return {0: 0, 1: b, -1: dd_neg(b)}[a]
    p = a[0] * b[0]
    e = product_error(p, split(a[0]), split(b[0]))
    return quick_two_sum(p, e + (a[0] * b[1] + a[1] * b[0]))


def dd_scale(factor, b):
    if isinstance(b, int):
        return 0 if b == 0 else (b * factor, jnp.zeros_like(factor))
    p = factor * b[0]
    e = product_error(p, split(factor), split(b[0]))
    return quick_two_sum(p, e + factor * b[1])


def solve_block(values, inverses, ratios, lower_planes):
    forward = []
    for k, current in enumerate(values):
        if k > 0:
            current = current + lower_planes[k] * forward[-1]
        forward.append(current * inverses[k])
    result = [forward[-1]]
    for k in range(len(values) - 2, -1, -1):
        result.insert(0, forward[k] - ratios[k] * result[0])
    return result


def pack_kernel(
    slabs, copies, ids_in, forces_in, weights_in, velocity_in, courant_in,
    message_out, fields_out, ids, forces, weights, arrived, message, sent,
):
    moves = [
        pltpu.make_async_copy(source, target, arrived.at[n])
        for n, (source, target) in enumerate(
            [
                (ids_in, ids),
                (weights_in, weights),
                (forces_in, forces),
                (velocity_in, fields_out.at[0]),
                (courant_in, fields_out.at[1]),
            ]
        )
    ]
    for move in moves:
        move.start()
    for move in moves[:3]:
        move.wait()
    tile = ids.shape[1]
    width = 128
    high = ids[...] // width
    code = 1.0 + (ids[...] - high * width).astype(F32) * (1.0 / width)
    code = code * 2.0**LOWEST
    for k in range(7):
        code = code * jnp.where((high >> k) & 1 == 1, 2.0 ** (2**k), 1.0)
    leaving = []
    for pair in range(0, slabs, 2):
        blocks = []
        for s in (pair, pair + 1):
            at = slice(s * tile, (s + 1) * tile)
            blocks.append(forces[:, at] * weights[s : s + 1])
        blocks.append(code[pair : pair + 2])
        block = jnp.concatenate(blocks, axis=0).astype(jnp.bfloat16)
        at = pl.ds(pair * copies, 2 * copies)
        for k in range(2 * copies):
            message[pair * copies + k] = block
        leave = pltpu.make_async_copy(message.at[at], message_out.at[at], sent.at[pair // 2])
        leave.start()
        leaving.append(leave)
    for move in moves[3:] + leaving:
        move.wait()


def own_block():
    return lax.axis_index("slab") % 2


def edges_kernel(here, beside, first_out, last_out):
    rows = here.shape[3]
    own = own_block()
    for block in range(2):
        for n in range(2):
            for d in range(COMPS):
                for out, at in ((first_out, slice(0, DEPTH)), (last_out, slice(rows - DEPTH, rows))):
                    out[block, n * COMPS + d] = jnp.where(
                        own == block, here[n, d, :, at], beside[n, d, :, at]
                    )


def deposit_kernel(rows, copies, group, message, momentum_sum):
    wide = rows + 2 * DEPTH
    height = rows * copies
    planes = momentum_sum.shape[1] // (COMPS * wide)
    width = momentum_sum.shape[2]
    start = lax.axis_index("batch") * rows
    tile = message.shape[2]
    narrow = jnp.bfloat16
    count = lax.broadcasted_iota(jnp.int32, (16, tile), 0).astype(F32)
    counts = [(count + 16.0 * g).astype(narrow) for g in range(width // 16)]
    nothing = jnp.zeros((16, tile), narrow)
    one = jnp.ones((16, tile), narrow)

    def over_sixteen(row):
        return jnp.broadcast_to(row, (16, tile)).astype(narrow)

    def deposit(step):
        row_values, column_hot = [[], []], [[], []]
        for k in range(group):
            part = message[step * group + k].astype(F32)
            rest = part * 2.0**-LOWEST
            cell_row = jnp.zeros(part.shape, jnp.int32)
            for bit in range(6, -1, -1):
                more = rest >= 2.0 ** (2**bit)
                rest = jnp.where(more, rest * 2.0 ** -(2**bit), rest)
                cell_row = cell_row + jnp.where(more, 2**bit, 0)
            columns = (rest - 1.0) * width
            plane = jnp.zeros_like(cell_row)
            for p in range(1, planes):
                plane = plane + (cell_row >= p * height).astype(jnp.int32)
            away = cell_row - plane * height - start
            away = jnp.where(away < 0, away + height, away)
            spot = jnp.where(away < rows + DEPTH, away, away - height + wide)
            inside = (away < rows + DEPTH) | (away >= height - DEPTH)
            spots = jnp.where(inside, spot + plane * wide, -1).astype(F32)
            for block in range(2):
                at = 2 * COMPS + block
                spot = over_sixteen(spots[at : at + 1])
                column = over_sixteen(columns[at : at + 1])
                here = [counts[g] == spot for g in range(planes * wide // 16)]
                first = block * COMPS
                values = [over_sixteen(part[c : c + 1]) for c in range(first, first + COMPS)]
                row_values[block].append(
                    jnp.concatenate(
                        [jnp.where(at, value, nothing) for value in values for at in here], axis=0
                    )
                )
                column_hot[block].append(
                    jnp.concatenate([jnp.where(n == column, one, nothing) for n in counts], axis=0)
                )
        return [
            lax.dot_general(
                jnp.concatenate(row_values[block], axis=1),
                jnp.concatenate(column_hot[block], axis=1),
                (((1,), (1,)), ((), ())),
                preferred_element_type=F32,
            )
            for block in range(2)
        ]

    steps = message.shape[0] // group
    if steps <= 4:
        totals = deposit(0)
        for step in range(1, steps):
            totals = [x + y for x, y in zip(totals, deposit(step))]
        for block in range(2):
            momentum_sum[block] = totals[block]
    else:
        momentum_sum[...] = jnp.zeros(momentum_sum.shape, F32)

        def add_step(step, carry):
            for block, total in enumerate(deposit(step)):
                momentum_sum[block] += total
            return carry

        lax.fori_loop(0, steps, add_step, 0)


def fill_coefficients(courant, slab, slabs, batch, copies, rows, side, block):
    planes, wide, width = side.shape[1:]
    spots = lax.broadcasted_iota(jnp.int32, (wide, width), 0)
    lanes = lax.broadcasted_iota(jnp.int32, (wide, width), 1)
    at_top = (spots == rows - 1) & (batch == copies - 1)
    at_bottom = (spots == 0) & (batch == 0)
    ratio = None
    for k in range(planes):
        upper, lower = [], []
        for d in range(3):
            half = 0.5 * courant(d, k)
            upper.append(diffusion_number - half)
            lower.append(diffusion_number + half)
        side[0, k] = jnp.where(at_top, 0.0, upper[1])
        side[1, k] = jnp.where(at_bottom, 0.0, lower[1])
        side[2, k] = jnp.where(lanes == width - 1, 0.0, upper[2])
        side[3, k] = jnp.where(lanes == 0, 0.0, lower[2])
        if k == 0:
            pivot = jnp.full((wide, width), diagonal_value, F32)
            block[3, 0] = jnp.where(slab <= 0, 0.0, lower[0])
        else:
            pivot = diagonal_value + lower[0] * ratio
        if k == planes - 1:
            block[3, 1] = jnp.where(slab >= slabs - 1, 0.0, upper[0])
        inverse = 1.0 / pivot
        ratio = -upper[0] * inverse
        block[0, k] = inverse
        block[1, k] = ratio
        block[2, k] = lower[0]


def solve(values, block):
    planes = len(values)
    return solve_block(values, *([block[n, k] for k in range(planes)] for n in range(3)))


def in_plane(planes_here, side):
    wide, width = planes_here[0].shape
    values = []
    for k, here in enumerate(planes_here):
        total = side[0, k] * pltpu.roll(here, wide - 1, 0)
        total = total + side[1, k] * pltpu.roll(here, 1, 0)
        total = total + side[2, k] * pltpu.roll(here, width - 1, 1)
        total = total + side[3, k] * pltpu.roll(here, 1, 1)
        values.append(total)
    return values


def add_below(values, face, block):
    return [values[0] + block[3, 0] * face] + list(values[1:])


def add_above(values, face, block):
    return list(values[:-1]) + [values[-1] + block[3, 1] * face]


def inside_pair(lower, upper, side, block):
    return (
        add_above(in_plane(lower, side.at[0]), upper[0], block.at[0]),
        add_below(in_plane(upper, side.at[1]), lower[-1], block.at[1]),
    )


def store_pair(c, pair, out):
    for n, values in enumerate(pair):
        for k, item in enumerate(values):
            out[n, c, k] = item


def store_own(c, pair, out):
    own = own_block()
    for k, (one, other) in enumerate(zip(*pair)):
        out[c, k] = jnp.where(own == 0, one, other)


def store_messages(c, solved, inner, block, rows, near_out):
    even = lax.axis_index("batch") % 2 == 0
    wide = solved[0][0].shape[0]
    up = (solved[1][-1], solve(inner[1], block.at[1])[-1])
    down = (solved[0][0], solve(inner[0], block.at[0])[0])
    start = COMPS * wide + c * rows
    for n, (one, other) in enumerate(((up, down), (down, up))):
        near_out[n][c * wide : (c + 1) * wide] = jnp.where(even, one[0], other[0])
        near_out[n][start : start + rows] = jnp.where(even, one[1], other[1])[:rows]


def setup_kernel(
    slabs, copies,
    here, beside, after, before, momentum_sum,
    value_out, own_out, solved_out, inner_out, near1, near2, side, block, wide_courant,
):
    planes, rows, width = here.shape[2:]
    wide = rows + 2 * DEPTH
    batch = lax.axis_index("batch")
    even = batch % 2 == 0
    slab, own = lax.axis_index("slab"), own_block()
    for n in range(2):
        for d in range(3):
            for k in range(planes):
                wide_courant[n, d, k] = jnp.concatenate(
                    [
                        jnp.where(own == n, here[1, d, k], beside[1, d, k]),
                        after[n, COMPS + d, k],
                        before[n, COMPS + d, k],
                    ],
                    axis=0,
                )
        fill_coefficients(
            lambda d, k: wide_courant[n, d, k],
            slab - own + n, slabs, batch, copies, rows, side.at[n], block.at[n],
        )
    zero = jnp.zeros((wide, width), F32)
    from_below = solve([block[0, 3, 0]] + [zero] * (planes - 1), block.at[0])[0]
    from_above = solve([zero] * (planes - 1) + [block[1, 3, 1]], block.at[1])[-1]
    at = slice(2 * COMPS * wide, (2 * COMPS + 1) * wide)
    near1[at] = jnp.where(even, from_above, from_below)
    near2[at] = jnp.where(even, from_below, from_above)
    for c in range(COMPS):
        pair, solved = [], []
        for n in range(2):
            values = []
            for k in range(planes):
                old = jnp.concatenate(
                    [
                        jnp.where(own == n, here[0, c, k], beside[0, c, k]),
                        after[n, c, k],
                        before[n, c, k],
                    ],
                    axis=0,
                )
                at = (c * planes + k) * wide
                values.append(old + momentum_sum[n, at : at + wide])
            pair.append(values)
            solved.append(solve(values, block.at[n]))
        inner = inside_pair(*solved, side, block)
        store_own(c, pair, value_out)
        store_own(c, solved, own_out)
        store_pair(c, solved, solved_out)
        store_pair(c, inner, inner_out)
        store_messages(c, solved, inner, block, wide, (near1, near2))


def next_level(solved, inner, near1, near2, first1, first2, block):
    planes, wide = solved.shape[2:4]
    rows = near1.shape[0] // COMPS - wide
    if near1 is first1:
        rows = wide
    even = lax.axis_index("batch") % 2 == 0

    def low(one, other):
        return jnp.where(even, one, other)

    def high(one, other):
        return jnp.where(even, other, one)

    def part(pick, start, count):
        at = slice(start, start + count)
        return pick(near1[at], near2[at])

    at = slice(2 * COMPS * wide, 2 * COMPS * wide + rows)
    low_response, high_response = (pick(first1[at], first2[at]) for pick in (low, high))
    pad = jnp.zeros((wide - rows, solved.shape[4]), F32)

    def widen(x):
        return x if rows == wide else jnp.concatenate([x, pad], axis=0)

    for c in range(COMPS):
        own = COMPS * wide + c * rows
        lower = [inner[0, c, k] for k in range(planes)]
        upper = [inner[1, c, k] for k in range(planes)]
        one = (
            add_below(lower, part(low, c * wide, wide), block.at[0]),
            add_above(upper, part(high, c * wide, wide), block.at[1]),
        )
        one_solved = tuple(solve(one[n], block.at[n]) for n in range(2))
        below = part(low, own, rows) + low_response * solved[0, c, 0][:rows]
        above = part(high, own, rows) + high_response * solved[1, c, planes - 1][:rows]
        yield c, one, one_solved, widen(below), widen(above)


def advance_kernel(
    repeat, *refs,
):
    solved, inner, near1, near2, first1, first2, side, block = refs[:8]
    if repeat:
        first1, first2 = near1, near2
    value_out, own_out, second_out, last_out, solved_out, inner_out, to1, to2 = refs[8:]
    wide = solved.shape[3]
    rows = to1.shape[0] // COMPS - wide
    for c, one, one_solved, below, above in next_level(
        solved, inner, near1, near2, first1, first2, block
    ):
        within = inside_pair(*one_solved, side, block)
        two = (
            add_below(within[0], below, block.at[0]),
            add_above(within[1], above, block.at[1]),
        )
        two_solved = tuple(solve(two[n], block.at[n]) for n in range(2))
        inner_next = inside_pair(*two_solved, side, block)
        store_own(c, one, value_out)
        store_own(c, one_solved, own_out)
        store_own(c, two, second_out)
        store_own(c, two_solved, last_out)
        store_pair(c, two_solved, solved_out)
        store_pair(c, inner_next, inner_out)
        store_messages(c, two_solved, inner_next, block, rows, (to1, to2))


def gram_sums(pieces, pairs, totals):
    halves = [split(piece) for piece in pieces]
    for n, (i, j) in enumerate(pairs):
        p = pieces[i] * pieces[j]
        e = product_error(p, halves[i], halves[j])
        if totals[n] is None:
            totals[n] = (p, e)
        else:
            s, t = two_sum(totals[n][0], p)
            totals[n] = (s, totals[n][1] + (t + e))


def stack_sums(sums, count):
    flat = [sums[c][n] for n in range(len(sums[0])) for c in range(COMPS)]
    flat += [(jnp.zeros_like(flat[0][0]),) * 2] * (count - len(flat))
    rows_of = [sum_to_sublanes(flat[n : n + 8]) for n in range(0, count, 8)]
    return [jnp.concatenate([x[p] for x in rows_of], axis=0) for p in (0, 1)]


def early_kernel(rows, *refs):
    values, (high_out, low_out) = refs[:EARLY], refs[EARLY:]
    sums = []
    for c in range(COMPS):
        totals = [None] * len(EARLY_PAIRS)
        for k in range(values[0].shape[1]):
            for r in range(0, rows, 8):
                gram_sums([v[c, k, r : r + 8, :] for v in values], EARLY_PAIRS, totals)
        sums.append(totals)
    high_out[...], low_out[...] = stack_sums(sums, EARLY_ROWS)


def gram_kernel(*refs):
    solved, inner, near1, near2, first1, first2, side, block = refs[:8]
    values = refs[8 : 8 + EARLY]
    early = refs[8 + EARLY : 10 + EARLY]
    value_out, solved_out, second_out, message_out = refs[10 + EARLY :]
    own = own_block()
    planes, wide, width = value_out.shape[1:]
    rows = wide - 2 * DEPTH
    sums = []
    for c, ones, one_pair, below, above in next_level(
        solved, inner, near1, near2, first1, first2, block
    ):
        one, one_solved = (
            [jnp.where(own == 0, x, y) for x, y in zip(*pair)] for pair in (ones, one_pair)
        )
        two = in_plane(one_solved, side.at[own])
        two = add_below(two, jnp.where(own == 0, below, one_pair[0][-1]), block.at[own])
        two = add_above(two, jnp.where(own == 0, one_pair[1][0], above), block.at[own])
        totals = [None] * len(LATE_PAIRS)
        for k in range(planes):
            value_out[c, k] = one[k]
            solved_out[c, k] = one_solved[k]
            second_out[c, k] = two[k]
            for r in range(0, rows, 8):
                pieces = [value[c, k, r : r + 8, :] for value in values]
                gram_sums(pieces + [one[k][r : r + 8], two[k][r : r + 8]], LATE_PAIRS, totals)
        sums.append(totals)
    late = stack_sums(sums, width // 2 - EARLY_ROWS)
    turned = [jnp.transpose(jnp.concatenate([e[...], x], axis=0)) for e, x in zip(early, late)]
    total = tuple(x[:8] for x in turned)
    for r in range(8, width, 8):
        total = dd_add(total, tuple(x[r : r + 8] for x in turned))
    for shift in (4, 2, 1):
        total = dd_add(total, tuple(pltpu.roll(x, shift, 0) for x in total))
    row = jnp.concatenate([x[:1] for x in total], axis=1)
    message_out[...] = jnp.broadcast_to(row, message_out.shape)


def sum_to_sublanes(parts):
    sub = lax.broadcasted_iota(jnp.int32, parts[0][0].shape, 0)
    level = parts
    for shift in (4, 2, 1):
        keep = (sub & shift) == 0
        merged = []
        for a, b in zip(level[:shift], level[shift:]):
            stay = tuple(jnp.where(keep, x, y) for x, y in zip(a, b))
            swap = [jnp.where(keep, y, x) for x, y in zip(a, b)]
            moved = tuple(
                pltpu.roll(w, 4, 0)
                if shift == 4
                else jnp.where(keep, pltpu.roll(w, 8 - shift, 0), pltpu.roll(w, shift, 0))
                for w in swap
            )
            merged.append(dd_add(stay, moved))
        level = merged
    return level[0]


def finish_kernel(*refs):
    gathered = refs[0]
    values = refs[1 : 1 + BASIS]
    solved = refs[1 + BASIS : 1 + BASIS + DEPTH]
    solution_out, residual_out, solution_here, residual_here, sent = refs[1 + BASIS + DEPTH :]
    planes, rows, _ = solution_here.shape[1:]
    count, lanes = gathered.shape
    total = None
    for r in range(0, count, 8):
        high = gathered[r : r + 8]
        item = (high, pltpu.roll(high, lanes // 2, 1))
        total = item if total is None else dd_add(total, item)
    for shift in (4, 2, 1):
        total = dd_add(total, tuple(pltpu.roll(x, shift, 0) for x in total))
    sub = lax.broadcasted_iota(jnp.int32, (8, lanes), 0)

    def entry(n):
        start = n * COMPS
        if n >= len(EARLY_PAIRS):
            start = EARLY_ROWS + (n - len(EARLY_PAIRS)) * COMPS
        return tuple(pltpu.roll(x, (lanes - start) % lanes, 1) for x in total)

    entries = {pair: entry(n) for n, pair in enumerate(PAIRS)}
    gram = []
    for i in range(BASIS):
        row = None
        for j in range(BASIS):
            item = entries[(min(i, j), max(i, j))]
            if row is None:
                row = item
            else:
                row = tuple(jnp.where(sub == j, x, y) for x, y in zip(item, row))
        gram.append(row)
    zero = jnp.zeros((8, lanes), F32)

    def stack(poly):
        out = (zero, zero)
        for j, item in enumerate(poly):
            if isinstance(item, int):
                item = (zero + item, zero)
            out = tuple(jnp.where(sub == j, x, y) for x, y in zip(item, out))
        return out

    def over_sublanes(x):
        for shift in (4, 2, 1):
            x = dd_add(x, tuple(pltpu.roll(y, shift, 0) for y in x))
        return x

    def gram_times(poly):
        out = 0
        for i, item in enumerate(poly):
            out = dd_add(out, dd_mul(item, gram[i]))
        return tuple(jnp.where(sub < BASIS, x, 0.0) for x in out)

    def with_shadow(poly):
        terms = [dd_mul(item, entries[(0, i)]) for i, item in enumerate(poly)]
        while len(terms) > 1:
            pairs = [dd_add(*terms[i : i + 2]) for i in range(0, len(terms) - 1, 2)]
            terms = pairs + terms[len(pairs) * 2 :]
        return terms[0]

    def operate(poly):
        out = list(poly) + [0]
        return [out[0]] + [dd_sub(out[i], out[i - 1]) for i in range(1, len(out))]

    def combine(first, factor, second):
        out = []
        for i in range(max(len(first), len(second))):
            item = first[i] if i < len(first) else 0
            if i < len(second):
                item = dd_add(item, dd_scale(factor, second[i]))
            out.append(item)
        return out

    def rounded(poly):
        return [zero + item if isinstance(item, int) else item[0] for item in poly]

    residual = [1]
    direction = [1]
    rho = entries[(0, 0)]
    steps = []
    for iteration in range(ITERS):
        image = operate(direction)
        alpha = rho[0] / with_shadow(image)[0]
        middle = combine(residual, -alpha, image)
        turned = operate(middle)
        weighted = gram_times(turned)
        cross = over_sublanes(dd_mul(weighted, stack(middle)))
        square = over_sublanes(dd_mul(weighted, stack(turned)))
        omega = cross[0] / square[0]
        steps += [(alpha, rounded(direction)), (omega, rounded(middle))]
        residual = combine(middle, -omega, turned)
        if iteration + 1 < ITERS:
            rho_next = with_shadow(residual)
            factor = (rho_next[0] / rho[0]) * (alpha / omega)
            direction = combine(direction, -omega, image)
            direction = combine(residual, factor, direction)
            rho = rho_next
    residual = rounded(residual)
    answer = []
    for step, poly in steps:
        for i, item in enumerate(poly):
            if i == len(answer):
                answer.append(step * item)
            else:
                answer[i] = answer[i] + step * item
    moves = []
    for c in range(COMPS):
        for n, (poly, basis, here, out) in enumerate(
            (
                (answer, solved, solution_here, solution_out),
                (residual, values, residual_here, residual_out),
            )
        ):
            scales = [item[:, c : c + 1] for item in poly]
            for k in range(planes):
                for r in range(0, rows, 8):
                    total = scales[0] * basis[0][c, k, r : r + 8, :]
                    for i in range(1, len(scales)):
                        total = total + scales[i] * basis[i][c, k, r : r + 8, :]
                    here[c, k, r : r + 8, :] = total
            moves.append(pltpu.make_async_copy(here.at[c], out.at[c], sent.at[n * COMPS + c]))
            moves[-1].start()
    for move in moves:
        move.wait()


def ring(array, axis, step):
    count = lax.axis_size(axis)
    return lax.ppermute(array, axis, [(i, (i + step) % count) for i in range(count)])


def race(array, step):
    slabs, copies = lax.axis_size("slab"), lax.axis_size("batch")
    pairs = []
    for s in range(slabs):
        for b in range(copies):
            t = s + abs(step) if b % 2 == 0 else s - abs(step)
            target = t * copies + b if 0 <= t < slabs else s * copies + (b ^ 1)
            pairs.append((s * copies + b, target))
    if step < 0:
        pairs = [(t, s) for s, t in pairs]
    return lax.ppermute(array, ("slab", "batch"), sorted(pairs))


def local(velocity_old, courant, cell_ids, forces, weights):
    planes, rows, width = velocity_old.shape[1:]
    slabs, copies = lax.axis_size("slab"), lax.axis_size("batch")
    everyone = ("slab", "batch")
    wide = rows + 2 * DEPTH
    height = rows * copies
    tile = cell_ids.shape[0] // slabs
    assert rows % 8 == 0 and width == 128 and copies % 2 == 0 and slabs % 2 == 0
    assert planes * height <= 128 and 2 * DEPTH <= height - rows
    field = jax.ShapeDtypeStruct((COMPS, planes, wide, width), F32)
    quad = jax.ShapeDtypeStruct((2, 4, planes, wide, width), F32)
    both = jax.ShapeDtypeStruct((2, COMPS, planes, wide, width), F32)
    edge = jax.ShapeDtypeStruct((2, 2 * COMPS, planes, DEPTH, width), F32)
    own = jax.ShapeDtypeStruct(velocity_old.shape, F32)

    def call(kernel, out_shape, in_specs, mib, scratch=(), out_space=VMEM, cost=None):
        if cost is not None:
            cost = pl.CostEstimate(flops=cost, bytes_accessed=0, transcendentals=0)
        return pl.pallas_call(
            kernel,
            out_shape=out_shape,
            in_specs=in_specs,
            out_specs=out_space if isinstance(out_space, list) else [out_space] * len(out_shape),
            cost_estimate=cost,
            scratch_shapes=list(scratch),
            compiler_params=pltpu.CompilerParams(vmem_limit_bytes=mib << 20),
        )

    def pack(*refs):
        pack_kernel(slabs, copies, *refs)

    message, fields = call(
        pack,
        (
            jax.ShapeDtypeStruct((slabs * copies, 2 * (COMPS + 1), tile), jnp.bfloat16),
            jax.ShapeDtypeStruct((2, *velocity_old.shape), F32),
        ),
        [ANY] * 5,
        8,
        [
            pltpu.VMEM((slabs, tile), jnp.int32),
            pltpu.VMEM(forces.shape, F32),
            pltpu.VMEM((slabs, tile), F32),
            pltpu.SemaphoreType.DMA((5,)),
            pltpu.VMEM((slabs * copies, 2 * (COMPS + 1), tile), jnp.bfloat16),
            pltpu.SemaphoreType.DMA((slabs // 2,)),
        ],
        [ANY, VMEM],
    )(
        *(
            pltpu.with_memory_space_constraint(x, pltpu.HBM)
            for x in (
                cell_ids.reshape(slabs, tile),
                forces,
                weights.reshape(slabs, tile),
                velocity_old,
                courant,
            )
        )
    )
    beside = lax.ppermute(fields, "slab", [(s, s ^ 1) for s in range(slabs)])
    received = lax.all_to_all(message, everyone, 0, 0, tiled=True)
    first, last = call(edges_kernel, (edge, edge), [VMEM] * 2, 2)(fields, beside)
    after = ring(first, "batch", -1)
    before = ring(last, "batch", 1)

    def deposit(*refs):
        deposit_kernel(rows, copies, 8, *refs)

    (deposited,) = call(
        deposit, (jax.ShapeDtypeStruct((2, COMPS * planes * wide, width), F32),), [VMEM], 12
    )(received)

    def setup(*refs):
        setup_kernel(slabs, copies, *refs)

    def flat(count):
        return jax.ShapeDtypeStruct((count, width), F32)

    value, own_solved, solved, inner, *sent, side, block = call(
        setup,
        (field,) * 2 + (both,) * 2 + (flat((2 * COMPS + 1) * wide),) * 2 + (quad,) * 2,
        [VMEM] * 5,
        2,
        [pltpu.VMEM((2, 3, planes, wide, width), F32)],
    )(fields, beside, after, before, deposited)

    values, solves = [value], [own_solved]
    first = None
    for iteration in range(ITERS):
        near = [race(sent[0], 2), race(sent[1], -2)]
        repeat = first is None
        first = first or near
        known = (solved, inner, *near, *first, side, block)
        if iteration + 1 < ITERS:
            reach = wide if iteration + 2 < ITERS else rows

            def advance(*refs):
                advance_kernel(repeat, *refs)

            value, one_solved, second, last_solved, solved, inner, *sent = call(
                advance,
                (field,) * 4 + (both,) * 2 + (flat(COMPS * (wide + reach)),) * 2,
                [VMEM] * 8,
                3,
            )(*known)
            solves += [one_solved, last_solved]
        else:

            def early(*refs):
                early_kernel(rows, *refs)

            sums = call(early, (flat(EARLY_ROWS),) * 2, [VMEM] * EARLY, 2, cost=4000000)(*values)
            value, one_solved, second, message = call(
                gram_kernel, (field,) * 3 + (flat(slabs * copies),), [VMEM] * (10 + EARLY), 4
            )(*known, *values, *sums)
            solves += [one_solved]
        values += [value, second]
    gathered = lax.all_to_all(message, ("batch", "slab"), 0, 0, tiled=True)
    return call(
        finish_kernel,
        (own, own),
        [VMEM] * (1 + BASIS + DEPTH),
        4,
        [pltpu.VMEM(own.shape, F32)] * 2 + [pltpu.SemaphoreType.DMA((2 * COMPS,))],
        ANY,
    )(gathered, *values, *solves)


def solution(mesh):
    placed = (
        P(None, "slab", "batch", None),
        P(None, "slab", "batch", None),
        P(("slab", "batch")),
        P(None, ("slab", "batch")),
        P(("slab", "batch")),
    )
    return jax.shard_map(
        local,
        mesh=mesh,
        in_specs=placed,
        out_specs=(P(None, "slab", "batch", None), P(None, "slab", "batch", None)),
        check_vma=False,
    )
```
